256 devices in a mesh: obs: 64 (over z, x, core), bel: 4 (over y).
Axes of the slice: x: 4, y: 4, z: 8, core: 2. Of those that a mesh axis runs over, the one named last changes fastest.
Arguments:
- alpha_set: bfloat16 [2048, 2048], P('bel'), may hold values from -600 to 600
- transitions: bfloat16 [16, 2048, 2048], P(None, 'obs'), may hold values from 0.0009994507 to 1
- obs_weights: float32 [256, 16, 2048], P('obs'), may hold values from 0.01 to 1
- rewards: float32 [16, 2048], replicated, may hold values from -1 to 1
- chosen_idx: int32 [1536, 16, 256], P('bel', None, 'obs'), may hold values from 0 to 2047
- chosen_action: int32 [1536], P('bel'), may hold values from 0 to 15
Outputs:
- new_alpha: float32 [1536, 2048], P(('bel', 'obs'))
The draws below stay inside these ranges and needn't reach their ends.
Inputs may be any that keep to these rules, and one draw needn't show every extreme that they name: `chosen_idx`: an index into the 2048 alpha vectors. `chosen_action`: an index into the 16 actions.
All inputs are finite; a program needn't handle non-finite values.
Results may differ from the reference program's by a relative error of at most 0.0003.
Values may be sent and summed in bfloat16 or wider, within the bound.
A program may use at most 64 MiB of HBM per device.

```python
import math
import jax
import jax.numpy as jnp
from jax import lax

S = 2048
A = 16
O = 256
K = 2048
BEL = 1536


def touch_ends(result, stream_key, low, largest):
    spot = [jax.random.randint(jax.random.fold_in(stream_key, axis), (), 0, length) for axis, length in enumerate(result.shape)]
    widest = result.shape.index(max(result.shape))
    next_to = spot[:widest] + [(spot[widest] + 1) % result.shape[widest]] + spot[widest + 1:]
    return result.at[tuple(spot)].set(low).at[tuple(next_to)].set(largest)


def levels(stream_key, shape, pieces, smallest, top_value):
    def one(axis_at, blocks):
        draws = jax.random.uniform(jax.random.fold_in(jax.random.fold_in(stream_key, 6), axis_at), (blocks,), jnp.float32, smallest / len(pieces), top_value / len(pieces))
        return jnp.repeat(jnp.exp(draws), shape[axis_at] // blocks).reshape((-1,) + (1,) * (len(shape) - axis_at - 1))

    gain = one(*pieces[0])
    for cut in pieces[1:]:
        gain = gain * one(*cut)
    return gain


def bell_draw(key, dims, spread, most, split=(), kind=jnp.bfloat16):
    gain = levels(key, dims, split, -0.22, 0.18) if split else 1.0
    array = jax.random.normal(key, dims, jnp.float32) * spread * gain
    return jnp.minimum(jnp.maximum(array, -most), most).astype(kind)


def setup_inputs(seed: int = 0) -> dict:
    streams_of = jax.random.split(jax.random.key(seed), 7)
    alpha_set = bell_draw(streams_of[0], (K, S), 100.0, 600.0, ((0, 4),))
    transitions = jnp.clip(jnp.exp(math.log(1.0) - 6.9083047 * jax.random.uniform(streams_of[1], (A, S, S), jnp.float32) ** levels(streams_of[1], (A, S, S), ((1, 64),), -0.2, 0.2)), 0.0009994507, 1.0).astype(jnp.bfloat16)
    obs_weights = jnp.clip(jnp.exp(math.log(1.0) - 4.6051702 * jax.random.uniform(streams_of[2], (O, A, S), jnp.float32) ** levels(streams_of[2], (O, A, S), ((0, 64),), -0.2, 0.2)), 0.01, 1.0)
    rewards = jnp.clip(jax.random.uniform(streams_of[3], (A, S), jnp.float32, -1.0, 1.0), -1.0, 1.0)
    chosen_idx = touch_ends(jax.random.randint(streams_of[4], (BEL, A, O), 0, K), jax.random.fold_in(streams_of[4], 1), 0, K - 1).astype(jnp.int32)
    chosen_action = touch_ends(jax.random.randint(streams_of[5], (BEL,), 0, A), jax.random.fold_in(streams_of[5], 1), 0, A - 1).astype(jnp.int32)
    return {"alpha_set": alpha_set, "transitions": transitions, "obs_weights": obs_weights, "rewards": rewards, "chosen_idx": chosen_idx, "chosen_action": chosen_action}


discount = 0.95


def reference(alpha_set, transitions, obs_weights, rewards, chosen_idx, chosen_action):
    obs_prob = obs_weights / jnp.sum(obs_weights, axis=0, keepdims=True)
    trans_raw = transitions.astype(jnp.float32)
    trans_prob = trans_raw / jnp.sum(trans_raw, axis=1, keepdims=True)
    picked = jnp.take_along_axis(chosen_idx, chosen_action[:, None, None], axis=1)[:, 0, :]

    def add_obs(total, index):
        rows = jnp.take(alpha_set, picked[:, index], axis=0).astype(jnp.float32)
        probs = jnp.take(obs_prob[index], chosen_action, axis=0)
        return total + probs * rows, None

    start = jnp.zeros((BEL, S), jnp.float32)
    weighted, _ = lax.scan(add_obs, start, jnp.arange(O, dtype=jnp.int32))
    action_hot = (chosen_action[:, None] == jnp.arange(A, dtype=jnp.int32)[None, :]).astype(jnp.float32)

    def add_action(total, index):
        block = lax.dynamic_index_in_dim(trans_prob, index, 0, keepdims=False)
        moved = jnp.dot(weighted, block, precision=lax.Precision.HIGHEST, preferred_element_type=jnp.float32)
        column = lax.dynamic_slice_in_dim(action_hot, index, 1, 1)
        return total + column * moved, None

    future, _ = lax.scan(add_action, jnp.zeros((BEL, S), jnp.float32), jnp.arange(A, dtype=jnp.int32))
    reward_rows = jnp.take(rewards, chosen_action, axis=0)
    return reward_rows + discount * future
```

```python
import functools

import jax
import jax.numpy as jnp
from jax import lax
from jax.experimental import pallas as pl
from jax.experimental.pallas import tpu as pltpu
from jax.sharding import Mesh
from jax.sharding import PartitionSpec as P

OBS = ("obs_0", "obs_1", "obs_2")
BEL_OBS = ("bel", "obs_0", "obs_1", "obs_2")
LANES = 128
DISCOUNT = 0.95
MESH = pl.DeviceIdType.MESH


def kernel(
    dims,
    act_s,
    picks_hbm,
    act_i,
    act_b,
    alpha_hbm,
    trans_hbm,
    obs_hbm,
    rew_hbm,
    out_ref,
    al_bf,
    al_rows,
    obs_all,
    obs_rows,
    pk_v,
    pk_s,
    part,
    rs_buf,
    tot_own,
    tot_buf,
    w_all,
    t_blk,
    spread,
    fut,
    f_buf,
    tt_own,
    tt_buf,
    rew_v,
    fin,
    local_sem,
    pk_send,
    pk_recv,
    al_send,
    al_recv,
    ob_send,
    ob_recv,
    t_send,
    t_recv,
    tot_send,
    tot_recv,
    rs_send,
    rs_recv,
    w_send,
    w_recv,
    f_send,
    f_recv,
    tt_send,
    tt_recv,
    o_send,
    o_recv,
):
    ny, nz, nx, nc = dims
    ng = nx * nc
    actions = t_blk.shape[0]
    width = t_blk.shape[1]
    qwidth = t_blk.shape[2]
    halves = width // LANES
    bel = fut.shape[0]
    own_rows = bel // ng
    z_rows = bel // nz
    rows_y = alpha_hbm.shape[0]
    obs_local = obs_hbm.shape[0]
    t_rows = trans_hbm.shape[1]
    pk_len = picks_hbm.shape[0]
    pk_pitch = pk_len // obs_local
    last = fin.shape[1]

    y = lax.axis_index("bel")
    z = lax.axis_index("obs_0")
    x = lax.axis_index("obs_1")
    c = lax.axis_index("obs_2")
    g = x * nc + c

    def y_at(t):
        return lax.rem(y + 1 + t, ny)

    def z_at(t):
        return lax.rem(z + 1 + t, nz)

    def g_at(t):
        return lax.rem(g + 1 + t, ng)

    def to_y(t):
        return {"bel": y_at(t)}

    def to_z(t):
        return {"obs_0": z_at(t)}

    def to_g(t):
        j = g_at(t)
        return {"obs_1": j // nc, "obs_2": lax.rem(j, nc)}

    peers = (
        [to_y(t) for t in range(ny - 1)]
        + [to_z(t) for t in range(nz - 1)]
        + [to_g(t) for t in range(ng - 1)]
    )
    barrier = pltpu.get_barrier_semaphore()
    for peer in peers:
        pl.semaphore_signal(barrier, inc=1, device_id=peer, device_id_type=MESH)

    z_cols = pl.ds(pl.multiple_of(z * width, width), width)
    q_cols = pl.ds(pl.multiple_of(g * qwidth, qwidth), qwidth)

    own_pk = pltpu.make_async_copy(
        picks_hbm, pk_v.at[pl.ds(pl.multiple_of(z * pk_len, pk_len), pk_len)], local_sem.at[0]
    )
    own_al = pltpu.make_async_copy(alpha_hbm.at[:, z_cols], al_bf.at[y], local_sem.at[1])
    own_ob = pltpu.make_async_copy(obs_hbm.at[:, :, z_cols], obs_all.at[z], local_sem.at[2])
    own_t = pltpu.make_async_copy(
        trans_hbm.at[:, :, q_cols],
        t_blk.at[:, pl.ds(pl.multiple_of(g * t_rows, t_rows), t_rows), :],
        local_sem.at[3],
    )
    own_rew = pltpu.make_async_copy(rew_hbm.at[:, q_cols], rew_v, local_sem.at[4])
    own_al.start()
    own_ob.start()
    own_pk.start()
    own_t.start()
    own_rew.start()
    pl.semaphore_wait(barrier, len(peers))

    pk_cp = [
        pltpu.make_async_remote_copy(
            picks_hbm,
            pk_v.at[pl.ds(pl.multiple_of(z * pk_len, pk_len), pk_len)],
            pk_send.at[t],
            pk_recv.at[t],
            device_id=to_z(t),
            device_id_type=MESH,
        )
        for t in range(nz - 1)
    ]
    al_cp = [
        pltpu.make_async_remote_copy(
            alpha_hbm.at[:, z_cols],
            al_bf.at[y],
            al_send.at[t],
            al_recv.at[t],
            device_id=to_y(t),
            device_id_type=MESH,
        )
        for t in range(ny - 1)
    ]
    ob_cp = [
        pltpu.make_async_remote_copy(
            obs_hbm.at[:, :, pl.ds(pl.multiple_of(z_at(t) * width, width), width)],
            obs_all.at[z],
            ob_send.at[t],
            ob_recv.at[t],
            device_id=to_z(t),
            device_id_type=MESH,
        )
        for t in range(nz - 1)
    ]
    t_cp = [
        pltpu.make_async_remote_copy(
            trans_hbm.at[:, :, pl.ds(pl.multiple_of(g_at(t) * qwidth, qwidth), qwidth)],
            t_blk.at[:, pl.ds(pl.multiple_of(g * t_rows, t_rows), t_rows), :],
            t_send.at[t],
            t_recv.at[t],
            device_id=to_g(t),
            device_id_type=MESH,
        )
        for t in range(ng - 1)
    ]
    for cp in pk_cp:
        cp.start()
    for cp in al_cp:
        cp.start()
    for cp in ob_cp:
        cp.start()
    for cp in t_cp:
        cp.start()

    def spread_alpha(block):
        def rows16(n, carry):
            r = pl.multiple_of(n * 16, 16)
            v = al_bf[block, pl.ds(r, 16), :].astype(jnp.float32)
            for h in range(halves):
                al_rows[pl.ds(block * rows_y + r, 16), h, :] = v[:, h * LANES : (h + 1) * LANES]
            return carry

        lax.fori_loop(0, rows_y // 16, rows16, 0, unroll=4)

    own_al.wait()
    spread_alpha(y)

    own_pk.wait()
    for cp in pk_cp:
        cp.wait_recv()
    to_scalar = pltpu.make_async_copy(pk_v, pk_s, local_sem.at[5])
    to_scalar.start()

    own_ob.wait()
    for cp in ob_cp:
        cp.wait_recv()
    totals = [jnp.zeros((actions, LANES), jnp.float32) for _ in range(halves)]
    for s in range(nz):
        for o in range(obs_local):
            for h in range(halves):
                v = obs_all[s, o, :, h * LANES : (h + 1) * LANES]
                totals[h] = totals[h] + v
                first = (s * obs_local + o) * actions
                obs_rows[first : first + actions, h, :] = v
    for h in range(halves):
        tot_own[h] = totals[h]
    tot_cp = [
        pltpu.make_async_remote_copy(
            tot_own, tot_buf.at[t], tot_send.at[t], tot_recv.at[t], device_id=to_g(t), device_id_type=MESH
        )
        for t in range(ng - 1)
    ]
    for cp in tot_cp:
        cp.start()

    for t in range(ny - 1):
        al_cp[t].wait_recv()
        spread_alpha(lax.rem(y + ny - 1 - t, ny))

    to_scalar.wait()
    rs_cp = []
    for t in range(ng):
        j = g_at(t)

        def one_belief(r, carry):
            b = j * own_rows + r
            a = act_s[b]
            sums = [None] * 4
            n = 0
            for s in range(nz):
                for o in range(obs_local):
                    k = pk_s[s * pk_len + o * pk_pitch + b]
                    rows = al_rows[k]
                    probs = obs_rows[(s * obs_local + o) * actions + a]
                    term = rows * probs
                    sums[n % 4] = term if sums[n % 4] is None else sums[n % 4] + term
                    n += 1
            part[pl.ds(pl.multiple_of(b * halves, halves), halves), :] = (sums[0] + sums[1]) + (
                sums[2] + sums[3]
            )
            return carry

        lax.fori_loop(0, own_rows, one_belief, 0)
        if t < ng - 1:
            rows = own_rows * halves
            cp = pltpu.make_async_remote_copy(
                part.at[pl.ds(pl.multiple_of(j * rows, rows), rows), :],
                rs_buf.at[t],
                rs_send.at[t],
                rs_recv.at[t],
                device_id=to_g(t),
                device_id_type=MESH,
            )
            cp.start()
            rs_cp.append(cp)

    for cp in tot_cp:
        cp.wait_recv()
    for cp in rs_cp:
        cp.wait_recv()
    act_own = act_i[pl.ds(pl.multiple_of(g * own_rows, own_rows), own_rows), :]
    for h in range(halves):
        total = tot_own[h]
        for t in range(ng - 1):
            total = total + tot_buf[t, h]
        raw = part[pl.ds(g * own_rows * halves + h, own_rows, stride=halves), :]
        for t in range(ng - 1):
            raw = raw + rs_buf[t, pl.ds(h, own_rows, stride=halves), :]
        divisor = jnp.ones((own_rows, LANES), jnp.float32)
        for a in range(actions):
            divisor = jnp.where(act_own == a, total[a : a + 1, :], divisor)
        w = raw / divisor
        hi = w.astype(jnp.bfloat16)
        lo = (w - hi.astype(jnp.float32)).astype(jnp.bfloat16)
        w_all[g, 0, :, h * LANES : (h + 1) * LANES] = hi
        w_all[g, 1, :, h * LANES : (h + 1) * LANES] = lo

    w_cp = [
        pltpu.make_async_remote_copy(
            w_all.at[g], w_all.at[g], w_send.at[t], w_recv.at[t], device_id=to_g(t), device_id_type=MESH
        )
        for t in range(ng - 1)
    ]
    for cp in w_cp:
        cp.start()
    for cp in w_cp:
        cp.wait_recv()

    def spread_action(a, carry):
        hot = act_b[...] == a.astype(jnp.bfloat16)
        for k in range(2):
            for h in range(halves):
                val = w_all[:, k, :, h * LANES : (h + 1) * LANES].reshape(bel, LANES)
                spread[
                    k * bel : (k + 1) * bel,
                    pl.ds(pl.multiple_of(a * width + h * LANES, LANES), LANES),
                ] = jnp.where(hot, val, jnp.zeros_like(val))
        return carry

    lax.fori_loop(0, actions, spread_action, 0)

    own_t.wait()
    for cp in t_cp:
        cp.wait_recv()
    both = jnp.dot(
        spread[...],
        t_blk[...].reshape(actions * width, qwidth),
        preferred_element_type=jnp.float32,
    )
    fut[...] = both[:bel] + both[bel:]
    f_cp = [
        pltpu.make_async_remote_copy(
            fut.at[pl.ds(pl.multiple_of(z_at(t) * z_rows, z_rows), z_rows), :],
            f_buf.at[t],
            f_send.at[t],
            f_recv.at[t],
            device_id=to_z(t),
            device_id_type=MESH,
        )
        for t in range(nz - 1)
    ]
    for cp in f_cp:
        cp.start()

    def total_action(a, carry):
        tt_own[pl.ds(a, 1), :] = jnp.sum(
            t_blk[a].astype(jnp.float32), axis=0, keepdims=True
        )
        return carry

    lax.fori_loop(0, actions, total_action, 0)
    tt_cp = [
        pltpu.make_async_remote_copy(
            tt_own, tt_buf.at[t], tt_send.at[t], tt_recv.at[t], device_id=to_z(t), device_id_type=MESH
        )
        for t in range(nz - 1)
    ]
    for cp in tt_cp:
        cp.start()
    own_rew.wait()
    for cp in f_cp:
        cp.wait_recv()
    for cp in tt_cp:
        cp.wait_recv()
    z_start = pl.multiple_of(z * z_rows, z_rows)
    act_z = act_i[pl.ds(z_start, z_rows), :]
    for h in range(qwidth // LANES):
        cols = slice(h * LANES, (h + 1) * LANES)
        total = tt_own[:, cols]
        for t in range(nz - 1):
            total = total + tt_buf[t, :, cols]
        future = fut[pl.ds(z_start, z_rows), cols]
        for t in range(nz - 1):
            future = future + f_buf[t, :, cols]
        divisor = jnp.ones((z_rows, LANES), jnp.float32)
        reward = jnp.zeros((z_rows, LANES), jnp.float32)
        for a in range(actions):
            hot = act_z == a
            divisor = jnp.where(hot, total[a : a + 1, :], divisor)
            reward = jnp.where(hot, rew_v[a : a + 1, cols], reward)
        result = reward + DISCOUNT * (future / divisor)
        for n in range(ng):
            fin[n, :, cols] = result[n * last : (n + 1) * last, :]
    o_cp = [
        pltpu.make_async_remote_copy(
            fin.at[g_at(t)],
            out_ref.at[:, q_cols],
            o_send.at[t],
            o_recv.at[t],
            device_id=to_g(t),
            device_id_type=MESH,
        )
        for t in range(ng - 1)
    ]
    for cp in o_cp:
        cp.start()
    out_ref[:, q_cols] = fin[g]
    for cp in o_cp:
        cp.wait_recv()
    for cp in ob_cp + pk_cp + al_cp + t_cp + tot_cp + rs_cp + w_cp + f_cp + tt_cp + o_cp:
        cp.wait_send()


def body(dims, alpha_set, transitions, obs_weights, rewards, chosen_idx, chosen_action):
    ny, nz, nx, nc = dims
    ng = nx * nc
    actions, states = rewards.shape
    bel = chosen_action.shape[0]
    obs_local = obs_weights.shape[0]
    width = states // nz
    qwidth = states // ng
    halves = width // LANES
    count = alpha_set.shape[0] * ny
    hot = chosen_action[:, None] == jnp.arange(actions, dtype=jnp.int32)[None, :]
    picks = jnp.sum(jnp.where(hot[:, :, None], chosen_idx, 0), axis=1).T
    pitch = -(-bel // 256) * 256
    picks = jnp.pad(picks, ((0, 0), (0, pitch - bel))).reshape(-1)
    act_i = jnp.broadcast_to(chosen_action[:, None], (bel, LANES))
    act_b = act_i.astype(jnp.bfloat16)
    f32, b16, i32 = jnp.float32, jnp.bfloat16, jnp.int32
    dma = pltpu.SemaphoreType.DMA
    vmem = pl.BlockSpec(memory_space=pltpu.VMEM)
    hbm = pl.BlockSpec(memory_space=pl.ANY)
    z_rows = bel // nz
    own_rows = bel // ng
    scratch = [
        pltpu.VMEM((ny, count // ny, width), b16),
        pltpu.VMEM((count, halves, LANES), f32),
        pltpu.VMEM((nz, obs_local, actions, width), f32),
        pltpu.VMEM((nz * obs_local * actions, halves, LANES), f32),
        pltpu.VMEM((nz * obs_local * pitch,), i32),
        pltpu.SMEM((nz * obs_local * pitch,), i32),
        pltpu.VMEM((bel * halves, LANES), f32),
        pltpu.VMEM((ng - 1, own_rows * halves, LANES), f32),
        pltpu.VMEM((halves, actions, LANES), f32),
        pltpu.VMEM((ng - 1, halves, actions, LANES), f32),
        pltpu.VMEM((ng, 2, own_rows, width), b16),
        pltpu.VMEM((actions, width, qwidth), b16),
        pltpu.VMEM((2 * bel, actions * width), b16),
        pltpu.VMEM((bel, qwidth), f32),
        pltpu.VMEM((nz - 1, z_rows, qwidth), f32),
        pltpu.VMEM((actions, qwidth), f32),
        pltpu.VMEM((nz - 1, actions, qwidth), f32),
        pltpu.VMEM((actions, qwidth), f32),
        pltpu.VMEM((ng, bel // (nz * ng), qwidth), f32),
        dma((6,)),
        dma((nz - 1,)),
        dma((nz - 1,)),
        dma((ny - 1,)),
        dma((ny - 1,)),
        dma((nz - 1,)),
        dma((nz - 1,)),
        dma((ng - 1,)),
        dma((ng - 1,)),
        dma((ng - 1,)),
        dma((ng - 1,)),
        dma((ng - 1,)),
        dma((ng - 1,)),
        dma((ng - 1,)),
        dma((ng - 1,)),
        dma((nz - 1,)),
        dma((nz - 1,)),
        dma((nz - 1,)),
        dma((nz - 1,)),
        dma((ng - 1,)),
        dma((ng - 1,)),
    ]
    return pl.pallas_call(
        functools.partial(kernel, dims),
        out_shape=jax.ShapeDtypeStruct((bel // (nz * ng), states), f32),
        in_specs=[
            pl.BlockSpec(memory_space=pltpu.SMEM),
            hbm,
            vmem,
            vmem,
            hbm,
            hbm,
            hbm,
            hbm,
        ],
        out_specs=vmem,
        scratch_shapes=scratch,
        compiler_params=pltpu.CompilerParams(
            collective_id=0, has_side_effects=True, vmem_limit_bytes=60 * 1024 * 1024
        ),
        name="backup",
    )(chosen_action, picks, act_i, act_b, alpha_set, transitions, obs_weights, rewards)


def solution(mesh):
    dims = (mesh.shape["bel"], 8, 4, 2)
    torus = Mesh(
        mesh.devices.reshape(*dims[1:], dims[0]), ("obs_0", "obs_1", "obs_2", "bel")
    )
    return jax.shard_map(
        functools.partial(body, dims),
        mesh=torus,
        in_specs=(
            P("bel", None),
            P(None, OBS, None),
            P(OBS, None, None),
            P(),
            P("bel", None, OBS),
            P("bel"),
        ),
        out_specs=P(BEL_OBS, None),
        check_vma=False,
    )
```

```python
import functools

import jax
import jax.numpy as jnp
from jax import lax
from jax.experimental import pallas as pl
from jax.experimental.pallas import tpu as pltpu
from jax.sharding import Mesh
from jax.sharding import PartitionSpec as P

OBS = ("obs_0", "obs_1", "obs_2")
BEL_OBS = ("bel", "obs_0", "obs_1", "obs_2")
LANES = 128
DISCOUNT = 0.95
CODE_SCALE = 14114.0
CODE_SHIFT = 2.302585093 * CODE_SCALE
MESH = pl.DeviceIdType.MESH


def kernel(
    dims,
    act_s,
    act_row,
    idx_ref,
    alpha_hbm,
    trans_hbm,
    obs_hbm,
    rew_hbm,
    out_ref,
    al_bf,
    al_rows,
    act_i,
    act_b,
    obs_v,
    obs_code,
    obs_all,
    obs_rows,
    pk_own,
    pk_v,
    pk_s,
    part,
    rs_buf,
    tot_own,
    tot_buf,
    w_all,
    t_blk,
    spread,
    fut,
    f_buf,
    tt_own,
    tt_buf,
    rew_v,
    fin,
    local_sem,
    pk_send,
    pk_recv,
    al_send,
    al_recv,
    al2_send,
    al2_recv,
    ob_send,
    ob_recv,
    t_send,
    t_recv,
    tot_send,
    tot_recv,
    rs_send,
    rs_recv,
    w_send,
    w_recv,
    f_send,
    f_recv,
    tt_send,
    tt_recv,
    o_send,
    o_recv,
):
    ny, nz, nx, nc = dims
    ng = nx * nc
    actions = t_blk.shape[0]
    width = t_blk.shape[1]
    qwidth = t_blk.shape[2]
    halves = width // LANES
    bel = fut.shape[0]
    own_rows = bel // ng
    z_rows = bel // nz
    rows_y = alpha_hbm.shape[0]
    half_y = rows_y // nc
    obs_local = obs_hbm.shape[0]
    t_rows = trans_hbm.shape[1]
    last = fin.shape[1]

    y = lax.axis_index("bel")
    z = lax.axis_index("obs_0")
    x = lax.axis_index("obs_1")
    c = lax.axis_index("obs_2")
    g = x * nc + c

    def y_at(t):
        return lax.rem(y + 1 + t, ny)

    def z_at(t):
        return lax.rem(z + 1 + t, nz)

    def g_at(t):
        return lax.rem(g + 1 + t, ng)

    def to_y(t):
        return {"bel": y_at(t)}

    def to_z(t):
        return {"obs_0": z_at(t)}

    def to_g(t):
        j = g_at(t)
        return {"obs_1": j // nc, "obs_2": lax.rem(j, nc)}

    peers = (
        [to_y(t) for t in range(ny - 1)]
        + [to_z(t) for t in range(nz - 1)]
        + [to_g(t) for t in range(ng - 1)]
    )
    barrier = pltpu.get_barrier_semaphore()
    for peer in peers:
        pl.semaphore_signal(barrier, inc=1, device_id=peer, device_id_type=MESH)

    z_cols = pl.ds(pl.multiple_of(z * width, width), width)
    q_cols = pl.ds(pl.multiple_of(g * qwidth, qwidth), qwidth)

    own_al = pltpu.make_async_copy(alpha_hbm.at[:, z_cols], al_bf.at[y], local_sem.at[1])
    own_ob = pltpu.make_async_copy(obs_hbm, obs_v, local_sem.at[2])
    own_t = pltpu.make_async_copy(
        trans_hbm.at[:, :, q_cols],
        t_blk.at[:, pl.ds(pl.multiple_of(g * t_rows, t_rows), t_rows), :],
        local_sem.at[3],
    )
    own_rew = pltpu.make_async_copy(rew_hbm.at[:, q_cols], rew_v, local_sem.at[4])
    own_ob.start()
    own_al.start()
    own_t.start()
    own_rew.start()

    picks = jnp.zeros((obs_local, bel), jnp.int32)
    for a in range(actions):
        picks = jnp.where(act_row[...] == a, idx_ref[a], picks)
    for o in range(obs_local):
        pk_own[o] = picks[o : o + 1, :]
        pk_v[z, o] = picks[o : o + 1, :]

    def fill_action(b, carry):
        act_i[pl.ds(b, 1), :] = jnp.full((1, LANES), act_s[b], jnp.int32)
        return carry

    lax.fori_loop(0, bel, fill_action, 0, unroll=8)
    act_b[...] = act_i[...].astype(jnp.float32).astype(jnp.bfloat16)
    own_ob.wait()
    for n in range(nz):
        for o in range(obs_local):
            v = jnp.log(obs_v[o, :, n * width : (n + 1) * width])
            obs_code[n, o] = jnp.round(v * CODE_SCALE + CODE_SHIFT).astype(jnp.int32).astype(jnp.int16)
    pl.semaphore_wait(barrier, len(peers))

    c_rows = pl.ds(pl.multiple_of(c * half_y, half_y), half_y)
    pk_cp = [
        pltpu.make_async_remote_copy(
            pk_own,
            pk_v.at[z],
            pk_send.at[t],
            pk_recv.at[t],
            device_id=to_z(t),
            device_id_type=MESH,
        )
        for t in range(nz - 1)
    ]
    al_cp = [
        pltpu.make_async_remote_copy(
            alpha_hbm.at[c_rows, z_cols],
            al_bf.at[y, c_rows],
            al_send.at[t],
            al_recv.at[t],
            device_id=to_y(t),
            device_id_type=MESH,
        )
        for t in range(ny - 1)
    ]
    ob_cp = [
        pltpu.make_async_remote_copy(
            obs_code.at[z_at(t)],
            obs_all.at[z],
            ob_send.at[t],
            ob_recv.at[t],
            device_id=to_z(t),
            device_id_type=MESH,
        )
        for t in range(nz - 1)
    ]
    t_cp = [
        pltpu.make_async_remote_copy(
            trans_hbm.at[:, :, pl.ds(pl.multiple_of(g_at(t) * qwidth, qwidth), qwidth)],
            t_blk.at[:, pl.ds(pl.multiple_of(g * t_rows, t_rows), t_rows), :],
            t_send.at[t],
            t_recv.at[t],
            device_id=to_g(t),
            device_id_type=MESH,
        )
        for t in range(ng - 1)
    ]
    for cp in pk_cp:
        cp.start()
    for cp in al_cp:
        cp.start()
    for cp in ob_cp:
        cp.start()
    for cp in t_cp:
        cp.start()

    def spread_alpha(block, start, rows):
        def rows16(n, carry):
            r = pl.multiple_of(start + n * 16, 16)
            v = al_bf[block, pl.ds(r, 16), :].astype(jnp.float32)
            for h in range(halves):
                al_rows[pl.ds(block * rows_y + r, 16), h, :] = v[:, h * LANES : (h + 1) * LANES]
            return carry

        lax.fori_loop(0, rows // 16, rows16, 0, unroll=4)

    own_al.wait()
    spread_alpha(y, 0, rows_y)

    for cp in pk_cp:
        cp.wait_recv()
    to_scalar = [
        [
            pltpu.make_async_copy(pk_v.at[n, o], pk_s[n][o], local_sem.at[5 + n * obs_local + o])
            for o in range(obs_local)
        ]
        for n in range(nz)
    ]
    for pair in to_scalar:
        for cp in pair:
            cp.start()

    for o in range(obs_local):
        obs_all[z, o] = obs_code[z, o]
    for cp in ob_cp:
        cp.wait_recv()
    totals = [jnp.zeros((actions, LANES), jnp.float32) for _ in range(halves)]
    for s in range(nz):
        for o in range(obs_local):
            v = jnp.exp(obs_all[s, o].astype(jnp.int32).astype(jnp.float32) * (1.0 / CODE_SCALE))
            for h in range(halves):
                part_h = v[:, h * LANES : (h + 1) * LANES]
                totals[h] = totals[h] + part_h
                obs_rows[s * actions : (s + 1) * actions, o * halves + h, :] = part_h
    for h in range(halves):
        tot_own[h] = totals[h]
    tot_cp = [
        pltpu.make_async_remote_copy(
            tot_own, tot_buf.at[t], tot_send.at[t], tot_recv.at[t], device_id=to_g(t), device_id_type=MESH
        )
        for t in range(ng - 1)
    ]
    for cp in tot_cp:
        cp.start()

    share_cp = []
    for t in range(ny - 1):
        al_cp[t].wait_recv()
        block = lax.rem(y + ny - 1 - t, ny)
        cp = pltpu.make_async_remote_copy(
            al_bf.at[block, c_rows],
            al_bf.at[block, c_rows],
            al2_send.at[t],
            al2_recv.at[t],
            device_id={"obs_2": 1 - c},
            device_id_type=MESH,
        )
        cp.start()
        share_cp.append(cp)
        spread_alpha(block, c * half_y, half_y)
    for t in range(ny - 1):
        share_cp[t].wait_recv()
        spread_alpha(lax.rem(y + ny - 1 - t, ny), (1 - c) * half_y, half_y)
    for pair in to_scalar:
        for cp in pair:
            cp.wait()
    rs_cp = []
    for t in range(ng):
        j = g_at(t)

        def one_belief(r, carry):
            b = j * own_rows + r
            a = act_s[b]
            sums = [None] * 4
            for n in range(nz):
                probs = obs_rows[n * actions + a]
                for o in range(obs_local):
                    term = al_rows[pk_s[n][o][0, b]] * probs[o * halves : (o + 1) * halves]
                    sums[o % 4] = term if n == 0 else sums[o % 4] + term
            part[pl.ds(pl.multiple_of(b * halves, halves), halves), :] = (sums[0] + sums[1]) + (
                sums[2] + sums[3]
            )
            return carry

        lax.fori_loop(0, own_rows, one_belief, 0, unroll=2)
        if t < ng - 1:
            rows = own_rows * halves
            cp = pltpu.make_async_remote_copy(
                part.at[pl.ds(pl.multiple_of(j * rows, rows), rows), :],
                rs_buf.at[t],
                rs_send.at[t],
                rs_recv.at[t],
                device_id=to_g(t),
                device_id_type=MESH,
            )
            cp.start()
            rs_cp.append(cp)

    for cp in tot_cp:
        cp.wait_recv()
    for cp in rs_cp:
        cp.wait_recv()
    act_own = act_i[pl.ds(pl.multiple_of(g * own_rows, own_rows), own_rows), :]
    for h in range(halves):
        total = tot_own[h]
        for t in range(ng - 1):
            total = total + tot_buf[t, h]
        raw = part[pl.ds(g * own_rows * halves + h, own_rows, stride=halves), :]
        for t in range(ng - 1):
            raw = raw + rs_buf[t, pl.ds(h, own_rows, stride=halves), :]
        divisor = jnp.ones((own_rows, LANES), jnp.float32)
        for a in range(actions):
            divisor = jnp.where(act_own == a, total[a : a + 1, :], divisor)
        w = raw / divisor
        hi = w.astype(jnp.bfloat16)
        lo = (w - hi.astype(jnp.float32)).astype(jnp.bfloat16)
        w_all[g, 0, :, h * LANES : (h + 1) * LANES] = hi
        w_all[g, 1, :, h * LANES : (h + 1) * LANES] = lo

    w_cp = [
        pltpu.make_async_remote_copy(
            w_all.at[g], w_all.at[g], w_send.at[t], w_recv.at[t], device_id=to_g(t), device_id_type=MESH
        )
        for t in range(ng - 1)
    ]
    for cp in w_cp:
        cp.start()
    for cp in w_cp:
        cp.wait_recv()

    def spread_action(a, carry):
        hot = act_b[...] == a.astype(jnp.bfloat16)
        for k in range(2):
            for h in range(halves):
                val = w_all[:, k, :, h * LANES : (h + 1) * LANES].reshape(bel, LANES)
                spread[
                    k * bel : (k + 1) * bel,
                    pl.ds(pl.multiple_of(a * width + h * LANES, LANES), LANES),
                ] = jnp.where(hot, val, jnp.zeros_like(val))
        return carry

    lax.fori_loop(0, actions, spread_action, 0)

    own_t.wait()
    for cp in t_cp:
        cp.wait_recv()
    both = jnp.dot(
        spread[...],
        t_blk[...].reshape(actions * width, qwidth),
        preferred_element_type=jnp.float32,
    )
    fut[...] = both[:bel] + both[bel:]
    f_cp = [
        pltpu.make_async_remote_copy(
            fut.at[pl.ds(pl.multiple_of(z_at(t) * z_rows, z_rows), z_rows), :],
            f_buf.at[t],
            f_send.at[t],
            f_recv.at[t],
            device_id=to_z(t),
            device_id_type=MESH,
        )
        for t in range(nz - 1)
    ]
    for cp in f_cp:
        cp.start()

    def total_action(a, carry):
        tt_own[pl.ds(a, 1), :] = jnp.sum(
            t_blk[a].astype(jnp.float32), axis=0, keepdims=True
        )
        return carry

    lax.fori_loop(0, actions, total_action, 0)
    tt_cp = [
        pltpu.make_async_remote_copy(
            tt_own, tt_buf.at[t], tt_send.at[t], tt_recv.at[t], device_id=to_z(t), device_id_type=MESH
        )
        for t in range(nz - 1)
    ]
    for cp in tt_cp:
        cp.start()
    own_rew.wait()
    for cp in f_cp:
        cp.wait_recv()
    for cp in tt_cp:
        cp.wait_recv()
    z_start = pl.multiple_of(z * z_rows, z_rows)
    act_z = act_i[pl.ds(z_start, z_rows), :]
    for h in range(qwidth // LANES):
        cols = slice(h * LANES, (h + 1) * LANES)
        total = tt_own[:, cols]
        for t in range(nz - 1):
            total = total + tt_buf[t, :, cols]
        future = fut[pl.ds(z_start, z_rows), cols]
        for t in range(nz - 1):
            future = future + f_buf[t, :, cols]
        divisor = jnp.ones((z_rows, LANES), jnp.float32)
        reward = jnp.zeros((z_rows, LANES), jnp.float32)
        for a in range(actions):
            hot = act_z == a
            divisor = jnp.where(hot, total[a : a + 1, :], divisor)
            reward = jnp.where(hot, rew_v[a : a + 1, cols], reward)
        result = reward + DISCOUNT * (future / divisor)
        for n in range(ng):
            fin[n, :, cols] = result[n * last : (n + 1) * last, :]
    o_cp = [
        pltpu.make_async_remote_copy(
            fin.at[g_at(t)],
            out_ref.at[:, q_cols],
            o_send.at[t],
            o_recv.at[t],
            device_id=to_g(t),
            device_id_type=MESH,
        )
        for t in range(ng - 1)
    ]
    for cp in o_cp:
        cp.start()
    out_ref[:, q_cols] = fin[g]
    for cp in o_cp:
        cp.wait_recv()
    for cp in ob_cp + pk_cp + al_cp + share_cp + t_cp + tot_cp + rs_cp + w_cp + f_cp + tt_cp + o_cp:
        cp.wait_send()


def body(dims, alpha_set, transitions, obs_weights, rewards, chosen_idx, chosen_action):
    ny, nz, nx, nc = dims
    ng = nx * nc
    actions, states = rewards.shape
    bel = chosen_action.shape[0]
    obs_local = obs_weights.shape[0]
    width = states // nz
    qwidth = states // ng
    halves = width // LANES
    count = alpha_set.shape[0] * ny
    f32, b16, i32 = jnp.float32, jnp.bfloat16, jnp.int32
    dma = pltpu.SemaphoreType.DMA
    vmem = pl.BlockSpec(memory_space=pltpu.VMEM)
    hbm = pl.BlockSpec(memory_space=pl.ANY)
    z_rows = bel // nz
    own_rows = bel // ng
    scratch = [
        pltpu.VMEM((ny, count // ny, width), b16),
        pltpu.VMEM((count, halves, LANES), f32),
        pltpu.VMEM((bel, LANES), i32),
        pltpu.VMEM((bel, LANES), b16),
        pltpu.VMEM((obs_local, actions, states), f32),
        pltpu.VMEM((nz, obs_local, actions, width), jnp.int16),
        pltpu.VMEM((nz, obs_local, actions, width), jnp.int16),
        pltpu.VMEM((nz * actions, obs_local * halves, LANES), f32),
        pltpu.VMEM((obs_local, 1, bel), i32),
        pltpu.VMEM((nz, obs_local, 1, bel), i32),
        [[pltpu.SMEM((1, bel), i32) for _ in range(obs_local)] for _ in range(nz)],
        pltpu.VMEM((bel * halves, LANES), f32),
        pltpu.VMEM((ng - 1, own_rows * halves, LANES), f32),
        pltpu.VMEM((halves, actions, LANES), f32),
        pltpu.VMEM((ng - 1, halves, actions, LANES), f32),
        pltpu.VMEM((ng, 2, own_rows, width), b16),
        pltpu.VMEM((actions, width, qwidth), b16),
        pltpu.VMEM((2 * bel, actions * width), b16),
        pltpu.VMEM((bel, qwidth), f32),
        pltpu.VMEM((nz - 1, z_rows, qwidth), f32),
        pltpu.VMEM((actions, qwidth), f32),
        pltpu.VMEM((nz - 1, actions, qwidth), f32),
        pltpu.VMEM((actions, qwidth), f32),
        pltpu.VMEM((ng, bel // (nz * ng), qwidth), f32),
        dma((5 + nz * obs_local,)),
        dma((nz - 1,)),
        dma((nz - 1,)),
        dma((ny - 1,)),
        dma((ny - 1,)),
        dma((ny - 1,)),
        dma((ny - 1,)),
        dma((nz - 1,)),
        dma((nz - 1,)),
        dma((ng - 1,)),
        dma((ng - 1,)),
        dma((ng - 1,)),
        dma((ng - 1,)),
        dma((ng - 1,)),
        dma((ng - 1,)),
        dma((ng - 1,)),
        dma((ng - 1,)),
        dma((nz - 1,)),
        dma((nz - 1,)),
        dma((nz - 1,)),
        dma((nz - 1,)),
        dma((ng - 1,)),
        dma((ng - 1,)),
    ]
    return pl.pallas_call(
        functools.partial(kernel, dims),
        out_shape=jax.ShapeDtypeStruct((bel // (nz * ng), states), f32),
        in_specs=[
            pl.BlockSpec(memory_space=pltpu.SMEM),
            vmem,
            vmem,
            hbm,
            hbm,
            hbm,
            hbm,
        ],
        out_specs=vmem,
        scratch_shapes=scratch,
        compiler_params=pltpu.CompilerParams(
            collective_id=0, has_side_effects=True, vmem_limit_bytes=60 * 1024 * 1024
        ),
        name="backup",
    )(
        chosen_action,
        chosen_action.reshape(1, bel),
        jnp.transpose(chosen_idx, (1, 2, 0)),
        alpha_set,
        transitions,
        obs_weights,
        rewards,
    )


def solution(mesh):
    dims = (mesh.shape["bel"], 8, 4, 2)
    torus = Mesh(
        mesh.devices.reshape(*dims[1:], dims[0]), ("obs_0", "obs_1", "obs_2", "bel")
    )
    return jax.shard_map(
        functools.partial(body, dims),
        mesh=torus,
        in_specs=(
            P("bel", None),
            P(None, OBS, None),
            P(OBS, None, None),
            P(),
            P("bel", None, OBS),
            P("bel"),
        ),
        out_specs=P(BEL_OBS, None),
        check_vma=False,
    )
```

```python
import functools

import jax
import jax.numpy as jnp
from jax import lax
from jax.experimental import pallas as pl
from jax.experimental.pallas import tpu as pltpu
from jax.sharding import Mesh
from jax.sharding import PartitionSpec as P

OBS = ("obs_0", "obs_1", "obs_2")
BEL_OBS = ("bel", "obs_0", "obs_1", "obs_2")
LANES = 128
DISCOUNT = 0.95
CODE_SCALE = 14114.0
CODE_SHIFT = 2.302585093 * CODE_SCALE
MESH = pl.DeviceIdType.MESH


def to_codes(values):
    largest = functools.reduce(
        jnp.maximum, [jnp.max(jnp.abs(v), axis=(0, 1), keepdims=True) for v in values]
    )
    level = jnp.ceil(32.0 * jnp.log(jnp.maximum(largest, 1e-30) * (1.0 / 32760.0)))
    inverse = jnp.exp(level * (-1.0 / 32.0))
    coded = [
        jnp.clip(jnp.round(v * inverse), -32767.0, 32767.0).astype(jnp.int32).astype(jnp.int16)
        for v in values
    ]
    return coded, jnp.broadcast_to(level, (8, LANES)).astype(jnp.int32).astype(jnp.int16)


def scale_of(level):
    return jnp.exp(level.astype(jnp.int32).astype(jnp.float32) * (1.0 / 32.0))


def kernel(
    dims,
    act_s,
    act_row,
    idx_ref,
    alpha_hbm,
    trans_hbm,
    obs_hbm,
    rew_hbm,
    out_ref,
    al_bf,
    al_rows,
    act_i,
    act_b,
    obs_v,
    obs_code,
    obs_all,
    obs_rows,
    pk_own,
    pk_v,
    pk_s,
    part,
    rs_buf,
    tot_own,
    tot_buf,
    w_all,
    t_blk,
    spread,
    w_scale,
    fut,
    fut_q,
    f_buf,
    tt_own,
    tt_buf,
    rew_v,
    fin,
    local_sem,
    pk_send,
    pk_recv,
    al_send,
    al_recv,
    al2_send,
    al2_recv,
    ob_send,
    ob_recv,
    t_send,
    t_recv,
    ts_send,
    ts_recv,
    ty_send,
    ty_recv,
    tot_send,
    tot_recv,
    rs_send,
    rs_recv,
    w_send,
    w_recv,
    f_send,
    f_recv,
    tt_send,
    tt_recv,
    o_send,
    o_recv,
):
    ny, nz, nx, nc = dims
    ng = nx * nc
    actions = t_blk.shape[0]
    width = t_blk.shape[1]
    qwidth = t_blk.shape[2]
    halves = width // LANES
    bel = fut.shape[0]
    own_rows = bel // ng
    z_rows = bel // nz
    rows_y = alpha_hbm.shape[0]
    half_y = rows_y // nc
    obs_local = obs_hbm.shape[0]
    t_rows = trans_hbm.shape[1]
    last = fin.shape[1]
    per_y = actions // (2 * ny)
    direct = actions - per_y * ny

    y = lax.axis_index("bel")
    z = lax.axis_index("obs_0")
    x = lax.axis_index("obs_1")
    c = lax.axis_index("obs_2")
    g = x * nc + c

    def y_at(t):
        return lax.rem(y + 1 + t, ny)

    def z_at(t):
        return lax.rem(z + 1 + t, nz)

    def g_at(t):
        return lax.rem(g + 1 + t, ng)

    def to_y(t):
        return {"bel": y_at(t)}

    def to_z(t):
        return {"obs_0": z_at(t)}

    def to_g(t):
        j = g_at(t)
        return {"obs_1": j // nc, "obs_2": lax.rem(j, nc)}

    peers = (
        [to_y(t) for t in range(ny - 1)]
        + [to_z(t) for t in range(nz - 1)]
        + [to_g(t) for t in range(ng - 1)]
    )
    barrier = pltpu.get_barrier_semaphore()
    for peer in peers:
        pl.semaphore_signal(barrier, inc=1, device_id=peer, device_id_type=MESH)

    z_cols = pl.ds(pl.multiple_of(z * width, width), width)
    q_cols = pl.ds(pl.multiple_of(g * qwidth, qwidth), qwidth)

    own_al = pltpu.make_async_copy(alpha_hbm.at[:, z_cols], al_bf.at[y], local_sem.at[1])
    own_ob = pltpu.make_async_copy(obs_hbm, obs_v, local_sem.at[2])
    g_rows = pl.ds(pl.multiple_of(g * t_rows, t_rows), t_rows)
    mine = pl.ds(direct + y * per_y, per_y)
    own_t = pltpu.make_async_copy(
        trans_hbm.at[:direct, :, q_cols], t_blk.at[:direct, g_rows, :], local_sem.at[3]
    )
    own_ts = pltpu.make_async_copy(
        trans_hbm.at[mine, :, q_cols], t_blk.at[mine, g_rows, :], local_sem.at[0]
    )
    own_rew = pltpu.make_async_copy(rew_hbm.at[:, q_cols], rew_v, local_sem.at[4])
    own_ob.start()
    own_al.start()
    own_t.start()
    own_ts.start()
    own_rew.start()

    picks = jnp.zeros((obs_local, bel), jnp.int32)
    for a in range(actions):
        picks = jnp.where(act_row[...] == a, idx_ref[a], picks)
    for o in range(obs_local):
        pk_own[o] = picks[o : o + 1, :]
        pk_v[z, o] = picks[o : o + 1, :]

    def fill_action(b, carry):
        act_i[pl.ds(b, 1), :] = jnp.full((1, LANES), act_s[b], jnp.int32)
        return carry

    lax.fori_loop(0, bel, fill_action, 0, unroll=8)
    act_b[...] = act_i[...].astype(jnp.float32).astype(jnp.bfloat16)
    own_ob.wait()
    for n in range(nz):
        for o in range(obs_local):
            v = jnp.log(obs_v[o, :, n * width : (n + 1) * width])
            obs_code[n, o] = jnp.round(v * CODE_SCALE + CODE_SHIFT).astype(jnp.int32).astype(jnp.int16)
    pl.semaphore_wait(barrier, len(peers))

    c_rows = pl.ds(pl.multiple_of(c * half_y, half_y), half_y)
    pk_cp = [
        pltpu.make_async_remote_copy(
            pk_own,
            pk_v.at[z],
            pk_send.at[t],
            pk_recv.at[t],
            device_id=to_z(t),
            device_id_type=MESH,
        )
        for t in range(nz - 1)
    ]
    al_cp = [
        pltpu.make_async_remote_copy(
            alpha_hbm.at[c_rows, z_cols],
            al_bf.at[y, c_rows],
            al_send.at[t],
            al_recv.at[t],
            device_id=to_y(t),
            device_id_type=MESH,
        )
        for t in range(ny - 1)
    ]
    ob_cp = [
        pltpu.make_async_remote_copy(
            obs_code.at[z_at(t)],
            obs_all.at[z],
            ob_send.at[t],
            ob_recv.at[t],
            device_id=to_z(t),
            device_id_type=MESH,
        )
        for t in range(nz - 1)
    ]
    def trans_copy(t, which, send, recv):
        return pltpu.make_async_remote_copy(
            trans_hbm.at[which, :, pl.ds(pl.multiple_of(g_at(t) * qwidth, qwidth), qwidth)],
            t_blk.at[which, g_rows, :],
            send.at[t],
            recv.at[t],
            device_id=to_g(t),
            device_id_type=MESH,
        )

    ts_cp = [trans_copy(t, mine, ts_send, ts_recv) for t in range(ng - 1)]
    t_cp = [trans_copy(t, pl.ds(0, direct), t_send, t_recv) for t in range(ng - 1)]
    for cp in pk_cp:
        cp.start()
    for cp in al_cp:
        cp.start()
    for cp in ob_cp:
        cp.start()
    for cp in ts_cp:
        cp.start()
    for cp in t_cp:
        cp.start()

    def spread_alpha(block, start, rows):
        def rows16(n, carry):
            r = pl.multiple_of(start + n * 16, 16)
            v = al_bf[block, pl.ds(r, 16), :].astype(jnp.float32)
            for h in range(halves):
                al_rows[pl.ds(block * rows_y + r, 16), h, :] = v[:, h * LANES : (h + 1) * LANES]
            return carry

        lax.fori_loop(0, rows // 16, rows16, 0, unroll=4)

    own_al.wait()
    spread_alpha(y, 0, rows_y)

    for cp in pk_cp:
        cp.wait_recv()
    to_scalar = [
        [
            pltpu.make_async_copy(pk_v.at[n, o], pk_s[n][o], local_sem.at[5 + n * obs_local + o])
            for o in range(obs_local)
        ]
        for n in range(nz)
    ]
    for pair in to_scalar:
        for cp in pair:
            cp.start()

    for o in range(obs_local):
        obs_all[z, o] = obs_code[z, o]
    for cp in ob_cp:
        cp.wait_recv()
    totals = [jnp.zeros((actions, LANES), jnp.float32) for _ in range(halves)]
    for s in range(nz):
        for o in range(obs_local):
            v = jnp.exp(obs_all[s, o].astype(jnp.int32).astype(jnp.float32) * (1.0 / CODE_SCALE))
            for h in range(halves):
                part_h = v[:, h * LANES : (h + 1) * LANES]
                totals[h] = totals[h] + part_h
                obs_rows[s * actions : (s + 1) * actions, o * halves + h, :] = part_h
    for h in range(halves):
        tot_own[h] = totals[h]
    tot_cp = [
        pltpu.make_async_remote_copy(
            tot_own, tot_buf.at[t], tot_send.at[t], tot_recv.at[t], device_id=to_g(t), device_id_type=MESH
        )
        for t in range(ng - 1)
    ]
    for cp in tot_cp:
        cp.start()

    share_cp = []
    for t in range(ny - 1):
        al_cp[t].wait_recv()
        block = lax.rem(y + ny - 1 - t, ny)
        cp = pltpu.make_async_remote_copy(
            al_bf.at[block, c_rows],
            al_bf.at[block, c_rows],
            al2_send.at[t],
            al2_recv.at[t],
            device_id={"obs_2": 1 - c},
            device_id_type=MESH,
        )
        cp.start()
        share_cp.append(cp)
        spread_alpha(block, c * half_y, half_y)
    for t in range(ny - 1):
        share_cp[t].wait_recv()
        spread_alpha(lax.rem(y + ny - 1 - t, ny), (1 - c) * half_y, half_y)
    own_ts.wait()
    for cp in ts_cp:
        cp.wait_recv()
    ty_cp = [
        pltpu.make_async_remote_copy(
            t_blk.at[mine],
            t_blk.at[mine],
            ty_send.at[t],
            ty_recv.at[t],
            device_id=to_y(t),
            device_id_type=MESH,
        )
        for t in range(ny - 1)
    ]
    for cp in ty_cp:
        cp.start()
    for pair in to_scalar:
        for cp in pair:
            cp.wait()
    rs_cp = []
    for t in range(ng):
        j = g_at(t)

        def one_belief(r, carry):
            b = j * own_rows + r
            a = act_s[b]
            sums = [None] * 4
            for n in range(nz):
                probs = obs_rows[n * actions + a]
                for o in range(obs_local):
                    term = al_rows[pk_s[n][o][0, b]] * probs[o * halves : (o + 1) * halves]
                    sums[o % 4] = term if n == 0 else sums[o % 4] + term
            part[pl.ds(pl.multiple_of(b * halves, halves), halves), :] = (sums[0] + sums[1]) + (
                sums[2] + sums[3]
            )
            return carry

        lax.fori_loop(0, own_rows, one_belief, 0, unroll=2)
        if t < ng - 1:
            rows = own_rows * halves
            cp = pltpu.make_async_remote_copy(
                part.at[pl.ds(pl.multiple_of(j * rows, rows), rows), :],
                rs_buf.at[t],
                rs_send.at[t],
                rs_recv.at[t],
                device_id=to_g(t),
                device_id_type=MESH,
            )
            cp.start()
            rs_cp.append(cp)

    for cp in tot_cp:
        cp.wait_recv()
    for cp in rs_cp:
        cp.wait_recv()
    act_own = act_i[pl.ds(pl.multiple_of(g * own_rows, own_rows), own_rows), :]
    values = []
    for h in range(halves):
        total = tot_own[h]
        for t in range(ng - 1):
            total = total + tot_buf[t, h]
        raw = part[pl.ds(g * own_rows * halves + h, own_rows, stride=halves), :]
        for t in range(ng - 1):
            raw = raw + rs_buf[t, pl.ds(h, own_rows, stride=halves), :]
        divisor = jnp.ones((own_rows, LANES), jnp.float32)
        for a in range(actions):
            divisor = jnp.where(act_own == a, total[a : a + 1, :], divisor)
        values.append(raw / divisor)
    coded, level = to_codes(values)
    for h in range(halves):
        cols = slice(h * LANES, (h + 1) * LANES)
        w_all[g, :own_rows, cols] = coded[h]
        w_all[g, own_rows:, cols] = level

    w_cp = [
        pltpu.make_async_remote_copy(
            w_all.at[g], w_all.at[g], w_send.at[t], w_recv.at[t], device_id=to_g(t), device_id_type=MESH
        )
        for t in range(ng - 1)
    ]
    for cp in w_cp:
        cp.start()

    def spread_owner(j):
        rows = pl.ds(pl.multiple_of(j * own_rows, own_rows), own_rows)
        low_rows = pl.ds(pl.multiple_of(bel + j * own_rows, own_rows), own_rows)
        w_scale[rows, :] = jnp.broadcast_to(
            scale_of(w_all[j, own_rows : own_rows + 1, :]), (own_rows, width)
        )[:, :qwidth]
        act = act_b[rows, :]
        pieces = []
        for h in range(halves):
            q = w_all[j, :own_rows, h * LANES : (h + 1) * LANES].astype(jnp.int32)
            high = jnp.right_shift(q + 128, 8)
            low = q - jnp.left_shift(high, 8)
            pieces.append((high.astype(jnp.float32).astype(jnp.bfloat16), low.astype(jnp.float32).astype(jnp.bfloat16)))

        for a in range(actions):
            hot = act == jnp.asarray(a, jnp.bfloat16)
            for h in range(halves):
                high, low = pieces[h]
                cols = slice(a * width + h * LANES, a * width + (h + 1) * LANES)
                spread[rows, cols] = jnp.where(hot, high, jnp.zeros_like(high))
                spread[low_rows, cols] = jnp.where(hot, low, jnp.zeros_like(low))

    spread_owner(g)
    own_t.wait()
    for cp in t_cp:
        cp.wait_recv()
    for cp in ty_cp:
        cp.wait_recv()

    def total_action(a, carry):
        tt_own[pl.ds(a, 1), :] = jnp.sum(
            t_blk[a].astype(jnp.float32), axis=0, keepdims=True
        )
        return carry

    lax.fori_loop(0, actions, total_action, 0)
    tt_cp = [
        pltpu.make_async_remote_copy(
            tt_own, tt_buf.at[t], tt_send.at[t], tt_recv.at[t], device_id=to_z(t), device_id_type=MESH
        )
        for t in range(nz - 1)
    ]
    for cp in tt_cp:
        cp.start()

    for t in range(ng - 1):
        w_cp[t].wait_recv()
        spread_owner(lax.rem(g + ng - 1 - t, ng))
    both = jnp.dot(
        spread[...],
        t_blk[...].reshape(actions * width, qwidth),
        preferred_element_type=jnp.float32,
    )
    fut[...] = (256.0 * both[:bel] + both[bel:]) * w_scale[...]
    f_cp = [
        pltpu.make_async_remote_copy(
            fut_q.at[z_at(t)],
            f_buf.at[t],
            f_send.at[t],
            f_recv.at[t],
            device_id=to_z(t),
            device_id_type=MESH,
        )
        for t in range(nz - 1)
    ]
    for t in range(nz - 1):
        j = z_at(t)
        rows = pl.ds(pl.multiple_of(j * z_rows, z_rows), z_rows)
        (coded,), level = to_codes([fut[rows, :]])
        fut_q[j, :z_rows, :] = coded
        for h in range(qwidth // LANES):
            fut_q[j, z_rows:, h * LANES : (h + 1) * LANES] = level
        f_cp[t].start()
    own_rew.wait()
    for cp in f_cp:
        cp.wait_recv()
    for cp in tt_cp:
        cp.wait_recv()
    z_start = pl.multiple_of(z * z_rows, z_rows)
    act_z = act_i[pl.ds(z_start, z_rows), :]
    for h in range(qwidth // LANES):
        cols = slice(h * LANES, (h + 1) * LANES)
        total = tt_own[:, cols]
        for t in range(nz - 1):
            total = total + tt_buf[t, :, cols]
        future = fut[pl.ds(z_start, z_rows), cols]
        for t in range(nz - 1):
            piece = f_buf[t, :z_rows, cols].astype(jnp.int32).astype(jnp.float32)
            future = future + piece * scale_of(f_buf[t, z_rows : z_rows + 1, cols])
        divisor = jnp.ones((z_rows, LANES), jnp.float32)
        reward = jnp.zeros((z_rows, LANES), jnp.float32)
        for a in range(actions):
            hot = act_z == a
            divisor = jnp.where(hot, total[a : a + 1, :], divisor)
            reward = jnp.where(hot, rew_v[a : a + 1, cols], reward)
        result = reward + DISCOUNT * (future / divisor)
        for n in range(ng):
            fin[n, :, cols] = result[n * last : (n + 1) * last, :]
    o_cp = [
        pltpu.make_async_remote_copy(
            fin.at[g_at(t)],
            out_ref.at[:, q_cols],
            o_send.at[t],
            o_recv.at[t],
            device_id=to_g(t),
            device_id_type=MESH,
        )
        for t in range(ng - 1)
    ]
    for cp in o_cp:
        cp.start()
    out_ref[:, q_cols] = fin[g]
    for cp in o_cp:
        cp.wait_recv()
    for cp in ob_cp + pk_cp + al_cp + share_cp + ts_cp + ty_cp + t_cp + tot_cp + rs_cp + w_cp + f_cp + tt_cp + o_cp:
        cp.wait_send()


def body(dims, alpha_set, transitions, obs_weights, rewards, chosen_idx, chosen_action):
    ny, nz, nx, nc = dims
    ng = nx * nc
    actions, states = rewards.shape
    bel = chosen_action.shape[0]
    obs_local = obs_weights.shape[0]
    width = states // nz
    qwidth = states // ng
    halves = width // LANES
    count = alpha_set.shape[0] * ny
    f32, b16, i32 = jnp.float32, jnp.bfloat16, jnp.int32
    dma = pltpu.SemaphoreType.DMA
    vmem = pl.BlockSpec(memory_space=pltpu.VMEM)
    hbm = pl.BlockSpec(memory_space=pl.ANY)
    z_rows = bel // nz
    own_rows = bel // ng
    scratch = [
        pltpu.VMEM((ny, count // ny, width), b16),
        pltpu.VMEM((count, halves, LANES), f32),
        pltpu.VMEM((bel, LANES), i32),
        pltpu.VMEM((bel, LANES), b16),
        pltpu.VMEM((obs_local, actions, states), f32),
        pltpu.VMEM((nz, obs_local, actions, width), jnp.int16),
        pltpu.VMEM((nz, obs_local, actions, width), jnp.int16),
        pltpu.VMEM((nz * actions, obs_local * halves, LANES), f32),
        pltpu.VMEM((obs_local, 1, bel), i32),
        pltpu.VMEM((nz, obs_local, 1, bel), i32),
        [[pltpu.SMEM((1, bel), i32) for _ in range(obs_local)] for _ in range(nz)],
        pltpu.VMEM((bel * halves, LANES), f32),
        pltpu.VMEM((ng - 1, own_rows * halves, LANES), f32),
        pltpu.VMEM((halves, actions, LANES), f32),
        pltpu.VMEM((ng - 1, halves, actions, LANES), f32),
        pltpu.VMEM((ng, own_rows + 8, width), jnp.int16),
        pltpu.VMEM((actions, width, qwidth), b16),
        pltpu.VMEM((2 * bel, actions * width), b16),
        pltpu.VMEM((bel, qwidth), f32),
        pltpu.VMEM((bel, qwidth), f32),
        pltpu.VMEM((nz, z_rows + 8, qwidth), jnp.int16),
        pltpu.VMEM((nz - 1, z_rows + 8, qwidth), jnp.int16),
        pltpu.VMEM((actions, qwidth), f32),
        pltpu.VMEM((nz - 1, actions, qwidth), f32),
        pltpu.VMEM((actions, qwidth), f32),
        pltpu.VMEM((ng, bel // (nz * ng), qwidth), f32),
        dma((5 + nz * obs_local,)),
        dma((nz - 1,)),
        dma((nz - 1,)),
        dma((ny - 1,)),
        dma((ny - 1,)),
        dma((ny - 1,)),
        dma((ny - 1,)),
        dma((nz - 1,)),
        dma((nz - 1,)),
        dma((ng - 1,)),
        dma((ng - 1,)),
        dma((ng - 1,)),
        dma((ng - 1,)),
        dma((ny - 1,)),
        dma((ny - 1,)),
        dma((ng - 1,)),
        dma((ng - 1,)),
        dma((ng - 1,)),
        dma((ng - 1,)),
        dma((ng - 1,)),
        dma((ng - 1,)),
        dma((nz - 1,)),
        dma((nz - 1,)),
        dma((nz - 1,)),
        dma((nz - 1,)),
        dma((ng - 1,)),
        dma((ng - 1,)),
    ]
    return pl.pallas_call(
        functools.partial(kernel, dims),
        out_shape=jax.ShapeDtypeStruct((bel // (nz * ng), states), f32),
        in_specs=[
            pl.BlockSpec(memory_space=pltpu.SMEM),
            vmem,
            vmem,
            hbm,
            hbm,
            hbm,
            hbm,
        ],
        out_specs=vmem,
        scratch_shapes=scratch,
        compiler_params=pltpu.CompilerParams(
            collective_id=0, has_side_effects=True, vmem_limit_bytes=60 * 1024 * 1024
        ),
        name="backup",
    )(
        chosen_action,
        chosen_action.reshape(1, bel),
        jnp.transpose(chosen_idx, (1, 2, 0)),
        alpha_set,
        transitions,
        obs_weights,
        rewards,
    )


def solution(mesh):
    dims = (mesh.shape["bel"], 8, 4, 2)
    torus = Mesh(
        mesh.devices.reshape(*dims[1:], dims[0]), ("obs_0", "obs_1", "obs_2", "bel")
    )
    return jax.shard_map(
        functools.partial(body, dims),
        mesh=torus,
        in_specs=(
            P("bel", None),
            P(None, OBS, None),
            P(OBS, None, None),
            P(),
            P("bel", None, OBS),
            P("bel"),
        ),
        out_specs=P(BEL_OBS, None),
        check_vma=False,
    )
```

```python
import functools

import jax
import jax.numpy as jnp
from jax import lax
from jax.experimental import pallas as pl
from jax.experimental.pallas import tpu as pltpu
from jax.sharding import Mesh
from jax.sharding import PartitionSpec as P

OBS = ("obs_0", "obs_1", "obs_2")
BEL_OBS = ("bel", "obs_0", "obs_1", "obs_2")
LANES = 128
DISCOUNT = 0.95
CODE_SCALE = 14114.0
CODE_SHIFT = 2.302585093 * CODE_SCALE
MESH = pl.DeviceIdType.MESH


def to_codes(values):
    largest = functools.reduce(
        jnp.maximum, [jnp.max(jnp.abs(v), axis=(0, 1), keepdims=True) for v in values]
    )
    level = jnp.ceil(32.0 * jnp.log(jnp.maximum(largest, 1e-30) * (1.0 / 32760.0)))
    inverse = jnp.exp(level * (-1.0 / 32.0))
    coded = [
        jnp.clip(jnp.round(v * inverse), -32767.0, 32767.0).astype(jnp.int32).astype(jnp.int16)
        for v in values
    ]
    return coded, jnp.broadcast_to(level, (8, LANES)).astype(jnp.int32).astype(jnp.int16)


def scale_of(level):
    return jnp.exp(level.astype(jnp.int32).astype(jnp.float32) * (1.0 / 32.0))


def far_first(n):
    return sorted(range(n - 1), key=lambda t: -min(t + 1, n - 1 - t))


def kernel(
    dims,
    act_s,
    act_row,
    idx_ref,
    alpha_hbm,
    trans_hbm,
    obs_hbm,
    rew_hbm,
    out_ref,
    al_bf,
    al_rows,
    act_i,
    act_b,
    obs_v,
    obs_code,
    obs_all,
    obs_rows,
    pk_own,
    pk_v,
    pk_s,
    part,
    rs_buf,
    tot_own,
    tot_buf,
    w_all,
    t_blk,
    spread,
    w_scale,
    fut,
    fut_q,
    f_buf,
    tt_own,
    tt_buf,
    rew_v,
    fin,
    local_sem,
    pk_send,
    pk_recv,
    al_send,
    al_recv,
    relay_send,
    relay_recv,
    share_send,
    share_recv,
    ob_send,
    ob_recv,
    t_send,
    t_recv,
    ts_send,
    ts_recv,
    ty_send,
    ty_recv,
    tot_send,
    tot_recv,
    rs_send,
    rs_recv,
    w_send,
    w_recv,
    f_send,
    f_recv,
    tt_send,
    tt_recv,
    o_send,
    o_recv,
):
    ny, nz, nx, nc = dims
    ng = nx * nc
    actions = t_blk.shape[0]
    width = t_blk.shape[1]
    qwidth = t_blk.shape[2]
    halves = width // LANES
    bel = fut.shape[0]
    own_rows = bel // ng
    z_rows = bel // nz
    rows_y = alpha_hbm.shape[0]
    half_y = rows_y // nc
    obs_local = obs_hbm.shape[0]
    t_rows = trans_hbm.shape[1]
    last = fin.shape[1]
    per_y = actions // (2 * ny)
    direct = actions - per_y * ny

    y = lax.axis_index("bel")
    z = lax.axis_index("obs_0")
    x = lax.axis_index("obs_1")
    c = lax.axis_index("obs_2")
    g = x * nc + c

    def y_at(t):
        return lax.rem(y + 1 + t, ny)

    def z_at(t):
        return lax.rem(z + 1 + t, nz)

    def g_at(t):
        return lax.rem(g + 1 + t, ng)

    def to_y(t):
        return {"bel": y_at(t)}

    def to_z(t):
        return {"obs_0": z_at(t)}

    def to_g(t):
        j = g_at(t)
        return {"obs_1": j // nc, "obs_2": lax.rem(j, nc)}

    peers = (
        [to_y(t) for t in range(ny - 1)]
        + [to_z(t) for t in range(nz - 1)]
        + [to_g(t) for t in range(ng - 1)]
    )
    barrier = pltpu.get_barrier_semaphore()
    for peer in peers:
        pl.semaphore_signal(barrier, inc=1, device_id=peer, device_id_type=MESH)

    z_cols = pl.ds(pl.multiple_of(z * width, width), width)
    q_cols = pl.ds(pl.multiple_of(g * qwidth, qwidth), qwidth)

    own_al = pltpu.make_async_copy(alpha_hbm.at[:, z_cols], al_bf.at[y], local_sem.at[1])
    own_ob = pltpu.make_async_copy(obs_hbm, obs_v, local_sem.at[2])
    g_rows = pl.ds(pl.multiple_of(g * t_rows, t_rows), t_rows)
    mine = pl.ds(direct + y * per_y, per_y)
    own_t = pltpu.make_async_copy(
        trans_hbm.at[:direct, :, q_cols], t_blk.at[:direct, g_rows, :], local_sem.at[3]
    )
    own_ts = pltpu.make_async_copy(
        trans_hbm.at[mine, :, q_cols], t_blk.at[mine, g_rows, :], local_sem.at[0]
    )
    own_rew = pltpu.make_async_copy(rew_hbm.at[:, q_cols], rew_v, local_sem.at[4])
    own_ob.start()
    own_al.start()
    own_t.start()
    own_ts.start()
    own_rew.start()

    picks = jnp.zeros((obs_local, bel), jnp.int32)
    for a in range(actions):
        picks = jnp.where(act_row[...] == a, idx_ref[a] * halves, picks)
    for o in range(obs_local):
        pk_own[o] = picks[o : o + 1, :]
        pk_v[z, o] = picks[o : o + 1, :]

    def fill_action(b, carry):
        act_i[pl.ds(b, 1), :] = jnp.full((1, LANES), act_s[b], jnp.int32)
        return carry

    lax.fori_loop(0, bel, fill_action, 0, unroll=8)
    act_b[...] = act_i[...].astype(jnp.float32).astype(jnp.bfloat16)
    own_ob.wait()
    for n in range(nz):
        for o in range(obs_local):
            v = jnp.log(obs_v[o, :, n * width : (n + 1) * width])
            obs_code[n, o] = jnp.round(v * CODE_SCALE + CODE_SHIFT).astype(jnp.int32).astype(jnp.int16)
    pl.semaphore_wait(barrier, len(peers))

    c_rows = pl.ds(pl.multiple_of(c * half_y, half_y), half_y)
    pk_cp = [
        pltpu.make_async_remote_copy(
            pk_own,
            pk_v.at[z],
            pk_send.at[t],
            pk_recv.at[t],
            device_id=to_z(t),
            device_id_type=MESH,
        )
        for t in range(nz - 1)
    ]
    al_cp = [
        pltpu.make_async_remote_copy(
            alpha_hbm.at[c_rows, z_cols],
            al_bf.at[y, c_rows],
            al_send.at[t],
            al_recv.at[t],
            device_id={"bel": lax.rem(y + step, ny)},
            device_id_type=MESH,
        )
        for t, step in ((0, 1), (1, ny - 1))
    ]
    ob_cp = [
        pltpu.make_async_remote_copy(
            obs_code.at[z_at(t)],
            obs_all.at[z],
            ob_send.at[t],
            ob_recv.at[t],
            device_id=to_z(t),
            device_id_type=MESH,
        )
        for t in range(nz - 1)
    ]
    def trans_copy(t, which, send, recv):
        return pltpu.make_async_remote_copy(
            trans_hbm.at[which, :, pl.ds(pl.multiple_of(g_at(t) * qwidth, qwidth), qwidth)],
            t_blk.at[which, g_rows, :],
            send.at[t],
            recv.at[t],
            device_id=to_g(t),
            device_id_type=MESH,
        )

    ts_cp = [trans_copy(t, mine, ts_send, ts_recv) for t in range(ng - 1)]
    t_cp = [trans_copy(t, pl.ds(0, direct), t_send, t_recv) for t in range(ng - 1)]
    for cp in pk_cp:
        cp.start()
    for cp in al_cp:
        cp.start()
    for t in far_first(nz):
        ob_cp[t].start()
    for cp in ts_cp:
        cp.start()
    for cp in t_cp:
        cp.start()

    def spread_alpha(block, start, rows):
        def rows16(n, carry):
            r = pl.multiple_of(start + n * 16, 16)
            v = al_bf[block, pl.ds(r, 16), :].astype(jnp.float32)
            for h in range(halves):
                al_rows[pl.ds((block * rows_y + r) * halves + h, 16, stride=halves), :] = v[
                    :, h * LANES : (h + 1) * LANES
                ]
            return carry

        lax.fori_loop(0, rows // 16, rows16, 0, unroll=4)

    own_al.wait()
    spread_alpha(y, 0, rows_y)

    for cp in pk_cp:
        cp.wait_recv()
    to_scalar = [
        [
            pltpu.make_async_copy(pk_v.at[n, o], pk_s[n][o], local_sem.at[5 + n * obs_local + o])
            for o in range(obs_local)
        ]
        for n in range(nz)
    ]
    for pair in to_scalar:
        for cp in pair:
            cp.start()

    totals = [jnp.zeros((actions, LANES), jnp.float32) for _ in range(halves)]

    def decode(code_ref, slot):
        for o in range(obs_local):
            v = jnp.exp(
                code_ref[slot, o].astype(jnp.int32).astype(jnp.float32) * (1.0 / CODE_SCALE)
            )
            for h in range(halves):
                part_h = v[:, h * LANES : (h + 1) * LANES]
                totals[h] = totals[h] + part_h
                obs_rows[pl.ds(slot * actions, actions), o * halves + h, :] = part_h

    decode(obs_code, z)
    share_cp = []

    def share(block, rows):
        cp = pltpu.make_async_remote_copy(
            al_bf.at[block, rows],
            al_bf.at[block, rows],
            share_send.at[len(share_cp)],
            share_recv.at[len(share_cp)],
            device_id={"obs_2": 1 - c},
            device_id_type=MESH,
        )
        cp.start()
        share_cp.append(cp)

    before, after, across = (lax.rem(y + n, ny) for n in (ny - 1, 1, ny - 2))
    quarter = half_y // 2
    quarters = [pl.ds(pl.multiple_of(c * half_y + n * quarter, quarter), quarter) for n in range(2)]
    relay_cp = []
    for t, (source, target) in enumerate(((before, after), (after, before))):
        al_cp[t].wait_recv()
        cp = pltpu.make_async_remote_copy(
            al_bf.at[source, quarters[t]],
            al_bf.at[source, quarters[t]],
            relay_send.at[t],
            relay_recv.at[t],
            device_id={"bel": target},
            device_id_type=MESH,
        )
        cp.start()
        relay_cp.append(cp)
        share(source, c_rows)
    for source in (before, after):
        spread_alpha(source, c * half_y, half_y)
    for t in range(2):
        relay_cp[t].wait_recv()
        share(across, quarters[t])
    spread_alpha(across, c * half_y, half_y)
    for t in far_first(nz):
        ob_cp[t].wait_recv()
        decode(obs_all, lax.rem(z + nz - 1 - t, nz))
    for h in range(halves):
        tot_own[h] = totals[h]
    tot_cp = [
        pltpu.make_async_remote_copy(
            tot_own, tot_buf.at[t], tot_send.at[t], tot_recv.at[t], device_id=to_g(t), device_id_type=MESH
        )
        for t in range(ng - 1)
    ]
    for cp in tot_cp:
        cp.start()

    other = (1 - c) * half_y
    for cp, (source, start, rows) in zip(
        share_cp,
        (
            (before, other, half_y),
            (after, other, half_y),
            (across, other, quarter),
            (across, other + quarter, quarter),
        ),
    ):
        cp.wait_recv()
        spread_alpha(source, start, rows)
    own_ts.wait()
    for cp in ts_cp:
        cp.wait_recv()
    ty_cp = [
        pltpu.make_async_remote_copy(
            t_blk.at[mine],
            t_blk.at[mine],
            ty_send.at[t],
            ty_recv.at[t],
            device_id=to_y(t),
            device_id_type=MESH,
        )
        for t in range(ny - 1)
    ]
    for cp in ty_cp:
        cp.start()
    for pair in to_scalar:
        for cp in pair:
            cp.wait()
    rs_cp = []
    for t in range(ng):
        j = g_at(t)

        def one_belief(r, carry):
            b = j * own_rows + r
            a = act_s[b]
            sums = [None] * 4
            for n in range(nz):
                probs = obs_rows[n * actions + a]
                for o in range(obs_local):
                    term = al_rows[pl.ds(pk_s[n][o][0, b], halves), :] * probs[o * halves : (o + 1) * halves]
                    sums[o % 4] = term if n == 0 else sums[o % 4] + term
            part[pl.ds(pl.multiple_of(b * halves, halves), halves), :] = (sums[0] + sums[1]) + (
                sums[2] + sums[3]
            )
            return carry

        lax.fori_loop(0, own_rows, one_belief, 0, unroll=4)
        if t < ng - 1:
            rows = own_rows * halves
            cp = pltpu.make_async_remote_copy(
                part.at[pl.ds(pl.multiple_of(j * rows, rows), rows), :],
                rs_buf.at[t],
                rs_send.at[t],
                rs_recv.at[t],
                device_id=to_g(t),
                device_id_type=MESH,
            )
            cp.start()
            rs_cp.append(cp)

    for cp in tot_cp:
        cp.wait_recv()
    for cp in rs_cp:
        cp.wait_recv()
    act_own = act_i[pl.ds(pl.multiple_of(g * own_rows, own_rows), own_rows), :]
    values = []
    for h in range(halves):
        total = tot_own[h]
        for t in range(ng - 1):
            total = total + tot_buf[t, h]
        raw = part[pl.ds(g * own_rows * halves + h, own_rows, stride=halves), :]
        for t in range(ng - 1):
            raw = raw + rs_buf[t, pl.ds(h, own_rows, stride=halves), :]
        divisor = jnp.ones((own_rows, LANES), jnp.float32)
        for a in range(actions):
            divisor = jnp.where(act_own == a, total[a : a + 1, :], divisor)
        values.append(raw / divisor)
    coded, level = to_codes(values)
    for h in range(halves):
        cols = slice(h * LANES, (h + 1) * LANES)
        w_all[g, :own_rows, cols] = coded[h]
        w_all[g, own_rows:, cols] = level

    w_cp = [
        pltpu.make_async_remote_copy(
            w_all.at[g], w_all.at[g], w_send.at[t], w_recv.at[t], device_id=to_g(t), device_id_type=MESH
        )
        for t in range(ng - 1)
    ]
    for cp in w_cp:
        cp.start()

    def spread_owner(j):
        rows = pl.ds(pl.multiple_of(j * own_rows, own_rows), own_rows)
        half = j // (ng // 2)
        high_rows = pl.ds(pl.multiple_of((half * (ng // 2) + j) * own_rows, own_rows), own_rows)
        low_rows = pl.ds(
            pl.multiple_of((half * (ng // 2) + j) * own_rows + bel // 2, own_rows), own_rows
        )
        w_scale[rows, :] = jnp.broadcast_to(
            scale_of(w_all[j, own_rows : own_rows + 1, :]), (own_rows, width)
        )[:, :qwidth]
        act = act_b[rows, :]
        pieces = []
        for h in range(halves):
            q = w_all[j, :own_rows, h * LANES : (h + 1) * LANES].astype(jnp.int32)
            high = jnp.right_shift(q + 128, 8)
            low = q - jnp.left_shift(high, 8)
            pieces.append((high.astype(jnp.float32).astype(jnp.bfloat16), low.astype(jnp.float32).astype(jnp.bfloat16)))

        for a in range(actions):
            hot = act == jnp.asarray(a, jnp.bfloat16)
            for h in range(halves):
                high, low = pieces[h]
                cols = slice(a * width + h * LANES, a * width + (h + 1) * LANES)
                spread[high_rows, cols] = jnp.where(hot, high, jnp.zeros_like(high))
                spread[low_rows, cols] = jnp.where(hot, low, jnp.zeros_like(low))

    spread_owner(g)
    own_t.wait()
    for cp in t_cp:
        cp.wait_recv()
    for cp in ty_cp:
        cp.wait_recv()

    def total_action(a, carry):
        tt_own[pl.ds(a, 1), :] = jnp.sum(
            t_blk[a].astype(jnp.float32), axis=0, keepdims=True
        )
        return carry

    lax.fori_loop(0, actions, total_action, 0)
    tt_cp = [
        pltpu.make_async_remote_copy(
            tt_own, tt_buf.at[t], tt_send.at[t], tt_recv.at[t], device_id=to_z(t), device_id_type=MESH
        )
        for t in range(nz - 1)
    ]
    for cp in tt_cp:
        cp.start()

    for t in range(ng - 1):
        w_cp[t].wait_recv()
        spread_owner(lax.rem(g + ng - 1 - t, ng))
    half_bel = bel // 2
    group = nz // 2

    def future_half(half):
        rows = pl.ds(pl.multiple_of(half * half_bel, half_bel), half_bel)
        both = jnp.dot(
            spread[pl.ds(pl.multiple_of(half * bel, bel), bel), :],
            t_blk[...].reshape(actions * width, qwidth),
            preferred_element_type=jnp.float32,
        )
        fut[rows, :] = (256.0 * both[:half_bel] + both[half_bel:]) * w_scale[rows, :]

    def send_future(j, t):
        rows = pl.ds(pl.multiple_of(j * z_rows, z_rows), z_rows)
        (coded,), level = to_codes([fut[rows, :]])
        fut_q[j, :z_rows, :] = coded
        for h in range(qwidth // LANES):
            fut_q[j, z_rows:, h * LANES : (h + 1) * LANES] = level
        cp = pltpu.make_async_remote_copy(
            fut_q.at[j],
            f_buf.at[t],
            f_send.at[t],
            f_recv.at[t],
            device_id={"obs_0": j},
            device_id_type=MESH,
        )
        cp.start()
        f_cp.append(cp)

    f_cp = []
    z_half = z // group
    far_half = 1 - z_half
    future_half(far_half)
    for n in range(group):
        send_future(far_half * group + lax.rem(z + n, group), n)
    future_half(z_half)
    for n in range(1, group):
        send_future(z_half * group + lax.rem(z + n, group), group - 1 + n)
    own_rew.wait()
    for cp in f_cp:
        cp.wait_recv()
    for cp in tt_cp:
        cp.wait_recv()
    z_start = pl.multiple_of(z * z_rows, z_rows)
    act_z = act_i[pl.ds(z_start, z_rows), :]
    for h in range(qwidth // LANES):
        cols = slice(h * LANES, (h + 1) * LANES)
        total = tt_own[:, cols]
        for t in range(nz - 1):
            total = total + tt_buf[t, :, cols]
        future = fut[pl.ds(z_start, z_rows), cols]
        for t in range(nz - 1):
            piece = f_buf[t, :z_rows, cols].astype(jnp.int32).astype(jnp.float32)
            future = future + piece * scale_of(f_buf[t, z_rows : z_rows + 1, cols])
        divisor = jnp.ones((z_rows, LANES), jnp.float32)
        reward = jnp.zeros((z_rows, LANES), jnp.float32)
        for a in range(actions):
            hot = act_z == a
            divisor = jnp.where(hot, total[a : a + 1, :], divisor)
            reward = jnp.where(hot, rew_v[a : a + 1, cols], reward)
        result = reward + DISCOUNT * (future / divisor)
        for n in range(ng):
            fin[n, :, cols] = result[n * last : (n + 1) * last, :]
    o_cp = [
        pltpu.make_async_remote_copy(
            fin.at[g_at(t)],
            out_ref.at[:, q_cols],
            o_send.at[t],
            o_recv.at[t],
            device_id=to_g(t),
            device_id_type=MESH,
        )
        for t in range(ng - 1)
    ]
    for cp in o_cp:
        cp.start()
    out_ref[:, q_cols] = fin[g]
    for cp in o_cp:
        cp.wait_recv()
    for cp in ob_cp + pk_cp + al_cp + share_cp + ts_cp + ty_cp + t_cp + relay_cp + tot_cp + rs_cp + w_cp + f_cp + tt_cp + o_cp:
        cp.wait_send()


def body(dims, alpha_set, transitions, obs_weights, rewards, chosen_idx, chosen_action):
    ny, nz, nx, nc = dims
    ng = nx * nc
    actions, states = rewards.shape
    bel = chosen_action.shape[0]
    obs_local = obs_weights.shape[0]
    width = states // nz
    qwidth = states // ng
    halves = width // LANES
    count = alpha_set.shape[0] * ny
    f32, b16, i32 = jnp.float32, jnp.bfloat16, jnp.int32
    dma = pltpu.SemaphoreType.DMA
    vmem = pl.BlockSpec(memory_space=pltpu.VMEM)
    hbm = pl.BlockSpec(memory_space=pl.ANY)
    z_rows = bel // nz
    own_rows = bel // ng
    scratch = [
        pltpu.VMEM((ny, count // ny, width), b16),
        pltpu.VMEM((count * halves, LANES), f32),
        pltpu.VMEM((bel, LANES), i32),
        pltpu.VMEM((bel, LANES), b16),
        pltpu.VMEM((obs_local, actions, states), f32),
        pltpu.VMEM((nz, obs_local, actions, width), jnp.int16),
        pltpu.VMEM((nz, obs_local, actions, width), jnp.int16),
        pltpu.VMEM((nz * actions, obs_local * halves, LANES), f32),
        pltpu.VMEM((obs_local, 1, bel), i32),
        pltpu.VMEM((nz, obs_local, 1, bel), i32),
        [[pltpu.SMEM((1, bel), i32) for _ in range(obs_local)] for _ in range(nz)],
        pltpu.VMEM((bel * halves, LANES), f32),
        pltpu.VMEM((ng - 1, own_rows * halves, LANES), f32),
        pltpu.VMEM((halves, actions, LANES), f32),
        pltpu.VMEM((ng - 1, halves, actions, LANES), f32),
        pltpu.VMEM((ng, own_rows + 8, width), jnp.int16),
        pltpu.VMEM((actions, width, qwidth), b16),
        pltpu.VMEM((2 * bel, actions * width), b16),
        pltpu.VMEM((bel, qwidth), f32),
        pltpu.VMEM((bel, qwidth), f32),
        pltpu.VMEM((nz, z_rows + 8, qwidth), jnp.int16),
        pltpu.VMEM((nz - 1, z_rows + 8, qwidth), jnp.int16),
        pltpu.VMEM((actions, qwidth), f32),
        pltpu.VMEM((nz - 1, actions, qwidth), f32),
        pltpu.VMEM((actions, qwidth), f32),
        pltpu.VMEM((ng, bel // (nz * ng), qwidth), f32),
        dma((5 + nz * obs_local,)),
        dma((nz - 1,)),
        dma((nz - 1,)),
        dma((2,)),
        dma((2,)),
        dma((2,)),
        dma((2,)),
        dma((4,)),
        dma((4,)),
        dma((nz - 1,)),
        dma((nz - 1,)),
        dma((ng - 1,)),
        dma((ng - 1,)),
        dma((ng - 1,)),
        dma((ng - 1,)),
        dma((ny - 1,)),
        dma((ny - 1,)),
        dma((ng - 1,)),
        dma((ng - 1,)),
        dma((ng - 1,)),
        dma((ng - 1,)),
        dma((ng - 1,)),
        dma((ng - 1,)),
        dma((nz - 1,)),
        dma((nz - 1,)),
        dma((nz - 1,)),
        dma((nz - 1,)),
        dma((ng - 1,)),
        dma((ng - 1,)),
    ]
    return pl.pallas_call(
        functools.partial(kernel, dims),
        out_shape=jax.ShapeDtypeStruct((bel // (nz * ng), states), f32),
        in_specs=[
            pl.BlockSpec(memory_space=pltpu.SMEM),
            vmem,
            vmem,
            hbm,
            hbm,
            hbm,
            hbm,
        ],
        out_specs=vmem,
        scratch_shapes=scratch,
        compiler_params=pltpu.CompilerParams(
            collective_id=0, has_side_effects=True, vmem_limit_bytes=60 * 1024 * 1024
        ),
        name="backup",
    )(
        chosen_action,
        chosen_action.reshape(1, bel),
        jnp.transpose(chosen_idx, (1, 2, 0)),
        alpha_set,
        transitions,
        obs_weights,
        rewards,
    )


def solution(mesh):
    dims = (mesh.shape["bel"], 8, 4, 2)
    torus = Mesh(
        mesh.devices.reshape(*dims[1:], dims[0]), ("obs_0", "obs_1", "obs_2", "bel")
    )
    return jax.shard_map(
        functools.partial(body, dims),
        mesh=torus,
        in_specs=(
            P("bel", None),
            P(None, OBS, None),
            P(OBS, None, None),
            P(),
            P("bel", None, OBS),
            P("bel"),
        ),
        out_specs=P(BEL_OBS, None),
        check_vma=False,
    )
```

```python
import functools

import jax
import jax.numpy as jnp
from jax import lax
from jax.experimental import pallas as pl
from jax.experimental.pallas import tpu as pltpu
from jax.sharding import Mesh
from jax.sharding import PartitionSpec as P

OBS = ("obs_0", "obs_1", "obs_2")
BEL_OBS = ("bel", "obs_0", "obs_1", "obs_2")
LANES = 128
DISCOUNT = 0.95
CODE_SCALE = 14114.0
CODE_SHIFT = 2.302585093 * CODE_SCALE
MESH = pl.DeviceIdType.MESH


def to_codes(values):
    largest = functools.reduce(
        jnp.maximum, [jnp.max(jnp.abs(v), axis=(0, 1), keepdims=True) for v in values]
    )
    level = jnp.ceil(32.0 * jnp.log(jnp.maximum(largest, 1e-30) * (1.0 / 32760.0)))
    inverse = jnp.exp(level * (-1.0 / 32.0))
    coded = [
        jnp.clip(jnp.round(v * inverse), -32767.0, 32767.0).astype(jnp.int32).astype(jnp.int16)
        for v in values
    ]
    return coded, jnp.broadcast_to(level, (8, LANES)).astype(jnp.int32).astype(jnp.int16)


def scale_of(level):
    return jnp.exp(level.astype(jnp.int32).astype(jnp.float32) * (1.0 / 32.0))


def far_first(n):
    return sorted(range(n - 1), key=lambda t: -min(t + 1, n - 1 - t))


def group_offsets(nx, nc):
    steps = [(dx, dc) for dx in range(nx) for dc in range(nc) if dx or dc]
    return sorted(steps, key=lambda step: -min(step[0], nx - step[0]))


def kernel(
    dims,
    act_s,
    act_row,
    idx_ref,
    alpha_hbm,
    trans_hbm,
    obs_hbm,
    rew_hbm,
    out_ref,
    al_bf,
    al_rows,
    act_i,
    act_b,
    obs_v,
    obs_code,
    obs_all,
    obs_rows,
    pk_own,
    pk_v,
    pk_s,
    part,
    rs_buf,
    tot_own,
    tot_buf,
    w_all,
    t_blk,
    spread,
    w_scale,
    fut,
    fut_q,
    f_buf,
    tt_own,
    tt_buf,
    rew_v,
    fin,
    local_sem,
    pk_send,
    pk_recv,
    al_send,
    al_recv,
    relay_send,
    relay_recv,
    share_send,
    share_recv,
    ob_send,
    ob_recv,
    t_send,
    t_recv,
    ts_send,
    ts_recv,
    ty_send,
    ty_recv,
    tot_send,
    tot_recv,
    rs_send,
    rs_recv,
    w_send,
    w_recv,
    f_send,
    f_recv,
    tt_send,
    tt_recv,
    o_send,
    o_recv,
):
    ny, nz, nx, nc = dims
    ng = nx * nc
    actions = t_blk.shape[0]
    width = t_blk.shape[1]
    qwidth = t_blk.shape[2]
    halves = width // LANES
    bel = fut.shape[0]
    own_rows = bel // ng
    z_rows = bel // nz
    rows_y = alpha_hbm.shape[0]
    half_y = rows_y // nc
    obs_local = obs_hbm.shape[0]
    t_rows = trans_hbm.shape[1]
    last = fin.shape[1]
    per_y = actions // (2 * ny)
    direct = actions - per_y * ny

    y = lax.axis_index("bel")
    z = lax.axis_index("obs_0")
    x = lax.axis_index("obs_1")
    c = lax.axis_index("obs_2")
    g = x * nc + c

    def y_at(t):
        return lax.rem(y + 1 + t, ny)

    def z_at(t):
        return lax.rem(z + 1 + t, nz)

    offsets = group_offsets(nx, nc)

    def g_at(t):
        dx, dc = offsets[t]
        return lax.rem(x + dx, nx) * nc + lax.rem(c + dc, nc)

    def g_from(t):
        dx, dc = offsets[t]
        return lax.rem(x + nx - dx, nx) * nc + lax.rem(c + nc - dc, nc)

    def to_y(t):
        return {"bel": y_at(t)}

    def to_z(t):
        return {"obs_0": z_at(t)}

    def to_g(t):
        j = g_at(t)
        return {"obs_1": j // nc, "obs_2": lax.rem(j, nc)}

    peers = (
        [to_y(t) for t in range(ny - 1)]
        + [to_z(t) for t in range(nz - 1)]
        + [to_g(t) for t in range(ng - 1)]
    )
    barrier = pltpu.get_barrier_semaphore()
    for peer in peers:
        pl.semaphore_signal(barrier, inc=1, device_id=peer, device_id_type=MESH)

    z_cols = pl.ds(pl.multiple_of(z * width, width), width)
    q_cols = pl.ds(pl.multiple_of(g * qwidth, qwidth), qwidth)

    own_al = pltpu.make_async_copy(alpha_hbm.at[:, z_cols], al_bf.at[y], local_sem.at[1])
    own_ob = pltpu.make_async_copy(obs_hbm, obs_v, local_sem.at[2])
    g_rows = pl.ds(pl.multiple_of(g * t_rows, t_rows), t_rows)
    mine = pl.ds(direct + y * per_y, per_y)
    own_t = pltpu.make_async_copy(
        trans_hbm.at[:direct, :, q_cols], t_blk.at[:direct, g_rows, :], local_sem.at[3]
    )
    own_ts = pltpu.make_async_copy(
        trans_hbm.at[mine, :, q_cols], t_blk.at[mine, g_rows, :], local_sem.at[0]
    )
    own_rew = pltpu.make_async_copy(rew_hbm.at[:, q_cols], rew_v, local_sem.at[4])
    own_ob.start()
    own_al.start()
    own_t.start()
    own_ts.start()
    own_rew.start()

    picks = jnp.zeros((obs_local, bel), jnp.int32)
    for a in range(actions):
        picks = jnp.where(act_row[...] == a, idx_ref[a] * halves, picks)
    for o in range(obs_local):
        pk_own[o] = picks[o : o + 1, :]
        pk_v[z, o] = picks[o : o + 1, :]

    def fill_action(b, carry):
        act_i[pl.ds(b, 1), :] = jnp.full((1, LANES), act_s[b], jnp.int32)
        return carry

    lax.fori_loop(0, bel, fill_action, 0, unroll=8)
    act_b[...] = act_i[...].astype(jnp.float32).astype(jnp.bfloat16)
    own_ob.wait()
    for n in range(nz):
        for o in range(obs_local):
            v = jnp.log(obs_v[o, :, n * width : (n + 1) * width])
            obs_code[n, o] = jnp.round(v * CODE_SCALE + CODE_SHIFT).astype(jnp.int32).astype(jnp.int16)
    pl.semaphore_wait(barrier, len(peers))

    quarter = half_y // 2
    quarters = [pl.ds(pl.multiple_of(c * half_y + n * quarter, quarter), quarter) for n in range(2)]
    pk_cp = [
        pltpu.make_async_remote_copy(
            pk_own,
            pk_v.at[z],
            pk_send.at[t],
            pk_recv.at[t],
            device_id=to_z(t),
            device_id_type=MESH,
        )
        for t in range(nz - 1)
    ]
    al_cp = [
        [
            pltpu.make_async_remote_copy(
                al_bf.at[y, quarters[n]],
                al_bf.at[y, quarters[n]],
                al_send.at[t, m],
                al_recv.at[t, m],
                device_id={"bel": lax.rem(y + step, ny)},
                device_id_type=MESH,
            )
            for m, n in enumerate((t, 1 - t))
        ]
        for t, step in ((0, 1), (1, ny - 1))
    ]
    ob_cp = [
        pltpu.make_async_remote_copy(
            obs_code.at[z_at(t)],
            obs_all.at[z],
            ob_send.at[t],
            ob_recv.at[t],
            device_id=to_z(t),
            device_id_type=MESH,
        )
        for t in range(nz - 1)
    ]
    def trans_copy(t, which, send, recv):
        return pltpu.make_async_remote_copy(
            trans_hbm.at[which, :, pl.ds(pl.multiple_of(g_at(t) * qwidth, qwidth), qwidth)],
            t_blk.at[which, g_rows, :],
            send.at[t],
            recv.at[t],
            device_id=to_g(t),
            device_id_type=MESH,
        )

    ts_cp = [trans_copy(t, mine, ts_send, ts_recv) for t in range(ng - 1)]
    t_cp = [trans_copy(t, pl.ds(0, direct), t_send, t_recv) for t in range(ng - 1)]
    for cp in pk_cp:
        cp.start()
    own_al.wait()
    for m in range(2):
        for pair in al_cp:
            pair[m].start()
    for t in far_first(nz):
        ob_cp[t].start()
    for cp in ts_cp:
        cp.start()
    for cp in t_cp:
        cp.start()

    def spread_alpha(block, start, rows):
        def rows16(n, carry):
            r = pl.multiple_of(start + n * 16, 16)
            v = al_bf[block, pl.ds(r, 16), :].astype(jnp.float32)
            for h in range(halves):
                al_rows[pl.ds((block * rows_y + r) * halves + h, 16, stride=halves), :] = v[
                    :, h * LANES : (h + 1) * LANES
                ]
            return carry

        lax.fori_loop(0, rows // 16, rows16, 0, unroll=4)

    spread_alpha(y, 0, rows_y)

    for cp in pk_cp:
        cp.wait_recv()
    to_scalar = [
        [
            pltpu.make_async_copy(pk_v.at[n, o], pk_s[n][o], local_sem.at[5 + n * obs_local + o])
            for o in range(obs_local)
        ]
        for n in range(nz)
    ]
    for pair in to_scalar:
        for cp in pair:
            cp.start()

    totals = [jnp.zeros((actions, LANES), jnp.float32) for _ in range(halves)]

    def decode(code_ref, slot):
        for o in range(obs_local):
            v = jnp.exp(
                code_ref[slot, o].astype(jnp.int32).astype(jnp.float32) * (1.0 / CODE_SCALE)
            )
            for h in range(halves):
                part_h = v[:, h * LANES : (h + 1) * LANES]
                totals[h] = totals[h] + part_h
                obs_rows[pl.ds(slot * actions, actions), o * halves + h, :] = part_h

    decode(obs_code, z)
    share_cp = []

    def share(block, rows):
        cp = pltpu.make_async_remote_copy(
            al_bf.at[block, rows],
            al_bf.at[block, rows],
            share_send.at[len(share_cp)],
            share_recv.at[len(share_cp)],
            device_id={"obs_2": 1 - c},
            device_id_type=MESH,
        )
        cp.start()
        share_cp.append(cp)

    before, after, across = (lax.rem(y + n, ny) for n in (ny - 1, 1, ny - 2))
    relay_cp = []
    for t, (source, target) in enumerate(((before, after), (after, before))):
        al_cp[t][0].wait_recv()
        cp = pltpu.make_async_remote_copy(
            al_bf.at[source, quarters[t]],
            al_bf.at[source, quarters[t]],
            relay_send.at[t],
            relay_recv.at[t],
            device_id={"bel": target},
            device_id_type=MESH,
        )
        cp.start()
        relay_cp.append(cp)
    for t, source in enumerate((before, after)):
        share(source, quarters[t])
    for t, source in enumerate((before, after)):
        al_cp[t][1].wait_recv()
        share(source, quarters[1 - t])
    own_ts.wait()
    for cp in ts_cp:
        cp.wait_recv()

    def trans_share(which, n, target):
        return pltpu.make_async_remote_copy(
            t_blk.at[which],
            t_blk.at[which],
            ty_send.at[n],
            ty_recv.at[n],
            device_id={"bel": target},
            device_id_type=MESH,
        )

    ty_cp = [trans_share(mine, 0, after), trans_share(mine, 1, before)]
    for cp in ty_cp:
        cp.start()
    for source in (before, after):
        spread_alpha(source, c * half_y, half_y)
    for t in range(2):
        relay_cp[t].wait_recv()
        share(across, quarters[t])
    spread_alpha(across, c * half_y, half_y)
    for t in far_first(nz):
        ob_cp[t].wait_recv()
        decode(obs_all, lax.rem(z + nz - 1 - t, nz))
    for h in range(halves):
        tot_own[h] = totals[h]
    tot_cp = [
        pltpu.make_async_remote_copy(
            tot_own, tot_buf.at[t], tot_send.at[t], tot_recv.at[t], device_id=to_g(t), device_id_type=MESH
        )
        for t in range(ng - 1)
    ]
    for cp in tot_cp:
        cp.start()

    other = (1 - c) * half_y
    for cp, (source, n) in zip(
        share_cp, ((before, 0), (after, 1), (before, 1), (after, 0), (across, 0), (across, 1))
    ):
        cp.wait_recv()
        spread_alpha(source, other + n * quarter, quarter)
    for pair in to_scalar:
        for cp in pair:
            cp.wait()
    rs_cp = []
    for t in range(ng):
        j = g_at(t) if t < ng - 1 else g

        def one_belief(r, carry):
            b = j * own_rows + r
            a = act_s[b]
            sums = [None] * 4
            for n in range(nz):
                probs = obs_rows[n * actions + a]
                for o in range(obs_local):
                    term = al_rows[pl.ds(pk_s[n][o][0, b], halves), :] * probs[o * halves : (o + 1) * halves]
                    sums[o % 4] = term if n == 0 else sums[o % 4] + term
            part[pl.ds(pl.multiple_of(b * halves, halves), halves), :] = (sums[0] + sums[1]) + (
                sums[2] + sums[3]
            )
            return carry

        lax.fori_loop(0, own_rows, one_belief, 0, unroll=4)
        if t < ng - 1:
            rows = own_rows * halves
            cp = pltpu.make_async_remote_copy(
                part.at[pl.ds(pl.multiple_of(j * rows, rows), rows), :],
                rs_buf.at[t],
                rs_send.at[t],
                rs_recv.at[t],
                device_id=to_g(t),
                device_id_type=MESH,
            )
            cp.start()
            rs_cp.append(cp)
        if t == ng // 2 - 1:
            for n, (source, target) in enumerate(((before, after), (after, before))):
                ty_cp[n].wait_recv()
                part_y = pl.ds(direct + source * per_y + n * (per_y // 2), per_y // 2)
                ty_cp.append(trans_share(part_y, 2 + n, target))
                ty_cp[-1].start()

    for cp in tot_cp:
        cp.wait_recv()
    for cp in rs_cp:
        cp.wait_recv()
    act_own = act_i[pl.ds(pl.multiple_of(g * own_rows, own_rows), own_rows), :]
    values = []
    for h in range(halves):
        total = tot_own[h]
        for t in range(ng - 1):
            total = total + tot_buf[t, h]
        raw = part[pl.ds(g * own_rows * halves + h, own_rows, stride=halves), :]
        for t in range(ng - 1):
            raw = raw + rs_buf[t, pl.ds(h, own_rows, stride=halves), :]
        divisor = jnp.ones((own_rows, LANES), jnp.float32)
        for a in range(actions):
            divisor = jnp.where(act_own == a, total[a : a + 1, :], divisor)
        values.append(raw / divisor)
    coded, level = to_codes(values)
    for h in range(halves):
        cols = slice(h * LANES, (h + 1) * LANES)
        w_all[g, :own_rows, cols] = coded[h]
        w_all[g, own_rows:, cols] = level

    w_cp = [
        pltpu.make_async_remote_copy(
            w_all.at[g], w_all.at[g], w_send.at[t], w_recv.at[t], device_id=to_g(t), device_id_type=MESH
        )
        for t in range(ng - 1)
    ]
    for cp in w_cp:
        cp.start()

    def spread_owner(j):
        rows = pl.ds(pl.multiple_of(j * own_rows, own_rows), own_rows)
        low_rows = pl.ds(pl.multiple_of(bel + j * own_rows, own_rows), own_rows)
        w_scale[rows, :] = jnp.broadcast_to(
            scale_of(w_all[j, own_rows : own_rows + 1, :]), (own_rows, width)
        )[:, :qwidth]
        act = act_b[rows, :]
        pieces = []
        for h in range(halves):
            q = w_all[j, :own_rows, h * LANES : (h + 1) * LANES].astype(jnp.int32)
            high = jnp.right_shift(q + 128, 8)
            low = q - jnp.left_shift(high, 8)
            pieces.append((high.astype(jnp.float32).astype(jnp.bfloat16), low.astype(jnp.float32).astype(jnp.bfloat16)))

        for a in range(actions):
            hot = act == jnp.asarray(a, jnp.bfloat16)
            for h in range(halves):
                high, low = pieces[h]
                cols = slice(a * width + h * LANES, a * width + (h + 1) * LANES)
                spread[rows, cols] = jnp.where(hot, high, jnp.zeros_like(high))
                spread[low_rows, cols] = jnp.where(hot, low, jnp.zeros_like(low))

    spread_owner(g)
    own_t.wait()
    for cp in t_cp:
        cp.wait_recv()
    for cp in ty_cp[2:]:
        cp.wait_recv()

    def total_action(a, carry):
        tt_own[pl.ds(a, 1), :] = jnp.sum(
            t_blk[a].astype(jnp.float32), axis=0, keepdims=True
        )
        return carry

    lax.fori_loop(0, actions, total_action, 0)
    tt_cp = [
        pltpu.make_async_remote_copy(
            tt_own, tt_buf.at[t], tt_send.at[t], tt_recv.at[t], device_id=to_z(t), device_id_type=MESH
        )
        for t in range(nz - 1)
    ]
    for cp in tt_cp:
        cp.start()

    for t in range(ng - 1):
        w_cp[t].wait_recv()
        spread_owner(g_from(t))
    both = jnp.dot(
        spread[...],
        t_blk[...].reshape(actions * width, qwidth),
        preferred_element_type=jnp.float32,
    )
    fut[...] = (256.0 * both[:bel] + both[bel:]) * w_scale[...]

    def send_future(j, t):
        rows = pl.ds(pl.multiple_of(j * z_rows, z_rows), z_rows)
        (coded,), level = to_codes([fut[rows, :]])
        fut_q[j, :z_rows, :] = coded
        for h in range(qwidth // LANES):
            fut_q[j, z_rows:, h * LANES : (h + 1) * LANES] = level
        cp = pltpu.make_async_remote_copy(
            fut_q.at[j],
            f_buf.at[t],
            f_send.at[t],
            f_recv.at[t],
            device_id={"obs_0": j},
            device_id_type=MESH,
        )
        cp.start()
        f_cp.append(cp)

    f_cp = []
    for t in far_first(nz):
        send_future(z_at(t), t)
    own_rew.wait()
    for cp in f_cp:
        cp.wait_recv()
    for cp in tt_cp:
        cp.wait_recv()
    z_start = pl.multiple_of(z * z_rows, z_rows)
    act_z = act_i[pl.ds(z_start, z_rows), :]
    for h in range(qwidth // LANES):
        cols = slice(h * LANES, (h + 1) * LANES)
        total = tt_own[:, cols]
        for t in range(nz - 1):
            total = total + tt_buf[t, :, cols]
        future = fut[pl.ds(z_start, z_rows), cols]
        for t in range(nz - 1):
            piece = f_buf[t, :z_rows, cols].astype(jnp.int32).astype(jnp.float32)
            future = future + piece * scale_of(f_buf[t, z_rows : z_rows + 1, cols])
        divisor = jnp.ones((z_rows, LANES), jnp.float32)
        reward = jnp.zeros((z_rows, LANES), jnp.float32)
        for a in range(actions):
            hot = act_z == a
            divisor = jnp.where(hot, total[a : a + 1, :], divisor)
            reward = jnp.where(hot, rew_v[a : a + 1, cols], reward)
        result = reward + DISCOUNT * (future / divisor)
        for n in range(ng):
            fin[n, :, cols] = result[n * last : (n + 1) * last, :]
    o_cp = [
        pltpu.make_async_remote_copy(
            fin.at[g_at(t)],
            out_ref.at[:, q_cols],
            o_send.at[t],
            o_recv.at[t],
            device_id=to_g(t),
            device_id_type=MESH,
        )
        for t in range(ng - 1)
    ]
    for cp in o_cp:
        cp.start()
    out_ref[:, q_cols] = fin[g]
    for cp in o_cp:
        cp.wait_recv()
    for cp in ob_cp + pk_cp + al_cp[0] + al_cp[1] + share_cp + ts_cp + ty_cp + t_cp + relay_cp + tot_cp + rs_cp + w_cp + f_cp + tt_cp + o_cp:
        cp.wait_send()


def body(dims, alpha_set, transitions, obs_weights, rewards, chosen_idx, chosen_action):
    ny, nz, nx, nc = dims
    ng = nx * nc
    actions, states = rewards.shape
    bel = chosen_action.shape[0]
    obs_local = obs_weights.shape[0]
    width = states // nz
    qwidth = states // ng
    halves = width // LANES
    count = alpha_set.shape[0] * ny
    f32, b16, i32 = jnp.float32, jnp.bfloat16, jnp.int32
    dma = pltpu.SemaphoreType.DMA
    vmem = pl.BlockSpec(memory_space=pltpu.VMEM)
    hbm = pl.BlockSpec(memory_space=pl.ANY)
    z_rows = bel // nz
    own_rows = bel // ng
    scratch = [
        pltpu.VMEM((ny, count // ny, width), b16),
        pltpu.VMEM((count * halves, LANES), f32),
        pltpu.VMEM((bel, LANES), i32),
        pltpu.VMEM((bel, LANES), b16),
        pltpu.VMEM((obs_local, actions, states), f32),
        pltpu.VMEM((nz, obs_local, actions, width), jnp.int16),
        pltpu.VMEM((nz, obs_local, actions, width), jnp.int16),
        pltpu.VMEM((nz * actions, obs_local * halves, LANES), f32),
        pltpu.VMEM((obs_local, 1, bel), i32),
        pltpu.VMEM((nz, obs_local, 1, bel), i32),
        [[pltpu.SMEM((1, bel), i32) for _ in range(obs_local)] for _ in range(nz)],
        pltpu.VMEM((bel * halves, LANES), f32),
        pltpu.VMEM((ng - 1, own_rows * halves, LANES), f32),
        pltpu.VMEM((halves, actions, LANES), f32),
        pltpu.VMEM((ng - 1, halves, actions, LANES), f32),
        pltpu.VMEM((ng, own_rows + 8, width), jnp.int16),
        pltpu.VMEM((actions, width, qwidth), b16),
        pltpu.VMEM((2 * bel, actions * width), b16),
        pltpu.VMEM((bel, qwidth), f32),
        pltpu.VMEM((bel, qwidth), f32),
        pltpu.VMEM((nz, z_rows + 8, qwidth), jnp.int16),
        pltpu.VMEM((nz - 1, z_rows + 8, qwidth), jnp.int16),
        pltpu.VMEM((actions, qwidth), f32),
        pltpu.VMEM((nz - 1, actions, qwidth), f32),
        pltpu.VMEM((actions, qwidth), f32),
        pltpu.VMEM((ng, bel // (nz * ng), qwidth), f32),
        dma((5 + nz * obs_local,)),
        dma((nz - 1,)),
        dma((nz - 1,)),
        dma((2, 2)),
        dma((2, 2)),
        dma((2,)),
        dma((2,)),
        dma((6,)),
        dma((6,)),
        dma((nz - 1,)),
        dma((nz - 1,)),
        dma((ng - 1,)),
        dma((ng - 1,)),
        dma((ng - 1,)),
        dma((ng - 1,)),
        dma((4,)),
        dma((4,)),
        dma((ng - 1,)),
        dma((ng - 1,)),
        dma((ng - 1,)),
        dma((ng - 1,)),
        dma((ng - 1,)),
        dma((ng - 1,)),
        dma((nz - 1,)),
        dma((nz - 1,)),
        dma((nz - 1,)),
        dma((nz - 1,)),
        dma((ng - 1,)),
        dma((ng - 1,)),
    ]
    return pl.pallas_call(
        functools.partial(kernel, dims),
        out_shape=jax.ShapeDtypeStruct((bel // (nz * ng), states), f32),
        in_specs=[
            pl.BlockSpec(memory_space=pltpu.SMEM),
            vmem,
            vmem,
            hbm,
            hbm,
            hbm,
            hbm,
        ],
        out_specs=vmem,
        scratch_shapes=scratch,
        compiler_params=pltpu.CompilerParams(
            collective_id=0, has_side_effects=True, vmem_limit_bytes=60 * 1024 * 1024
        ),
        name="backup",
    )(
        chosen_action,
        chosen_action.reshape(1, bel),
        jnp.transpose(chosen_idx, (1, 2, 0)),
        alpha_set,
        transitions,
        obs_weights,
        rewards,
    )


def solution(mesh):
    dims = (mesh.shape["bel"], 8, 4, 2)
    torus = Mesh(
        mesh.devices.reshape(*dims[1:], dims[0]), ("obs_0", "obs_1", "obs_2", "bel")
    )
    return jax.shard_map(
        functools.partial(body, dims),
        mesh=torus,
        in_specs=(
            P("bel", None),
            P(None, OBS, None),
            P(OBS, None, None),
            P(),
            P("bel", None, OBS),
            P("bel"),
        ),
        out_specs=P(BEL_OBS, None),
        check_vma=False,
    )
```

```python
import functools

import jax
import jax.numpy as jnp
from jax import lax
from jax.experimental import pallas as pl
from jax.experimental.pallas import tpu as pltpu
from jax.sharding import Mesh
from jax.sharding import PartitionSpec as P

OBS = ("obs_0", "obs_1", "obs_2")
BEL_OBS = ("bel", "obs_0", "obs_1", "obs_2")
LANES = 128
DISCOUNT = 0.95
CODE_SCALE = 14114.0
CODE_SHIFT = 2.302585093 * CODE_SCALE
MESH = pl.DeviceIdType.MESH


def to_codes(values):
    largest = functools.reduce(
        jnp.maximum, [jnp.max(jnp.abs(v), axis=(0, 1), keepdims=True) for v in values]
    )
    level = jnp.ceil(32.0 * jnp.log(jnp.maximum(largest, 1e-30) * (1.0 / 32760.0)))
    inverse = jnp.exp(level * (-1.0 / 32.0))
    coded = [
        jnp.clip(jnp.round(v * inverse), -32767.0, 32767.0).astype(jnp.int32)
        for v in values
    ]
    return coded, jnp.broadcast_to(level, (8, LANES)).astype(jnp.int32)


def scale_of(level):
    return jnp.exp(level * (1.0 / 32.0))


def far_first(n):
    return sorted(range(n - 1), key=lambda t: -min(t + 1, n - 1 - t))


def group_offsets(nx, nc):
    steps = [(dx, dc) for dx in range(nx) for dc in range(nc) if dx or dc]
    return sorted(steps, key=lambda step: -min(step[0], nx - step[0]))


def kernel(
    dims,
    act_s,
    act_row,
    idx_ref,
    alpha_hbm,
    trans_hbm,
    obs_hbm,
    rew_hbm,
    out_ref,
    rew_ref,
    al_bf,
    al_rows,
    act_i,
    act_b,
    obs_v,
    obs_code,
    obs_all,
    obs_rows,
    pk_own,
    pk_v,
    pk_s,
    part,
    rs_buf,
    tot_own,
    tot_buf,
    w_all,
    t_blk,
    spread,
    w_scale,
    fut,
    fut_q,
    f_buf,
    tt_own,
    tt_buf,
    rew_v,
    tt_all,
    local_sem,
    pk_send,
    pk_recv,
    al_send,
    al_recv,
    relay_send,
    relay_recv,
    share_send,
    share_recv,
    ob_send,
    ob_recv,
    t_send,
    t_recv,
    ts_send,
    ts_recv,
    ty_send,
    ty_recv,
    tot_send,
    tot_recv,
    rs_send,
    rs_recv,
    w_send,
    w_recv,
    f_send,
    f_recv,
    tt_send,
    tt_recv,
):
    ny, nz, nx, nc = dims
    ng = nx * nc
    actions = t_blk.shape[0]
    width = t_blk.shape[1]
    qwidth = t_blk.shape[2]
    halves = width // LANES
    bel = fut.shape[0]
    own_rows = bel // ng
    z_rows = bel // nz
    rows_y = alpha_hbm.shape[0]
    half_y = rows_y // nc
    obs_local = obs_hbm.shape[0]
    t_rows = trans_hbm.shape[1]
    last = out_ref.shape[0]
    per_y = actions // (2 * ny)
    direct = actions - per_y * ny

    y = lax.axis_index("bel")
    z = lax.axis_index("obs_0")
    x = lax.axis_index("obs_1")
    c = lax.axis_index("obs_2")
    g = x * nc + c

    def y_at(t):
        return lax.rem(y + 1 + t, ny)

    def z_at(t):
        return lax.rem(z + 1 + t, nz)

    offsets = group_offsets(nx, nc)

    def g_at(t):
        dx, dc = offsets[t]
        return lax.rem(x + dx, nx) * nc + lax.rem(c + dc, nc)

    def g_from(t):
        dx, dc = offsets[t]
        return lax.rem(x + nx - dx, nx) * nc + lax.rem(c + nc - dc, nc)

    def to_y(t):
        return {"bel": y_at(t)}

    def to_z(t):
        return {"obs_0": z_at(t)}

    def to_g(t):
        j = g_at(t)
        return {"obs_1": j // nc, "obs_2": lax.rem(j, nc)}

    peers = (
        [to_y(t) for t in range(ny - 1)]
        + [to_z(t) for t in range(nz - 1)]
        + [to_g(t) for t in range(ng - 1)]
    )
    barrier = pltpu.get_barrier_semaphore()
    for peer in peers:
        pl.semaphore_signal(barrier, inc=1, device_id=peer, device_id_type=MESH)

    z_cols = pl.ds(pl.multiple_of(z * width, width), width)
    q_cols = pl.ds(pl.multiple_of(g * qwidth, qwidth), qwidth)

    own_al = pltpu.make_async_copy(alpha_hbm.at[:, z_cols], al_bf.at[y], local_sem.at[1])
    own_ob = pltpu.make_async_copy(obs_hbm, obs_v, local_sem.at[2])
    g_rows = pl.ds(pl.multiple_of(g * t_rows, t_rows), t_rows)
    mine = pl.ds(direct + y * per_y, per_y)
    own_t = pltpu.make_async_copy(
        trans_hbm.at[:direct, :, q_cols], t_blk.at[:direct, g_rows, :], local_sem.at[3]
    )
    own_ts = pltpu.make_async_copy(
        trans_hbm.at[mine, :, q_cols], t_blk.at[mine, g_rows, :], local_sem.at[0]
    )
    own_rew = pltpu.make_async_copy(rew_hbm, rew_v, local_sem.at[4])
    own_ob.start()
    own_al.start()
    own_t.start()
    own_ts.start()
    own_rew.start()

    picks = jnp.zeros((obs_local, bel), jnp.int32)
    for a in range(actions):
        picks = jnp.where(act_row[...] == a, idx_ref[a] * halves, picks)
    for o in range(obs_local):
        pk_own[o] = picks[o : o + 1, :]
        pk_v[z, o] = picks[o : o + 1, :]

    def fill_action(b, carry):
        act_i[pl.ds(b, 1), :] = jnp.full((1, LANES), act_s[b], jnp.int32)
        return carry

    lax.fori_loop(0, bel, fill_action, 0, unroll=8)
    act_b[...] = act_i[...].astype(jnp.float32).astype(jnp.bfloat16)
    own_ob.wait()
    for n in range(nz):
        for o in range(obs_local):
            v = jnp.log(obs_v[o, :, n * width : (n + 1) * width])
            obs_code[n, o] = jnp.round(v * CODE_SCALE + CODE_SHIFT).astype(jnp.int32).astype(jnp.int16)
    pl.semaphore_wait(barrier, len(peers))

    quarter = half_y // 2
    quarters = [pl.ds(pl.multiple_of(c * half_y + n * quarter, quarter), quarter) for n in range(2)]
    pk_cp = [
        pltpu.make_async_remote_copy(
            pk_own,
            pk_v.at[z],
            pk_send.at[t],
            pk_recv.at[t],
            device_id=to_z(t),
            device_id_type=MESH,
        )
        for t in range(nz - 1)
    ]
    al_cp = [
        [
            pltpu.make_async_remote_copy(
                al_bf.at[y, quarters[n]],
                al_bf.at[y, quarters[n]],
                al_send.at[t, m],
                al_recv.at[t, m],
                device_id={"bel": lax.rem(y + step, ny)},
                device_id_type=MESH,
            )
            for m, n in enumerate((t, 1 - t))
        ]
        for t, step in ((0, 1), (1, ny - 1))
    ]
    ob_cp = [
        pltpu.make_async_remote_copy(
            obs_code.at[z_at(t)],
            obs_all.at[z],
            ob_send.at[t],
            ob_recv.at[t],
            device_id=to_z(t),
            device_id_type=MESH,
        )
        for t in range(nz - 1)
    ]
    def trans_copy(t, which, send, recv):
        return pltpu.make_async_remote_copy(
            trans_hbm.at[which, :, pl.ds(pl.multiple_of(g_at(t) * qwidth, qwidth), qwidth)],
            t_blk.at[which, g_rows, :],
            send.at[t],
            recv.at[t],
            device_id=to_g(t),
            device_id_type=MESH,
        )

    ts_cp = [trans_copy(t, mine, ts_send, ts_recv) for t in range(ng - 1)]
    t_cp = [trans_copy(t, pl.ds(0, direct), t_send, t_recv) for t in range(ng - 1)]
    for cp in pk_cp:
        cp.start()
    own_al.wait()
    for m in range(2):
        for pair in al_cp:
            pair[m].start()
    for t in far_first(nz):
        ob_cp[t].start()
    for cp in ts_cp:
        cp.start()
    for cp in t_cp:
        cp.start()

    def spread_alpha(block, start, rows):
        def rows16(n, carry):
            r = pl.multiple_of(start + n * 16, 16)
            v = al_bf[block, pl.ds(r, 16), :].astype(jnp.float32)
            for h in range(halves):
                al_rows[pl.ds((block * rows_y + r) * halves + h, 16, stride=halves), :] = v[
                    :, h * LANES : (h + 1) * LANES
                ]
            return carry

        lax.fori_loop(0, rows // 16, rows16, 0, unroll=4)

    spread_alpha(y, 0, rows_y)

    for cp in pk_cp:
        cp.wait_recv()
    to_scalar = [
        [
            pltpu.make_async_copy(pk_v.at[n, o], pk_s[n][o], local_sem.at[5 + n * obs_local + o])
            for o in range(obs_local)
        ]
        for n in range(nz)
    ]
    for pair in to_scalar:
        for cp in pair:
            cp.start()

    totals = [jnp.zeros((actions, LANES), jnp.float32) for _ in range(halves)]

    def decode(code_ref, slot):
        for o in range(obs_local):
            v = jnp.exp(
                code_ref[slot, o].astype(jnp.int32).astype(jnp.float32) * (1.0 / CODE_SCALE)
            )
            for h in range(halves):
                part_h = v[:, h * LANES : (h + 1) * LANES]
                totals[h] = totals[h] + part_h
                obs_rows[pl.ds(slot * actions, actions), o * halves + h, :] = part_h

    decode(obs_code, z)
    share_cp = []

    def share(block, rows):
        cp = pltpu.make_async_remote_copy(
            al_bf.at[block, rows],
            al_bf.at[block, rows],
            share_send.at[len(share_cp)],
            share_recv.at[len(share_cp)],
            device_id={"obs_2": 1 - c},
            device_id_type=MESH,
        )
        cp.start()
        share_cp.append(cp)

    before, after, across = (lax.rem(y + n, ny) for n in (ny - 1, 1, ny - 2))
    relay_cp = []
    for t, (source, target) in enumerate(((before, after), (after, before))):
        al_cp[t][0].wait_recv()
        cp = pltpu.make_async_remote_copy(
            al_bf.at[source, quarters[t]],
            al_bf.at[source, quarters[t]],
            relay_send.at[t],
            relay_recv.at[t],
            device_id={"bel": target},
            device_id_type=MESH,
        )
        cp.start()
        relay_cp.append(cp)
    for t, source in enumerate((before, after)):
        share(source, quarters[t])
    for t, source in enumerate((before, after)):
        al_cp[t][1].wait_recv()
        share(source, quarters[1 - t])
    for source in (before, after):
        spread_alpha(source, c * half_y, half_y)
    for t in range(2):
        relay_cp[t].wait_recv()
        share(across, quarters[t])
    spread_alpha(across, c * half_y, half_y)
    for t in far_first(nz):
        ob_cp[t].wait_recv()
        decode(obs_all, lax.rem(z + nz - 1 - t, nz))
    for h in range(halves):
        tot_own[h] = totals[h]
    tot_cp = [
        pltpu.make_async_remote_copy(
            tot_own, tot_buf.at[t], tot_send.at[t], tot_recv.at[t], device_id=to_g(t), device_id_type=MESH
        )
        for t in range(ng - 1)
    ]
    for cp in tot_cp:
        cp.start()

    own_ts.wait()
    for cp in ts_cp:
        cp.wait_recv()

    def trans_share(which, n, target):
        return pltpu.make_async_remote_copy(
            t_blk.at[which],
            t_blk.at[which],
            ty_send.at[n],
            ty_recv.at[n],
            device_id={"bel": target},
            device_id_type=MESH,
        )

    ty_cp = [trans_share(mine, 0, after), trans_share(mine, 1, before)]
    for cp in ty_cp:
        cp.start()
    other = (1 - c) * half_y
    for cp, (source, n) in zip(
        share_cp, ((before, 0), (after, 1), (before, 1), (after, 0), (across, 0), (across, 1))
    ):
        cp.wait_recv()
        spread_alpha(source, other + n * quarter, quarter)
    for pair in to_scalar:
        for cp in pair:
            cp.wait()
    rs_cp = []
    for t in range(ng):
        j = g_at(t) if t < ng - 1 else g

        def one_belief(r, carry):
            b = j * own_rows + r
            a = act_s[b]
            sums = [None] * 4
            for n in range(nz):
                probs = obs_rows[n * actions + a]
                for o in range(obs_local):
                    term = al_rows[pl.ds(pk_s[n][o][0, b], halves), :] * probs[o * halves : (o + 1) * halves]
                    sums[o % 4] = term if n == 0 else sums[o % 4] + term
            part[pl.ds(pl.multiple_of(b * halves, halves), halves), :] = (sums[0] + sums[1]) + (
                sums[2] + sums[3]
            )
            return carry

        lax.fori_loop(0, own_rows, one_belief, 0, unroll=4)
        if t < ng - 1:
            rows = own_rows * halves
            cp = pltpu.make_async_remote_copy(
                part.at[pl.ds(pl.multiple_of(j * rows, rows), rows), :],
                rs_buf.at[t],
                rs_send.at[t],
                rs_recv.at[t],
                device_id=to_g(t),
                device_id_type=MESH,
            )
            cp.start()
            rs_cp.append(cp)
        if t == ng // 2 - 1:
            for n, (source, target) in enumerate(((before, after), (after, before))):
                ty_cp[n].wait_recv()
                part_y = pl.ds(direct + source * per_y + n * (per_y // 2), per_y // 2)
                ty_cp.append(trans_share(part_y, 2 + n, target))
                ty_cp[-1].start()

    for cp in tot_cp:
        cp.wait_recv()
    for cp in rs_cp:
        cp.wait_recv()
    act_own = act_i[pl.ds(pl.multiple_of(g * own_rows, own_rows), own_rows), :]
    values = []
    for h in range(halves):
        total = tot_own[h]
        for t in range(ng - 1):
            total = total + tot_buf[t, h]
        raw = part[pl.ds(g * own_rows * halves + h, own_rows, stride=halves), :]
        for t in range(ng - 1):
            raw = raw + rs_buf[t, pl.ds(h, own_rows, stride=halves), :]
        divisor = jnp.ones((own_rows, LANES), jnp.float32)
        for a in range(actions):
            divisor = jnp.where(act_own == a, total[a : a + 1, :], divisor)
        values.append(raw / divisor)
    coded, level = to_codes(values)
    for h in range(halves):
        cols = slice(h * LANES, (h + 1) * LANES)
        w_all[g, :own_rows, cols] = coded[h].astype(jnp.int16)
        w_all[g, own_rows:, cols] = level.astype(jnp.int16)

    w_cp = [
        pltpu.make_async_remote_copy(
            w_all.at[g], w_all.at[g], w_send.at[t], w_recv.at[t], device_id=to_g(t), device_id_type=MESH
        )
        for t in range(ng - 1)
    ]
    for cp in w_cp:
        cp.start()

    def spread_owner(j):
        rows = pl.ds(pl.multiple_of(j * own_rows, own_rows), own_rows)
        low_rows = pl.ds(pl.multiple_of(bel + j * own_rows, own_rows), own_rows)
        w_scale[rows, :] = jnp.broadcast_to(
            scale_of(w_all[j, own_rows : own_rows + 1, :].astype(jnp.int32).astype(jnp.float32)), (own_rows, width)
        )[:, :qwidth]
        act = act_b[rows, :]
        pieces = []
        for h in range(halves):
            q = w_all[j, :own_rows, h * LANES : (h + 1) * LANES].astype(jnp.int32)
            high = jnp.right_shift(q + 128, 8)
            low = q - jnp.left_shift(high, 8)
            pieces.append((high.astype(jnp.float32).astype(jnp.bfloat16), low.astype(jnp.float32).astype(jnp.bfloat16)))

        for a in range(actions):
            hot = act == jnp.asarray(a, jnp.bfloat16)
            for h in range(halves):
                high, low = pieces[h]
                cols = slice(a * width + h * LANES, a * width + (h + 1) * LANES)
                spread[rows, cols] = jnp.where(hot, high, jnp.zeros_like(high))
                spread[low_rows, cols] = jnp.where(hot, low, jnp.zeros_like(low))

    spread_owner(g)
    own_t.wait()
    for cp in t_cp:
        cp.wait_recv()
    for cp in ty_cp[2:]:
        cp.wait_recv()

    def total_action(a, carry):
        tt_own[pl.ds(a, 1), :] = jnp.sum(
            t_blk[a].astype(jnp.float32), axis=0, keepdims=True
        )
        return carry

    lax.fori_loop(0, actions, total_action, 0)
    tt_cp = [
        pltpu.make_async_remote_copy(
            tt_own, tt_buf.at[t], tt_send.at[t], tt_recv.at[t], device_id=to_z(t), device_id_type=MESH
        )
        for t in range(nz - 1)
    ]
    for cp in tt_cp:
        cp.start()

    for t in range(ng - 1):
        w_cp[t].wait_recv()
        spread_owner(g_from(t))
    both = jnp.dot(
        spread[...],
        t_blk[...].reshape(actions * width, qwidth),
        preferred_element_type=jnp.float32,
    )
    fut[...] = (256.0 * both[:bel] + both[bel:]) * w_scale[...]

    def send_future(j, t):
        rows = pl.ds(pl.multiple_of(j * z_rows, z_rows), z_rows)
        act = act_i[rows, :]
        values = []
        for h in range(qwidth // LANES):
            cols = slice(h * LANES, (h + 1) * LANES)
            divisor = jnp.ones((z_rows, LANES), jnp.float32)
            for a in range(actions):
                divisor = jnp.where(act == a, tt_all[a : a + 1, cols], divisor)
            values.append(fut[rows, cols] / divisor)
        coded, level = to_codes(values)
        for h, code in enumerate(coded):
            cols = slice(h * LANES, (h + 1) * LANES)
            for n in range(ng):
                piece = jnp.concatenate([code[n * last : (n + 1) * last], level[: 8 - last]], axis=0)
                fut_q[t + 1, n, :, cols] = piece.astype(jnp.int16)
        for u in range(-1, ng - 1):
            if t < 0 and u < 0:
                continue
            n = g if u < 0 else g_at(u)
            cp = pltpu.make_async_remote_copy(
                fut_q.at[t + 1, n],
                f_buf.at[t + 1, u + 1],
                f_send.at[t + 1, u + 1],
                f_recv.at[t + 1, u + 1],
                device_id={"obs_0": j, "obs_1": n // nc, "obs_2": lax.rem(n, nc)},
                device_id_type=MESH,
            )
            cp.start()
            f_cp.append(cp)

    for cp in tt_cp:
        cp.wait_recv()
    total = tt_own[...]
    for t in range(nz - 1):
        total = total + tt_buf[t]
    tt_all[...] = total
    f_cp = []
    for t in far_first(nz):
        send_future(z_at(t), t)
    send_future(z, -1)
    own_rew.wait()
    for r in range(last):
        rew_ref[r : r + 1, :] = rew_v[pl.ds(act_s[(z * ng + g) * last + r], 1), :]
    for cp in f_cp:
        cp.wait_recv()

    def add_pieces(u, at, read):
        for h in range(qwidth // LANES):
            cols = slice(h * LANES, (h + 1) * LANES)
            future = None
            for t in range(nz):
                piece = read(t, cols)
                term = piece * scale_of(piece[last : last + 1])
                future = term if future is None else future + term
            out_ref[:, pl.ds(pl.multiple_of(at * qwidth + h * LANES, LANES), LANES)] = future[:last]

    for u in range(ng):
        def read(t, cols):
            piece = fut_q[0, g, :, cols] if u == 0 and t == 0 else f_buf[t, u, :, cols]
            return piece.astype(jnp.int32).astype(jnp.float32)

        add_pieces(u, g if u == 0 else g_from(u - 1), read)
    for cp in ob_cp + pk_cp + al_cp[0] + al_cp[1] + share_cp + ts_cp + ty_cp + t_cp + relay_cp + tot_cp + rs_cp + w_cp + f_cp + tt_cp:
        cp.wait_send()


def body(dims, alpha_set, transitions, obs_weights, rewards, chosen_idx, chosen_action):
    ny, nz, nx, nc = dims
    ng = nx * nc
    actions, states = rewards.shape
    bel = chosen_action.shape[0]
    obs_local = obs_weights.shape[0]
    width = states // nz
    qwidth = states // ng
    halves = width // LANES
    count = alpha_set.shape[0] * ny
    f32, b16, i32 = jnp.float32, jnp.bfloat16, jnp.int32
    dma = pltpu.SemaphoreType.DMA
    vmem = pl.BlockSpec(memory_space=pltpu.VMEM)
    hbm = pl.BlockSpec(memory_space=pl.ANY)
    z_rows = bel // nz
    own_rows = bel // ng
    scratch = [
        pltpu.VMEM((ny, count // ny, width), b16),
        pltpu.VMEM((count * halves, LANES), f32),
        pltpu.VMEM((bel, LANES), i32),
        pltpu.VMEM((bel, LANES), b16),
        pltpu.VMEM((obs_local, actions, states), f32),
        pltpu.VMEM((nz, obs_local, actions, width), jnp.int16),
        pltpu.VMEM((nz, obs_local, actions, width), jnp.int16),
        pltpu.VMEM((nz * actions, obs_local * halves, LANES), f32),
        pltpu.VMEM((obs_local, 1, bel), i32),
        pltpu.VMEM((nz, obs_local, 1, bel), i32),
        [[pltpu.SMEM((1, bel), i32) for _ in range(obs_local)] for _ in range(nz)],
        pltpu.VMEM((bel * halves, LANES), f32),
        pltpu.VMEM((ng - 1, own_rows * halves, LANES), f32),
        pltpu.VMEM((halves, actions, LANES), f32),
        pltpu.VMEM((ng - 1, halves, actions, LANES), f32),
        pltpu.VMEM((ng, own_rows + 8, width), jnp.int16),
        pltpu.VMEM((actions, width, qwidth), b16),
        pltpu.VMEM((2 * bel, actions * width), b16),
        pltpu.VMEM((bel, qwidth), f32),
        pltpu.VMEM((bel, qwidth), f32),
        pltpu.VMEM((nz, ng, 8, qwidth), jnp.int16),
        pltpu.VMEM((nz, ng, 8, qwidth), jnp.int16),
        pltpu.VMEM((actions, qwidth), f32),
        pltpu.VMEM((nz - 1, actions, qwidth), f32),
        pltpu.VMEM((actions, states), f32),
        pltpu.VMEM((actions, qwidth), f32),
        dma((5 + nz * obs_local,)),
        dma((nz - 1,)),
        dma((nz - 1,)),
        dma((2, 2)),
        dma((2, 2)),
        dma((2,)),
        dma((2,)),
        dma((6,)),
        dma((6,)),
        dma((nz - 1,)),
        dma((nz - 1,)),
        dma((ng - 1,)),
        dma((ng - 1,)),
        dma((ng - 1,)),
        dma((ng - 1,)),
        dma((4,)),
        dma((4,)),
        dma((ng - 1,)),
        dma((ng - 1,)),
        dma((ng - 1,)),
        dma((ng - 1,)),
        dma((ng - 1,)),
        dma((ng - 1,)),
        dma((nz, ng)),
        dma((nz, ng)),
        dma((nz - 1,)),
        dma((nz - 1,)),
    ]
    rows = jax.ShapeDtypeStruct((bel // (nz * ng), states), f32)
    future, reward = pl.pallas_call(
        functools.partial(kernel, dims),
        out_shape=(rows, rows),
        in_specs=[
            pl.BlockSpec(memory_space=pltpu.SMEM),
            vmem,
            vmem,
            hbm,
            hbm,
            hbm,
            hbm,
        ],
        out_specs=(vmem, vmem),
        scratch_shapes=scratch,
        compiler_params=pltpu.CompilerParams(
            collective_id=0, has_side_effects=True, vmem_limit_bytes=60 * 1024 * 1024
        ),
        name="backup",
    )(
        chosen_action,
        chosen_action.reshape(1, bel),
        jnp.transpose(chosen_idx, (1, 2, 0)),
        alpha_set,
        transitions,
        obs_weights,
        rewards,
    )
    return reward + DISCOUNT * future


def solution(mesh):
    dims = (mesh.shape["bel"], 8, 4, 2)
    torus = Mesh(
        mesh.devices.reshape(*dims[1:], dims[0]), ("obs_0", "obs_1", "obs_2", "bel")
    )
    return jax.shard_map(
        functools.partial(body, dims),
        mesh=torus,
        in_specs=(
            P("bel", None),
            P(None, OBS, None),
            P(OBS, None, None),
            P(),
            P("bel", None, OBS),
            P("bel"),
        ),
        out_specs=P(BEL_OBS, None),
        check_vma=False,
    )
```

```python
import functools

import jax
import jax.numpy as jnp
from jax import lax
from jax.experimental import pallas as pl
from jax.experimental.pallas import tpu as pltpu
from jax.sharding import Mesh
from jax.sharding import PartitionSpec as P

OBS = ("obs_0", "obs_1", "obs_2")
BEL_OBS = ("bel", "obs_0", "obs_1", "obs_2")
LANES = 128
PIECE = 16
DISCOUNT = 0.95
CODE_SCALE = 14114.0
CODE_SHIFT = 2.302585093 * CODE_SCALE
MESH = pl.DeviceIdType.MESH


def to_codes(values):
    largest = functools.reduce(
        jnp.maximum, [jnp.max(jnp.abs(v), axis=(0, 1), keepdims=True) for v in values]
    )
    level = jnp.ceil(32.0 * jnp.log(jnp.maximum(largest, 1e-30) * (1.0 / 32760.0)))
    inverse = jnp.exp(level * (-1.0 / 32.0))
    coded = [
        jnp.clip(jnp.round(v * inverse), -32767.0, 32767.0).astype(jnp.int32)
        for v in values
    ]
    return coded, jnp.broadcast_to(level, (8, LANES)).astype(jnp.int32)


def scale_of(level):
    return jnp.exp(level * (1.0 / 32.0))


def far_first(n):
    return sorted(range(n - 1), key=lambda t: -min(t + 1, n - 1 - t))


def group_offsets(nx, nc):
    steps = [(dx, dc) for dx in range(nx) for dc in range(nc) if dx or dc]
    return sorted(steps, key=lambda step: -min(step[0], nx - step[0]))


def kernel(
    dims,
    act_s,
    act_row,
    idx_ref,
    alpha_hbm,
    trans_hbm,
    obs_hbm,
    rew_hbm,
    out_ref,
    rew_ref,
    al_bf,
    al_rows,
    act_i,
    act_b,
    obs_v,
    obs_code,
    obs_all,
    obs_rows,
    pk_own,
    pk_v,
    pk_s,
    part,
    rs_buf,
    tot_own,
    tot_buf,
    w_all,
    t_blk,
    spread,
    w_scale,
    fut,
    fut_q,
    f_buf,
    tt_own,
    tt_buf,
    rew_v,
    tt_all,
    local_sem,
    pk_send,
    pk_recv,
    al_send,
    al_recv,
    relay_send,
    relay_recv,
    share_send,
    share_recv,
    ob_send,
    ob_recv,
    t_send,
    t_recv,
    ts_send,
    ts_recv,
    ty_send,
    ty_recv,
    tot_send,
    tot_recv,
    rs_send,
    rs_recv,
    w_send,
    w_recv,
    f_send,
    f_recv,
    tt_send,
    tt_recv,
):
    ny, nz, nx, nc = dims
    ng = nx * nc
    actions = t_blk.shape[0]
    width = t_blk.shape[1]
    qwidth = t_blk.shape[2]
    halves = width // LANES
    bel = fut.shape[0]
    own_rows = bel // ng
    z_rows = bel // nz
    rows_y = alpha_hbm.shape[0]
    half_y = rows_y // nc
    obs_local = obs_hbm.shape[0]
    t_rows = trans_hbm.shape[1]
    last = out_ref.shape[0]
    used = last * (qwidth // LANES)
    per_y = actions // (2 * ny)
    direct = actions - per_y * ny

    y = lax.axis_index("bel")
    z = lax.axis_index("obs_0")
    x = lax.axis_index("obs_1")
    c = lax.axis_index("obs_2")
    g = x * nc + c

    def y_at(t):
        return lax.rem(y + 1 + t, ny)

    def z_at(t):
        return lax.rem(z + 1 + t, nz)

    offsets = group_offsets(nx, nc)

    def g_at(t):
        dx, dc = offsets[t]
        return lax.rem(x + dx, nx) * nc + lax.rem(c + dc, nc)

    def g_from(t):
        dx, dc = offsets[t]
        return lax.rem(x + nx - dx, nx) * nc + lax.rem(c + nc - dc, nc)

    def to_y(t):
        return {"bel": y_at(t)}

    def to_z(t):
        return {"obs_0": z_at(t)}

    def to_g(t):
        j = g_at(t)
        return {"obs_1": j // nc, "obs_2": lax.rem(j, nc)}

    peers = (
        [to_y(t) for t in range(ny - 1)]
        + [to_z(t) for t in range(nz - 1)]
        + [to_g(t) for t in range(ng - 1)]
    )
    barrier = pltpu.get_barrier_semaphore()
    for peer in peers:
        pl.semaphore_signal(barrier, inc=1, device_id=peer, device_id_type=MESH)

    z_cols = pl.ds(pl.multiple_of(z * width, width), width)
    q_cols = pl.ds(pl.multiple_of(g * qwidth, qwidth), qwidth)

    own_al = pltpu.make_async_copy(alpha_hbm.at[:, z_cols], al_bf.at[y], local_sem.at[1])
    own_ob = pltpu.make_async_copy(obs_hbm, obs_v, local_sem.at[2])
    g_rows = pl.ds(pl.multiple_of(g * t_rows, t_rows), t_rows)
    mine = pl.ds(direct + y * per_y, per_y)
    own_t = pltpu.make_async_copy(
        trans_hbm.at[:direct, :, q_cols], t_blk.at[:direct, g_rows, :], local_sem.at[3]
    )
    own_ts = pltpu.make_async_copy(
        trans_hbm.at[mine, :, q_cols], t_blk.at[mine, g_rows, :], local_sem.at[0]
    )
    own_rew = pltpu.make_async_copy(rew_hbm, rew_v, local_sem.at[4])
    own_ob.start()
    own_al.start()
    own_t.start()
    own_ts.start()
    own_rew.start()

    picks = jnp.zeros((obs_local, bel), jnp.int32)
    for a in range(actions):
        picks = jnp.where(act_row[...] == a, idx_ref[a] * halves, picks)
    for o in range(obs_local):
        pk_own[o] = picks[o : o + 1, :]
        pk_v[z, o] = picks[o : o + 1, :]

    def fill_action(b, carry):
        act_i[pl.ds(b, 1), :] = jnp.full((1, LANES), act_s[b], jnp.int32)
        return carry

    lax.fori_loop(0, bel, fill_action, 0, unroll=8)
    act_b[...] = act_i[...].astype(jnp.float32).astype(jnp.bfloat16)
    own_ob.wait()
    for n in range(nz):
        for o in range(obs_local):
            v = jnp.log(obs_v[o, :, n * width : (n + 1) * width])
            obs_code[n, o] = jnp.round(v * CODE_SCALE + CODE_SHIFT).astype(jnp.int32).astype(jnp.int16)
    pl.semaphore_wait(barrier, len(peers))

    quarter = half_y // 2
    quarters = [pl.ds(pl.multiple_of(c * half_y + n * quarter, quarter), quarter) for n in range(2)]
    pk_cp = [
        pltpu.make_async_remote_copy(
            pk_own,
            pk_v.at[z],
            pk_send.at[t],
            pk_recv.at[t],
            device_id=to_z(t),
            device_id_type=MESH,
        )
        for t in range(nz - 1)
    ]
    al_cp = [
        [
            pltpu.make_async_remote_copy(
                al_bf.at[y, quarters[n]],
                al_bf.at[y, quarters[n]],
                al_send.at[t, m],
                al_recv.at[t, m],
                device_id={"bel": lax.rem(y + step, ny)},
                device_id_type=MESH,
            )
            for m, n in enumerate((t, 1 - t))
        ]
        for t, step in ((0, 1), (1, ny - 1))
    ]
    ob_cp = [
        pltpu.make_async_remote_copy(
            obs_code.at[z_at(t)],
            obs_all.at[z],
            ob_send.at[t],
            ob_recv.at[t],
            device_id=to_z(t),
            device_id_type=MESH,
        )
        for t in range(nz - 1)
    ]
    def trans_copy(t, which, send, recv):
        return pltpu.make_async_remote_copy(
            trans_hbm.at[which, :, pl.ds(pl.multiple_of(g_at(t) * qwidth, qwidth), qwidth)],
            t_blk.at[which, g_rows, :],
            send.at[t],
            recv.at[t],
            device_id=to_g(t),
            device_id_type=MESH,
        )

    ts_cp = [trans_copy(t, mine, ts_send, ts_recv) for t in range(ng - 1)]
    t_cp = [trans_copy(t, pl.ds(0, direct), t_send, t_recv) for t in range(ng - 1)]
    for cp in pk_cp:
        cp.start()
    own_al.wait()
    for m in range(2):
        for pair in al_cp:
            pair[m].start()
    for t in far_first(nz):
        ob_cp[t].start()
    for cp in ts_cp:
        cp.start()
    for cp in t_cp:
        cp.start()

    def spread_alpha(block, start, rows):
        def rows16(n, carry):
            r = pl.multiple_of(start + n * 16, 16)
            v = al_bf[block, pl.ds(r, 16), :].astype(jnp.float32)
            for h in range(halves):
                al_rows[pl.ds((block * rows_y + r) * halves + h, 16, stride=halves), :] = v[
                    :, h * LANES : (h + 1) * LANES
                ]
            return carry

        lax.fori_loop(0, rows // 16, rows16, 0, unroll=4)

    spread_alpha(y, 0, rows_y)

    for cp in pk_cp:
        cp.wait_recv()
    to_scalar = [
        [
            pltpu.make_async_copy(pk_v.at[n, o], pk_s[n][o], local_sem.at[5 + n * obs_local + o])
            for o in range(obs_local)
        ]
        for n in range(nz)
    ]
    for pair in to_scalar:
        for cp in pair:
            cp.start()

    totals = [jnp.zeros((actions, LANES), jnp.float32) for _ in range(halves)]

    def decode(code_ref, slot):
        for o in range(obs_local):
            v = jnp.exp(
                code_ref[slot, o].astype(jnp.int32).astype(jnp.float32) * (1.0 / CODE_SCALE)
            )
            for h in range(halves):
                part_h = v[:, h * LANES : (h + 1) * LANES]
                totals[h] = totals[h] + part_h
                obs_rows[pl.ds(slot * actions, actions), o * halves + h, :] = part_h

    decode(obs_code, z)
    share_cp = []

    def share(block, rows):
        cp = pltpu.make_async_remote_copy(
            al_bf.at[block, rows],
            al_bf.at[block, rows],
            share_send.at[len(share_cp)],
            share_recv.at[len(share_cp)],
            device_id={"obs_2": 1 - c},
            device_id_type=MESH,
        )
        cp.start()
        share_cp.append(cp)

    before, after, across = (lax.rem(y + n, ny) for n in (ny - 1, 1, ny - 2))
    relay_cp = []
    for t, (source, target) in enumerate(((before, after), (after, before))):
        al_cp[t][0].wait_recv()
        cp = pltpu.make_async_remote_copy(
            al_bf.at[source, quarters[t]],
            al_bf.at[source, quarters[t]],
            relay_send.at[t],
            relay_recv.at[t],
            device_id={"bel": target},
            device_id_type=MESH,
        )
        cp.start()
        relay_cp.append(cp)
    for t, source in enumerate((before, after)):
        share(source, quarters[t])
    for t, source in enumerate((before, after)):
        al_cp[t][1].wait_recv()
        share(source, quarters[1 - t])
    for source in (before, after):
        spread_alpha(source, c * half_y, half_y)
    for t in range(2):
        relay_cp[t].wait_recv()
        share(across, quarters[t])
    spread_alpha(across, c * half_y, half_y)
    for t in far_first(nz):
        ob_cp[t].wait_recv()
        decode(obs_all, lax.rem(z + nz - 1 - t, nz))
    for h in range(halves):
        tot_own[h] = totals[h]
    tot_cp = [
        pltpu.make_async_remote_copy(
            tot_own, tot_buf.at[t], tot_send.at[t], tot_recv.at[t], device_id=to_g(t), device_id_type=MESH
        )
        for t in range(ng - 1)
    ]
    for cp in tot_cp:
        cp.start()

    own_ts.wait()
    for cp in ts_cp:
        cp.wait_recv()

    def trans_share(which, n, target):
        return pltpu.make_async_remote_copy(
            t_blk.at[which],
            t_blk.at[which],
            ty_send.at[n],
            ty_recv.at[n],
            device_id={"bel": target},
            device_id_type=MESH,
        )

    ty_cp = [trans_share(mine, n, to) for n, to in enumerate((across, after, before))]
    for cp in ty_cp:
        cp.start()
    other = (1 - c) * half_y
    for cp, (source, n) in zip(
        share_cp, ((before, 0), (after, 1), (before, 1), (after, 0), (across, 0), (across, 1))
    ):
        cp.wait_recv()
        spread_alpha(source, other + n * quarter, quarter)
    for pair in to_scalar:
        for cp in pair:
            cp.wait()
    rs_cp = []
    for t in range(ng):
        j = g_at(t) if t < ng - 1 else g

        def one_belief(r, carry):
            b = j * own_rows + r
            a = act_s[b]
            sums = [None] * 4
            for n in range(nz):
                probs = obs_rows[n * actions + a]
                for o in range(obs_local):
                    term = al_rows[pl.ds(pk_s[n][o][0, b], halves), :] * probs[o * halves : (o + 1) * halves]
                    sums[o % 4] = term if n == 0 else sums[o % 4] + term
            part[pl.ds(pl.multiple_of(b * halves, halves), halves), :] = (sums[0] + sums[1]) + (
                sums[2] + sums[3]
            )
            return carry

        lax.fori_loop(0, own_rows, one_belief, 0, unroll=4)
        if t < ng - 1:
            rows = own_rows * halves
            cp = pltpu.make_async_remote_copy(
                part.at[pl.ds(pl.multiple_of(j * rows, rows), rows), :],
                rs_buf.at[t],
                rs_send.at[t],
                rs_recv.at[t],
                device_id=to_g(t),
                device_id_type=MESH,
            )
            cp.start()
            rs_cp.append(cp)

    for cp in tot_cp:
        cp.wait_recv()
    for cp in rs_cp:
        cp.wait_recv()
    act_own = act_i[pl.ds(pl.multiple_of(g * own_rows, own_rows), own_rows), :]
    values = []
    for h in range(halves):
        total = tot_own[h]
        for t in range(ng - 1):
            total = total + tot_buf[t, h]
        raw = part[pl.ds(g * own_rows * halves + h, own_rows, stride=halves), :]
        for t in range(ng - 1):
            raw = raw + rs_buf[t, pl.ds(h, own_rows, stride=halves), :]
        divisor = jnp.ones((own_rows, LANES), jnp.float32)
        for a in range(actions):
            divisor = jnp.where(act_own == a, total[a : a + 1, :], divisor)
        values.append(raw / divisor)
    coded, level = to_codes(values)
    for h in range(halves):
        cols = slice(h * LANES, (h + 1) * LANES)
        w_all[g, :own_rows, cols] = coded[h].astype(jnp.int16)
        w_all[g, own_rows:, cols] = level.astype(jnp.int16)

    w_cp = [
        pltpu.make_async_remote_copy(
            w_all.at[g], w_all.at[g], w_send.at[t], w_recv.at[t], device_id=to_g(t), device_id_type=MESH
        )
        for t in range(ng - 1)
    ]
    for cp in w_cp:
        cp.start()

    def spread_owner(j):
        rows = pl.ds(pl.multiple_of(j * own_rows, own_rows), own_rows)
        low_rows = pl.ds(pl.multiple_of(bel + j * own_rows, own_rows), own_rows)
        w_scale[rows, :] = jnp.broadcast_to(
            scale_of(w_all[j, own_rows : own_rows + 1, :].astype(jnp.int32).astype(jnp.float32)), (own_rows, width)
        )[:, :qwidth]
        act = act_b[rows, :]
        pieces = []
        for h in range(halves):
            q = w_all[j, :own_rows, h * LANES : (h + 1) * LANES].astype(jnp.int32)
            high = jnp.right_shift(q + 128, 8)
            low = q - jnp.left_shift(high, 8)
            pieces.append((high.astype(jnp.float32).astype(jnp.bfloat16), low.astype(jnp.float32).astype(jnp.bfloat16)))

        for a in range(actions):
            hot = act == jnp.asarray(a, jnp.bfloat16)
            for h in range(halves):
                high, low = pieces[h]
                cols = slice(a * width + h * LANES, a * width + (h + 1) * LANES)
                spread[rows, cols] = jnp.where(hot, high, jnp.zeros_like(high))
                spread[low_rows, cols] = jnp.where(hot, low, jnp.zeros_like(low))

    spread_owner(g)
    own_t.wait()
    for cp in t_cp:
        cp.wait_recv()
    for cp in ty_cp:
        cp.wait_recv()

    def total_action(a, carry):
        tt_own[pl.ds(a, 1), :] = jnp.sum(
            t_blk[a].astype(jnp.float32), axis=0, keepdims=True
        )
        return carry

    lax.fori_loop(0, actions, total_action, 0)
    tt_cp = [
        pltpu.make_async_remote_copy(
            tt_own, tt_buf.at[t], tt_send.at[t], tt_recv.at[t], device_id=to_z(t), device_id_type=MESH
        )
        for t in range(nz - 1)
    ]
    for cp in tt_cp:
        cp.start()

    for t in range(ng - 1):
        w_cp[t].wait_recv()
        spread_owner(g_from(t))
    both = jnp.dot(
        spread[...],
        t_blk[...].reshape(actions * width, qwidth),
        preferred_element_type=jnp.float32,
    )
    fut[...] = (256.0 * both[:bel] + both[bel:]) * w_scale[...]

    def send_future(j, t):
        rows = pl.ds(pl.multiple_of(j * z_rows, z_rows), z_rows)
        act = act_i[rows, :]
        values = []
        for h in range(qwidth // LANES):
            cols = slice(h * LANES, (h + 1) * LANES)
            divisor = jnp.ones((z_rows, LANES), jnp.float32)
            for a in range(actions):
                divisor = jnp.where(act == a, tt_all[a : a + 1, cols], divisor)
            values.append(fut[rows, cols] / divisor)
        coded, level = to_codes(values)
        for n in range(ng):
            parts = [code[n * last : (n + 1) * last] for code in coded]
            piece = jnp.concatenate(parts + [level[: PIECE - used]], axis=0)
            fut_q[t + 1, n] = piece.astype(jnp.int16)
        for u in range(-1, ng - 1):
            if t < 0 and u < 0:
                continue
            n = g if u < 0 else g_at(u)
            cp = pltpu.make_async_remote_copy(
                fut_q.at[t + 1, n, pl.ds(0, used + 2)],
                f_buf.at[t + 1, u + 1, pl.ds(0, used + 2)],
                f_send.at[t + 1, u + 1],
                f_recv.at[t + 1, u + 1],
                device_id={"obs_0": j, "obs_1": n // nc, "obs_2": lax.rem(n, nc)},
                device_id_type=MESH,
            )
            cp.start()
            f_cp.append(cp)

    for cp in tt_cp:
        cp.wait_recv()
    total = tt_own[...]
    for t in range(nz - 1):
        total = total + tt_buf[t]
    tt_all[...] = total
    f_cp = []
    for t in far_first(nz):
        send_future(z_at(t), t)
    send_future(z, -1)
    own_rew.wait()
    for r in range(last):
        rew_ref[r : r + 1, :] = rew_v[pl.ds(act_s[(z * ng + g) * last + r], 1), :]
    for cp in f_cp:
        cp.wait_recv()

    for u in range(ng):
        at = g if u == 0 else g_from(u - 1)
        future = None
        for t in range(nz):
            codes = fut_q[0, g] if u == 0 and t == 0 else f_buf[t, u]
            codes = codes.astype(jnp.int32).astype(jnp.float32)
            term = codes * scale_of(codes[used : used + 1])
            future = term if future is None else future + term
        for h in range(qwidth // LANES):
            out_ref[:, pl.ds(pl.multiple_of(at * qwidth + h * LANES, LANES), LANES)] = future[
                h * last : (h + 1) * last
            ]
    for cp in ob_cp + pk_cp + al_cp[0] + al_cp[1] + share_cp + ts_cp + ty_cp + t_cp + relay_cp + tot_cp + rs_cp + w_cp + f_cp + tt_cp:
        cp.wait_send()


def body(dims, alpha_set, transitions, obs_weights, rewards, chosen_idx, chosen_action):
    ny, nz, nx, nc = dims
    ng = nx * nc
    actions, states = rewards.shape
    bel = chosen_action.shape[0]
    obs_local = obs_weights.shape[0]
    width = states // nz
    qwidth = states // ng
    halves = width // LANES
    count = alpha_set.shape[0] * ny
    f32, b16, i32 = jnp.float32, jnp.bfloat16, jnp.int32
    dma = pltpu.SemaphoreType.DMA
    vmem = pl.BlockSpec(memory_space=pltpu.VMEM)
    hbm = pl.BlockSpec(memory_space=pl.ANY)
    z_rows = bel // nz
    own_rows = bel // ng
    scratch = [
        pltpu.VMEM((ny, count // ny, width), b16),
        pltpu.VMEM((count * halves, LANES), f32),
        pltpu.VMEM((bel, LANES), i32),
        pltpu.VMEM((bel, LANES), b16),
        pltpu.VMEM((obs_local, actions, states), f32),
        pltpu.VMEM((nz, obs_local, actions, width), jnp.int16),
        pltpu.VMEM((nz, obs_local, actions, width), jnp.int16),
        pltpu.VMEM((nz * actions, obs_local * halves, LANES), f32),
        pltpu.VMEM((obs_local, 1, bel), i32),
        pltpu.VMEM((nz, obs_local, 1, bel), i32),
        [[pltpu.SMEM((1, bel), i32) for _ in range(obs_local)] for _ in range(nz)],
        pltpu.VMEM((bel * halves, LANES), f32),
        pltpu.VMEM((ng - 1, own_rows * halves, LANES), f32),
        pltpu.VMEM((halves, actions, LANES), f32),
        pltpu.VMEM((ng - 1, halves, actions, LANES), f32),
        pltpu.VMEM((ng, own_rows + 8, width), jnp.int16),
        pltpu.VMEM((actions, width, qwidth), b16),
        pltpu.VMEM((2 * bel, actions * width), b16),
        pltpu.VMEM((bel, qwidth), f32),
        pltpu.VMEM((bel, qwidth), f32),
        pltpu.VMEM((nz, ng, PIECE, LANES), jnp.int16),
        pltpu.VMEM((nz, ng, PIECE, LANES), jnp.int16),
        pltpu.VMEM((actions, qwidth), f32),
        pltpu.VMEM((nz - 1, actions, qwidth), f32),
        pltpu.VMEM((actions, states), f32),
        pltpu.VMEM((actions, qwidth), f32),
        dma((5 + nz * obs_local,)),
        dma((nz - 1,)),
        dma((nz - 1,)),
        dma((2, 2)),
        dma((2, 2)),
        dma((2,)),
        dma((2,)),
        dma((6,)),
        dma((6,)),
        dma((nz - 1,)),
        dma((nz - 1,)),
        dma((ng - 1,)),
        dma((ng - 1,)),
        dma((ng - 1,)),
        dma((ng - 1,)),
        dma((ny - 1,)),
        dma((ny - 1,)),
        dma((ng - 1,)),
        dma((ng - 1,)),
        dma((ng - 1,)),
        dma((ng - 1,)),
        dma((ng - 1,)),
        dma((ng - 1,)),
        dma((nz, ng)),
        dma((nz, ng)),
        dma((nz - 1,)),
        dma((nz - 1,)),
    ]
    rows = pltpu.VMEM((bel // (nz * ng), states), f32)
    future, reward = pl.pallas_call(
        functools.partial(kernel, dims),
        out_shape=(rows, rows),
        in_specs=[
            pl.BlockSpec(memory_space=pltpu.SMEM),
            vmem,
            vmem,
            hbm,
            hbm,
            hbm,
            hbm,
        ],
        out_specs=(vmem, vmem),
        scratch_shapes=scratch,
        compiler_params=pltpu.CompilerParams(
            collective_id=0, has_side_effects=True, vmem_limit_bytes=60 * 1024 * 1024
        ),
        name="backup",
    )(
        chosen_action,
        chosen_action.reshape(1, bel),
        jnp.transpose(chosen_idx, (1, 2, 0)),
        alpha_set,
        transitions,
        obs_weights,
        rewards,
    )
    return reward + DISCOUNT * future


def solution(mesh):
    dims = (mesh.shape["bel"], 8, 4, 2)
    torus = Mesh(
        mesh.devices.reshape(*dims[1:], dims[0]), ("obs_0", "obs_1", "obs_2", "bel")
    )
    return jax.shard_map(
        functools.partial(body, dims),
        mesh=torus,
        in_specs=(
            P("bel", None),
            P(None, OBS, None),
            P(OBS, None, None),
            P(),
            P("bel", None, OBS),
            P("bel"),
        ),
        out_specs=P(BEL_OBS, None),
        check_vma=False,
    )
```

```python
import functools

import jax
import jax.numpy as jnp
from jax import lax
from jax.experimental import pallas as pl
from jax.experimental.pallas import tpu as pltpu
from jax.sharding import Mesh
from jax.sharding import PartitionSpec as P

OBS = ("obs_0", "obs_1", "obs_2")
BEL_OBS = ("bel", "obs_0", "obs_1", "obs_2")
LANES = 128
PIECE = 16
DISCOUNT = 0.95
CODE_SCALE = 14114.0
CODE_SHIFT = 2.302585093 * CODE_SCALE
MESH = pl.DeviceIdType.MESH


def to_codes(values):
    largest = functools.reduce(
        jnp.maximum, [jnp.max(jnp.abs(v), axis=(0, 1), keepdims=True) for v in values]
    )
    level = jnp.ceil(32.0 * jnp.log(jnp.maximum(largest, 1e-30) * (1.0 / 32760.0)))
    inverse = jnp.exp(level * (-1.0 / 32.0))
    coded = [
        jnp.clip(jnp.round(v * inverse), -32767.0, 32767.0).astype(jnp.int32)
        for v in values
    ]
    return coded, jnp.broadcast_to(level, (8, LANES)).astype(jnp.int32)


def scale_of(level):
    return jnp.exp(level * (1.0 / 32.0))


def far_first(n):
    return sorted(range(n - 1), key=lambda t: -min(t + 1, n - 1 - t))


def group_offsets(nx, nc):
    steps = [(dx, dc) for dx in range(nx) for dc in range(nc) if dx or dc]
    return sorted(steps, key=lambda step: -min(step[0], nx - step[0]))


def kernel(
    dims,
    act_hbm,
    idx_hbm,
    alpha_hbm,
    trans_hbm,
    obs_hbm,
    rew_hbm,
    out_ref,
    rew_ref,
    al_bf,
    al_rows,
    act_s,
    act_v,
    idx_v,
    act_i,
    act_b,
    obs_v,
    obs_code,
    obs_all,
    obs_rows,
    pk_own,
    pk_v,
    pk_s,
    part,
    rs_buf,
    tot_own,
    tot_buf,
    w_all,
    t_blk,
    spread,
    w_scale,
    fut,
    fut_q,
    f_buf,
    tt_own,
    tt_buf,
    rew_v,
    tt_all,
    local_sem,
    pk_send,
    pk_recv,
    al_send,
    al_recv,
    relay_send,
    relay_recv,
    share_send,
    share_recv,
    ob_send,
    ob_recv,
    t_send,
    t_recv,
    ts_send,
    ts_recv,
    ty_send,
    ty_recv,
    tot_send,
    tot_recv,
    rs_send,
    rs_recv,
    w_send,
    w_recv,
    f_send,
    f_recv,
    tt_send,
    tt_recv,
):
    ny, nz, nx, nc = dims
    ng = nx * nc
    actions = t_blk.shape[0]
    width = t_blk.shape[1]
    qwidth = t_blk.shape[2]
    halves = width // LANES
    bel = fut.shape[0]
    own_rows = bel // ng
    z_rows = bel // nz
    rows_y = alpha_hbm.shape[0]
    half_y = rows_y // nc
    obs_local = obs_hbm.shape[0]
    t_rows = trans_hbm.shape[1]
    last = out_ref.shape[0]
    used = last * (qwidth // LANES)
    per_y = actions // (2 * ny)
    direct = actions - per_y * ny

    y = lax.axis_index("bel")
    z = lax.axis_index("obs_0")
    x = lax.axis_index("obs_1")
    c = lax.axis_index("obs_2")
    g = x * nc + c

    def y_at(t):
        return lax.rem(y + 1 + t, ny)

    def z_at(t):
        return lax.rem(z + 1 + t, nz)

    offsets = group_offsets(nx, nc)

    def g_at(t):
        dx, dc = offsets[t]
        return lax.rem(x + dx, nx) * nc + lax.rem(c + dc, nc)

    def g_from(t):
        dx, dc = offsets[t]
        return lax.rem(x + nx - dx, nx) * nc + lax.rem(c + nc - dc, nc)

    def to_y(t):
        return {"bel": y_at(t)}

    def to_z(t):
        return {"obs_0": z_at(t)}

    def to_g(t):
        j = g_at(t)
        return {"obs_1": j // nc, "obs_2": lax.rem(j, nc)}

    peers = (
        [to_y(t) for t in range(ny - 1)]
        + [to_z(t) for t in range(nz - 1)]
        + [to_g(t) for t in range(ng - 1)]
    )
    barrier = pltpu.get_barrier_semaphore()
    for peer in peers:
        pl.semaphore_signal(barrier, inc=1, device_id=peer, device_id_type=MESH)

    z_cols = pl.ds(pl.multiple_of(z * width, width), width)
    q_cols = pl.ds(pl.multiple_of(g * qwidth, qwidth), qwidth)

    own_al = pltpu.make_async_copy(alpha_hbm.at[:, z_cols], al_bf.at[y], local_sem.at[7])
    own_ob = pltpu.make_async_copy(obs_hbm, obs_v, local_sem.at[2])
    g_rows = pl.ds(pl.multiple_of(g * t_rows, t_rows), t_rows)
    mine = pl.ds(direct + y * per_y, per_y)
    own_t = pltpu.make_async_copy(
        trans_hbm.at[:direct, :, q_cols], t_blk.at[:direct, g_rows, :], local_sem.at[3]
    )
    own_ts = pltpu.make_async_copy(
        trans_hbm.at[mine, :, q_cols], t_blk.at[mine, g_rows, :], local_sem.at[0]
    )
    own_rew = pltpu.make_async_copy(rew_hbm, rew_v, local_sem.at[4])
    own_act = [
        pltpu.make_async_copy(act_hbm, act_s, local_sem.at[1]),
        pltpu.make_async_copy(act_hbm, act_v, local_sem.at[5]),
        pltpu.make_async_copy(idx_hbm, idx_v, local_sem.at[6]),
    ]
    for cp in own_act:
        cp.start()
    own_ob.start()
    own_al.start()
    own_t.start()
    own_ts.start()
    own_rew.start()

    for cp in own_act:
        cp.wait()
    act_row = act_v[...].reshape(1, bel)
    picks = jnp.zeros((obs_local, bel), jnp.int32)
    for a in range(actions):
        picks = jnp.where(act_row == a, idx_v[a] * halves, picks)
    for o in range(obs_local):
        pk_own[o] = picks[o : o + 1, :]
        pk_v[z, o] = picks[o : o + 1, :]

    def fill_action(b, carry):
        act_i[pl.ds(b, 1), :] = jnp.full((1, LANES), act_s[b], jnp.int32)
        return carry

    lax.fori_loop(0, bel, fill_action, 0, unroll=8)
    act_b[...] = act_i[...].astype(jnp.float32).astype(jnp.bfloat16)
    own_ob.wait()
    for n in range(nz):
        for o in range(obs_local):
            v = jnp.log(obs_v[o, :, n * width : (n + 1) * width])
            obs_code[n, o] = jnp.round(v * CODE_SCALE + CODE_SHIFT).astype(jnp.int32).astype(jnp.int16)
    pl.semaphore_wait(barrier, len(peers))

    quarter = half_y // 2
    quarters = [pl.ds(pl.multiple_of(c * half_y + n * quarter, quarter), quarter) for n in range(2)]
    pk_cp = [
        pltpu.make_async_remote_copy(
            pk_own,
            pk_v.at[z],
            pk_send.at[t],
            pk_recv.at[t],
            device_id=to_z(t),
            device_id_type=MESH,
        )
        for t in range(nz - 1)
    ]
    al_cp = [
        [
            pltpu.make_async_remote_copy(
                al_bf.at[y, quarters[n]],
                al_bf.at[y, quarters[n]],
                al_send.at[t, m],
                al_recv.at[t, m],
                device_id={"bel": lax.rem(y + step, ny)},
                device_id_type=MESH,
            )
            for m, n in enumerate((t, 1 - t))
        ]
        for t, step in ((0, 1), (1, ny - 1))
    ]
    ob_cp = [
        pltpu.make_async_remote_copy(
            obs_code.at[z_at(t)],
            obs_all.at[z],
            ob_send.at[t],
            ob_recv.at[t],
            device_id=to_z(t),
            device_id_type=MESH,
        )
        for t in range(nz - 1)
    ]
    def trans_copy(t, which, send, recv):
        return pltpu.make_async_remote_copy(
            trans_hbm.at[which, :, pl.ds(pl.multiple_of(g_at(t) * qwidth, qwidth), qwidth)],
            t_blk.at[which, g_rows, :],
            send.at[t],
            recv.at[t],
            device_id=to_g(t),
            device_id_type=MESH,
        )

    ts_cp = [trans_copy(t, mine, ts_send, ts_recv) for t in range(ng - 1)]
    t_cp = [trans_copy(t, pl.ds(0, direct), t_send, t_recv) for t in range(ng - 1)]
    for cp in pk_cp:
        cp.start()
    own_al.wait()
    for m in range(2):
        for pair in al_cp:
            pair[m].start()
    for t in far_first(nz):
        ob_cp[t].start()
    for cp in ts_cp:
        cp.start()

    def spread_alpha(block, start, rows):
        def rows16(n, carry):
            r = pl.multiple_of(start + n * 16, 16)
            v = al_bf[block, pl.ds(r, 16), :].astype(jnp.float32)
            for h in range(halves):
                al_rows[pl.ds((block * rows_y + r) * halves + h, 16, stride=halves), :] = v[
                    :, h * LANES : (h + 1) * LANES
                ]
            return carry

        lax.fori_loop(0, rows // 16, rows16, 0, unroll=4)

    spread_alpha(y, 0, rows_y)

    for cp in pk_cp:
        cp.wait_recv()
    to_scalar = [
        [
            pltpu.make_async_copy(pk_v.at[n, o], pk_s[n][o], local_sem.at[8 + n * obs_local + o])
            for o in range(obs_local)
        ]
        for n in range(nz)
    ]
    for pair in to_scalar:
        for cp in pair:
            cp.start()

    totals = [jnp.zeros((actions, LANES), jnp.float32) for _ in range(halves)]

    def decode(code_ref, slot):
        for o in range(obs_local):
            v = jnp.exp(
                code_ref[slot, o].astype(jnp.int32).astype(jnp.float32) * (1.0 / CODE_SCALE)
            )
            for h in range(halves):
                part_h = v[:, h * LANES : (h + 1) * LANES]
                totals[h] = totals[h] + part_h
                obs_rows[pl.ds(slot * actions, actions), o * halves + h, :] = part_h

    decode(obs_code, z)
    share_cp = []

    def share(block, rows):
        cp = pltpu.make_async_remote_copy(
            al_bf.at[block, rows],
            al_bf.at[block, rows],
            share_send.at[len(share_cp)],
            share_recv.at[len(share_cp)],
            device_id={"obs_2": 1 - c},
            device_id_type=MESH,
        )
        cp.start()
        share_cp.append(cp)

    before, after, across = (lax.rem(y + n, ny) for n in (ny - 1, 1, ny - 2))
    relay_cp = []
    for t, (source, target) in enumerate(((before, after), (after, before))):
        al_cp[t][0].wait_recv()
        cp = pltpu.make_async_remote_copy(
            al_bf.at[source, quarters[t]],
            al_bf.at[source, quarters[t]],
            relay_send.at[t],
            relay_recv.at[t],
            device_id={"bel": target},
            device_id_type=MESH,
        )
        cp.start()
        relay_cp.append(cp)
    for t, source in enumerate((before, after)):
        share(source, quarters[t])
    for t, source in enumerate((before, after)):
        al_cp[t][1].wait_recv()
        share(source, quarters[1 - t])
    for cp in t_cp:
        cp.start()
    for source in (before, after):
        spread_alpha(source, c * half_y, half_y)
    for t in range(2):
        relay_cp[t].wait_recv()
        share(across, quarters[t])
    spread_alpha(across, c * half_y, half_y)
    own_ts.wait()
    for cp in ts_cp:
        cp.wait_recv()

    def trans_share(which, n, target):
        return pltpu.make_async_remote_copy(
            t_blk.at[which],
            t_blk.at[which],
            ty_send.at[n],
            ty_recv.at[n],
            device_id={"bel": target},
            device_id_type=MESH,
        )

    ty_cp = [trans_share(mine, n, to) for n, to in enumerate((across, after, before))]
    for cp in ty_cp:
        cp.start()
    for t in far_first(nz):
        ob_cp[t].wait_recv()
        decode(obs_all, lax.rem(z + nz - 1 - t, nz))
    for h in range(halves):
        tot_own[h] = totals[h]
    tot_cp = [
        pltpu.make_async_remote_copy(
            tot_own, tot_buf.at[t], tot_send.at[t], tot_recv.at[t], device_id=to_g(t), device_id_type=MESH
        )
        for t in range(ng - 1)
    ]
    for cp in tot_cp:
        cp.start()

    other = (1 - c) * half_y
    for cp, (source, n) in zip(
        share_cp, ((before, 0), (after, 1), (before, 1), (after, 0), (across, 0), (across, 1))
    ):
        cp.wait_recv()
        spread_alpha(source, other + n * quarter, quarter)
    for pair in to_scalar:
        for cp in pair:
            cp.wait()
    rs_cp = []
    for t in range(ng):
        j = g_at(t) if t < ng - 1 else g

        def one_belief(r, carry):
            b = j * own_rows + r
            a = act_s[b]
            sums = [None] * 4
            for n in range(nz):
                probs = obs_rows[n * actions + a]
                for o in range(obs_local):
                    term = al_rows[pl.ds(pk_s[n][o][0, b], halves), :] * probs[o * halves : (o + 1) * halves]
                    sums[o % 4] = term if n == 0 else sums[o % 4] + term
            part[pl.ds(pl.multiple_of(b * halves, halves), halves), :] = (sums[0] + sums[1]) + (
                sums[2] + sums[3]
            )
            return carry

        lax.fori_loop(0, own_rows, one_belief, 0, unroll=4)
        if t < ng - 1:
            rows = own_rows * halves
            cp = pltpu.make_async_remote_copy(
                part.at[pl.ds(pl.multiple_of(j * rows, rows), rows), :],
                rs_buf.at[t],
                rs_send.at[t],
                rs_recv.at[t],
                device_id=to_g(t),
                device_id_type=MESH,
            )
            cp.start()
            rs_cp.append(cp)

    for cp in tot_cp:
        cp.wait_recv()
    for cp in rs_cp:
        cp.wait_recv()
    act_own = act_i[pl.ds(pl.multiple_of(g * own_rows, own_rows), own_rows), :]
    values = []
    for h in range(halves):
        total = tot_own[h]
        for t in range(ng - 1):
            total = total + tot_buf[t, h]
        raw = part[pl.ds(g * own_rows * halves + h, own_rows, stride=halves), :]
        for t in range(ng - 1):
            raw = raw + rs_buf[t, pl.ds(h, own_rows, stride=halves), :]
        divisor = jnp.ones((own_rows, LANES), jnp.float32)
        for a in range(actions):
            divisor = jnp.where(act_own == a, total[a : a + 1, :], divisor)
        values.append(raw / divisor)
    coded, level = to_codes(values)
    for h in range(halves):
        cols = slice(h * LANES, (h + 1) * LANES)
        w_all[g, :own_rows, cols] = coded[h].astype(jnp.int16)
        w_all[g, own_rows:, cols] = level.astype(jnp.int16)

    w_cp = [
        pltpu.make_async_remote_copy(
            w_all.at[g], w_all.at[g], w_send.at[t], w_recv.at[t], device_id=to_g(t), device_id_type=MESH
        )
        for t in range(ng - 1)
    ]
    for cp in w_cp:
        cp.start()

    def spread_owner(j):
        rows = pl.ds(pl.multiple_of(j * own_rows, own_rows), own_rows)
        low_rows = pl.ds(pl.multiple_of(bel + j * own_rows, own_rows), own_rows)
        w_scale[rows, :] = jnp.broadcast_to(
            scale_of(w_all[j, own_rows : own_rows + 1, :].astype(jnp.int32).astype(jnp.float32)), (own_rows, width)
        )[:, :qwidth]
        act = act_b[rows, :]
        pieces = []
        for h in range(halves):
            q = w_all[j, :own_rows, h * LANES : (h + 1) * LANES].astype(jnp.int32)
            high = jnp.right_shift(q + 128, 8)
            low = q - jnp.left_shift(high, 8)
            pieces.append((high.astype(jnp.float32).astype(jnp.bfloat16), low.astype(jnp.float32).astype(jnp.bfloat16)))

        for a in range(actions):
            hot = act == jnp.asarray(a, jnp.bfloat16)
            for h in range(halves):
                high, low = pieces[h]
                cols = slice(a * width + h * LANES, a * width + (h + 1) * LANES)
                spread[rows, cols] = jnp.where(hot, high, jnp.zeros_like(high))
                spread[low_rows, cols] = jnp.where(hot, low, jnp.zeros_like(low))

    spread_owner(g)
    own_t.wait()
    for cp in t_cp:
        cp.wait_recv()
    for cp in ty_cp:
        cp.wait_recv()

    def total_action(a, carry):
        tt_own[pl.ds(a, 1), :] = jnp.sum(
            t_blk[a].astype(jnp.float32), axis=0, keepdims=True
        )
        return carry

    lax.fori_loop(0, actions, total_action, 0)
    tt_cp = [
        pltpu.make_async_remote_copy(
            tt_own, tt_buf.at[t], tt_send.at[t], tt_recv.at[t], device_id=to_z(t), device_id_type=MESH
        )
        for t in range(nz - 1)
    ]
    for cp in tt_cp:
        cp.start()

    for t in range(ng - 1):
        w_cp[t].wait_recv()
        spread_owner(g_from(t))
    both = jnp.dot(
        spread[...],
        t_blk[...].reshape(actions * width, qwidth),
        preferred_element_type=jnp.float32,
    )
    fut[...] = (256.0 * both[:bel] + both[bel:]) * w_scale[...]

    def send_future(j, t):
        rows = pl.ds(pl.multiple_of(j * z_rows, z_rows), z_rows)
        act = act_i[rows, :]
        values = []
        for h in range(qwidth // LANES):
            cols = slice(h * LANES, (h + 1) * LANES)
            divisor = jnp.ones((z_rows, LANES), jnp.float32)
            for a in range(actions):
                divisor = jnp.where(act == a, tt_all[a : a + 1, cols], divisor)
            values.append(fut[rows, cols] / divisor)
        coded, level = to_codes(values)
        for n in range(ng):
            parts = [code[n * last : (n + 1) * last] for code in coded]
            piece = jnp.concatenate(parts + [level[: PIECE - used]], axis=0)
            fut_q[t + 1, n] = piece.astype(jnp.int16)
        for u in range(-1, ng - 1):
            if t < 0 and u < 0:
                continue
            n = g if u < 0 else g_at(u)
            cp = pltpu.make_async_remote_copy(
                fut_q.at[t + 1, n, pl.ds(0, used + 2)],
                f_buf.at[t + 1, u + 1, pl.ds(0, used + 2)],
                f_send.at[t + 1, u + 1],
                f_recv.at[t + 1, u + 1],
                device_id={"obs_0": j, "obs_1": n // nc, "obs_2": lax.rem(n, nc)},
                device_id_type=MESH,
            )
            cp.start()
            f_cp.append(cp)

    for cp in tt_cp:
        cp.wait_recv()
    total = tt_own[...]
    for t in range(nz - 1):
        total = total + tt_buf[t]
    tt_all[...] = total
    f_cp = []
    for t in far_first(nz):
        send_future(z_at(t), t)
    send_future(z, -1)
    own_rew.wait()
    for r in range(last):
        rew_ref[r : r + 1, :] = rew_v[pl.ds(act_s[(z * ng + g) * last + r], 1), :]
    for cp in f_cp:
        cp.wait_recv()

    for u in range(ng):
        at = g if u == 0 else g_from(u - 1)
        future = None
        for t in range(nz):
            codes = fut_q[0, g] if u == 0 and t == 0 else f_buf[t, u]
            codes = codes.astype(jnp.int32).astype(jnp.float32)
            term = codes * scale_of(codes[used : used + 1])
            future = term if future is None else future + term
        for h in range(qwidth // LANES):
            out_ref[:, pl.ds(pl.multiple_of(at * qwidth + h * LANES, LANES), LANES)] = future[
                h * last : (h + 1) * last
            ]
    for cp in ob_cp + pk_cp + al_cp[0] + al_cp[1] + share_cp + ts_cp + ty_cp + t_cp + relay_cp + tot_cp + rs_cp + w_cp + f_cp + tt_cp:
        cp.wait_send()


def body(dims, alpha_set, transitions, obs_weights, rewards, chosen_idx, chosen_action):
    ny, nz, nx, nc = dims
    ng = nx * nc
    actions, states = rewards.shape
    bel = chosen_action.shape[0]
    obs_local = obs_weights.shape[0]
    width = states // nz
    qwidth = states // ng
    halves = width // LANES
    count = alpha_set.shape[0] * ny
    f32, b16, i32 = jnp.float32, jnp.bfloat16, jnp.int32
    dma = pltpu.SemaphoreType.DMA
    vmem = pl.BlockSpec(memory_space=pltpu.VMEM)
    hbm = pl.BlockSpec(memory_space=pl.ANY)
    z_rows = bel // nz
    own_rows = bel // ng
    scratch = [
        pltpu.VMEM((ny, count // ny, width), b16),
        pltpu.VMEM((count * halves, LANES), f32),
        pltpu.SMEM((bel,), i32),
        pltpu.VMEM((bel,), i32),
        pltpu.VMEM((actions, obs_local, bel), i32),
        pltpu.VMEM((bel, LANES), i32),
        pltpu.VMEM((bel, LANES), b16),
        pltpu.VMEM((obs_local, actions, states), f32),
        pltpu.VMEM((nz, obs_local, actions, width), jnp.int16),
        pltpu.VMEM((nz, obs_local, actions, width), jnp.int16),
        pltpu.VMEM((nz * actions, obs_local * halves, LANES), f32),
        pltpu.VMEM((obs_local, 1, bel), i32),
        pltpu.VMEM((nz, obs_local, 1, bel), i32),
        [[pltpu.SMEM((1, bel), i32) for _ in range(obs_local)] for _ in range(nz)],
        pltpu.VMEM((bel * halves, LANES), f32),
        pltpu.VMEM((ng - 1, own_rows * halves, LANES), f32),
        pltpu.VMEM((halves, actions, LANES), f32),
        pltpu.VMEM((ng - 1, halves, actions, LANES), f32),
        pltpu.VMEM((ng, own_rows + 8, width), jnp.int16),
        pltpu.VMEM((actions, width, qwidth), b16),
        pltpu.VMEM((2 * bel, actions * width), b16),
        pltpu.VMEM((bel, qwidth), f32),
        pltpu.VMEM((bel, qwidth), f32),
        pltpu.VMEM((nz, ng, PIECE, LANES), jnp.int16),
        pltpu.VMEM((nz, ng, PIECE, LANES), jnp.int16),
        pltpu.VMEM((actions, qwidth), f32),
        pltpu.VMEM((nz - 1, actions, qwidth), f32),
        pltpu.VMEM((actions, states), f32),
        pltpu.VMEM((actions, qwidth), f32),
        dma((8 + nz * obs_local,)),
        dma((nz - 1,)),
        dma((nz - 1,)),
        dma((2, 2)),
        dma((2, 2)),
        dma((2,)),
        dma((2,)),
        dma((6,)),
        dma((6,)),
        dma((nz - 1,)),
        dma((nz - 1,)),
        dma((ng - 1,)),
        dma((ng - 1,)),
        dma((ng - 1,)),
        dma((ng - 1,)),
        dma((ny - 1,)),
        dma((ny - 1,)),
        dma((ng - 1,)),
        dma((ng - 1,)),
        dma((ng - 1,)),
        dma((ng - 1,)),
        dma((ng - 1,)),
        dma((ng - 1,)),
        dma((nz, ng)),
        dma((nz, ng)),
        dma((nz - 1,)),
        dma((nz - 1,)),
    ]
    rows = pltpu.VMEM((bel // (nz * ng), states), f32)
    future, reward = pl.pallas_call(
        functools.partial(kernel, dims),
        out_shape=(rows, rows),
        in_specs=[
            hbm,
            hbm,
            hbm,
            hbm,
            hbm,
            hbm,
        ],
        out_specs=(vmem, vmem),
        scratch_shapes=scratch,
        compiler_params=pltpu.CompilerParams(
            collective_id=0, has_side_effects=True, vmem_limit_bytes=60 * 1024 * 1024
        ),
        name="backup",
    )(
        chosen_action,
        jnp.transpose(chosen_idx, (1, 2, 0)),
        alpha_set,
        transitions,
        obs_weights,
        rewards,
    )
    return reward + DISCOUNT * future


def solution(mesh):
    dims = (mesh.shape["bel"], 8, 4, 2)
    torus = Mesh(
        mesh.devices.reshape(*dims[1:], dims[0]), ("obs_0", "obs_1", "obs_2", "bel")
    )
    return jax.shard_map(
        functools.partial(body, dims),
        mesh=torus,
        in_specs=(
            P("bel", None),
            P(None, OBS, None),
            P(OBS, None, None),
            P(),
            P("bel", None, OBS),
            P("bel"),
        ),
        out_specs=P(BEL_OBS, None),
        check_vma=False,
    )
```

```python
import functools

import jax
import jax.numpy as jnp
from jax import lax
from jax.experimental import pallas as pl
from jax.experimental.pallas import tpu as pltpu
from jax.sharding import Mesh
from jax.sharding import PartitionSpec as P

OBS = ("obs_0", "obs_1", "obs_2")
BEL_OBS = ("bel", "obs_0", "obs_1", "obs_2")
LANES = 128
PIECE = 16
DISCOUNT = 0.95
CODE_SCALE = 14114.0
CODE_SHIFT = 2.302585093 * CODE_SCALE
MESH = pl.DeviceIdType.MESH


def to_codes(values):
    largest = functools.reduce(
        jnp.maximum, [jnp.max(jnp.abs(v), axis=(0, 1), keepdims=True) for v in values]
    )
    level = jnp.ceil(32.0 * jnp.log(jnp.maximum(largest, 1e-30) * (1.0 / 32760.0)))
    inverse = jnp.exp(level * (-1.0 / 32.0))
    coded = [
        jnp.clip(jnp.round(v * inverse), -32767.0, 32767.0).astype(jnp.int32)
        for v in values
    ]
    return coded, jnp.broadcast_to(level, (8, LANES)).astype(jnp.int32)


def scale_of(level):
    return jnp.exp(level * (1.0 / 32.0))


def far_first(n):
    return sorted(range(n - 1), key=lambda t: -min(t + 1, n - 1 - t))


def group_offsets(nx, nc):
    steps = [(dx, dc) for dx in range(nx) for dc in range(nc) if dx or dc]
    return sorted(steps, key=lambda step: -min(step[0], nx - step[0]))


def kernel(
    dims,
    act_hbm,
    idx_hbm,
    alpha_hbm,
    trans_hbm,
    obs_hbm,
    rew_hbm,
    out_ref,
    rew_ref,
    al_bf,
    al_rows,
    act_s,
    act_v,
    idx_v,
    act_i,
    act_b,
    obs_v,
    obs_code,
    obs_all,
    obs_rows,
    pk_own,
    pk_v,
    pk_s,
    part,
    rs_buf,
    tot_own,
    tot_buf,
    w_all,
    t_blk,
    spread,
    w_scale,
    fut,
    fut_q,
    f_buf,
    tt_own,
    tt_buf,
    rew_v,
    tt_all,
    local_sem,
    pk_send,
    pk_recv,
    al_send,
    al_recv,
    relay_send,
    relay_recv,
    share_send,
    share_recv,
    ob_send,
    ob_recv,
    t_send,
    t_recv,
    ts_send,
    ts_recv,
    ty_send,
    ty_recv,
    tot_send,
    tot_recv,
    rs_send,
    rs_recv,
    w_send,
    w_recv,
    f_send,
    f_recv,
    tt_send,
    tt_recv,
):
    ny, nz, nx, nc = dims
    ng = nx * nc
    actions = t_blk.shape[0]
    width = t_blk.shape[1]
    qwidth = t_blk.shape[2]
    halves = width // LANES
    bel = fut.shape[0]
    own_rows = bel // ng
    z_rows = bel // nz
    rows_y = alpha_hbm.shape[0]
    half_y = rows_y // nc
    obs_local = obs_hbm.shape[0]
    t_rows = trans_hbm.shape[1]
    last = out_ref.shape[0]
    used = last * (qwidth // LANES)
    per_y = actions // (2 * ny)
    direct = actions - per_y * ny

    y = lax.axis_index("bel")
    z = lax.axis_index("obs_0")
    x = lax.axis_index("obs_1")
    c = lax.axis_index("obs_2")
    g = x * nc + c

    def y_at(t):
        return lax.rem(y + 1 + t, ny)

    def z_at(t):
        return lax.rem(z + 1 + t, nz)

    offsets = group_offsets(nx, nc)

    def g_at(t):
        dx, dc = offsets[t]
        return lax.rem(x + dx, nx) * nc + lax.rem(c + dc, nc)

    def g_from(t):
        dx, dc = offsets[t]
        return lax.rem(x + nx - dx, nx) * nc + lax.rem(c + nc - dc, nc)

    def to_y(t):
        return {"bel": y_at(t)}

    def to_z(t):
        return {"obs_0": z_at(t)}

    def to_g(t):
        j = g_at(t)
        return {"obs_1": j // nc, "obs_2": lax.rem(j, nc)}

    peers = (
        [to_y(t) for t in range(ny - 1)]
        + [to_z(t) for t in range(nz - 1)]
        + [to_g(t) for t in range(ng - 1)]
    )
    barrier = pltpu.get_barrier_semaphore()
    for peer in peers:
        pl.semaphore_signal(barrier, inc=1, device_id=peer, device_id_type=MESH)

    z_cols = pl.ds(pl.multiple_of(z * width, width), width)
    q_cols = pl.ds(pl.multiple_of(g * qwidth, qwidth), qwidth)

    own_al = pltpu.make_async_copy(alpha_hbm.at[:, z_cols], al_bf.at[y], local_sem.at[7])
    own_ob = pltpu.make_async_copy(obs_hbm, obs_v, local_sem.at[2])
    g_rows = pl.ds(pl.multiple_of(g * t_rows, t_rows), t_rows)
    mine = pl.ds(direct + y * per_y, per_y)
    own_t = pltpu.make_async_copy(
        trans_hbm.at[:direct, :, q_cols], t_blk.at[:direct, g_rows, :], local_sem.at[3]
    )
    own_ts = pltpu.make_async_copy(
        trans_hbm.at[mine, :, q_cols], t_blk.at[mine, g_rows, :], local_sem.at[0]
    )
    own_rew = pltpu.make_async_copy(rew_hbm, rew_v, local_sem.at[4])
    own_act = [
        pltpu.make_async_copy(act_hbm, act_s, local_sem.at[1]),
        pltpu.make_async_copy(act_hbm, act_v, local_sem.at[5]),
        pltpu.make_async_copy(idx_hbm, idx_v, local_sem.at[6]),
    ]
    for cp in own_act:
        cp.start()
    own_ob.start()
    own_al.start()
    own_t.start()
    own_ts.start()
    own_rew.start()

    for cp in own_act:
        cp.wait()
    act_row = act_v[...].reshape(1, bel)
    picks = jnp.zeros((obs_local, bel), jnp.int32)
    for a in range(actions):
        picks = jnp.where(act_row == a, idx_v[a] * halves, picks)
    for o in range(obs_local):
        pk_own[o] = picks[o : o + 1, :]
        pk_v[z, o] = picks[o : o + 1, :]

    def fill_action(b, carry):
        act_i[pl.ds(b, 1), :] = jnp.full((1, LANES), act_s[b], jnp.int32)
        return carry

    lax.fori_loop(0, bel, fill_action, 0, unroll=8)
    act_b[...] = act_i[...].astype(jnp.float32).astype(jnp.bfloat16)
    own_ob.wait()
    for n in range(nz):
        for o in range(obs_local):
            v = jnp.log(obs_v[o, :, n * width : (n + 1) * width])
            obs_code[n, o] = jnp.round(v * CODE_SCALE + CODE_SHIFT).astype(jnp.int32).astype(jnp.int16)
    pl.semaphore_wait(barrier, len(peers))

    quarter = half_y // 2
    quarters = [pl.ds(pl.multiple_of(c * half_y + n * quarter, quarter), quarter) for n in range(2)]
    pk_cp = [
        pltpu.make_async_remote_copy(
            pk_own,
            pk_v.at[z],
            pk_send.at[t],
            pk_recv.at[t],
            device_id=to_z(t),
            device_id_type=MESH,
        )
        for t in range(nz - 1)
    ]
    al_cp = [
        [
            pltpu.make_async_remote_copy(
                al_bf.at[y, quarters[n]],
                al_bf.at[y, quarters[n]],
                al_send.at[t, m],
                al_recv.at[t, m],
                device_id={"bel": lax.rem(y + step, ny)},
                device_id_type=MESH,
            )
            for m, n in enumerate((t, 1 - t))
        ]
        for t, step in ((0, 1), (1, ny - 1))
    ]
    ob_cp = [
        pltpu.make_async_remote_copy(
            obs_code.at[z_at(t)],
            obs_all.at[z],
            ob_send.at[t],
            ob_recv.at[t],
            device_id=to_z(t),
            device_id_type=MESH,
        )
        for t in range(nz - 1)
    ]
    def trans_copy(t, which, send, recv):
        return pltpu.make_async_remote_copy(
            trans_hbm.at[which, :, pl.ds(pl.multiple_of(g_at(t) * qwidth, qwidth), qwidth)],
            t_blk.at[which, g_rows, :],
            send.at[t],
            recv.at[t],
            device_id=to_g(t),
            device_id_type=MESH,
        )

    ts_cp = [trans_copy(t, mine, ts_send, ts_recv) for t in range(ng - 1)]
    t_cp = [trans_copy(t, pl.ds(0, direct), t_send, t_recv) for t in range(ng - 1)]
    for cp in pk_cp:
        cp.start()
    own_al.wait()
    for m in range(2):
        for pair in al_cp:
            pair[m].start()
    for t in far_first(nz):
        ob_cp[t].start()
    for cp in ts_cp:
        cp.start()
    for cp in t_cp:
        cp.start()

    def spread_alpha(block, start, rows):
        def rows16(n, carry):
            r = pl.multiple_of(start + n * 16, 16)
            v = al_bf[block, pl.ds(r, 16), :].astype(jnp.float32)
            for h in range(halves):
                al_rows[pl.ds((block * rows_y + r) * halves + h, 16, stride=halves), :] = v[
                    :, h * LANES : (h + 1) * LANES
                ]
            return carry

        lax.fori_loop(0, rows // 16, rows16, 0, unroll=4)

    spread_alpha(y, 0, rows_y)

    for cp in pk_cp:
        cp.wait_recv()
    to_scalar = [
        [
            pltpu.make_async_copy(pk_v.at[n, o], pk_s[n][o], local_sem.at[8 + n * obs_local + o])
            for o in range(obs_local)
        ]
        for n in range(nz)
    ]
    for pair in to_scalar:
        for cp in pair:
            cp.start()

    totals = [jnp.zeros((actions, LANES), jnp.float32) for _ in range(halves)]

    def decode(code_ref, slot):
        for o in range(obs_local):
            v = jnp.exp(
                code_ref[slot, o].astype(jnp.int32).astype(jnp.float32) * (1.0 / CODE_SCALE)
            )
            for h in range(halves):
                part_h = v[:, h * LANES : (h + 1) * LANES]
                totals[h] = totals[h] + part_h
                obs_rows[pl.ds(slot * actions, actions), o * halves + h, :] = part_h

    decode(obs_code, z)
    share_cp = []

    def share(block, rows):
        cp = pltpu.make_async_remote_copy(
            al_bf.at[block, rows],
            al_bf.at[block, rows],
            share_send.at[len(share_cp)],
            share_recv.at[len(share_cp)],
            device_id={"obs_2": 1 - c},
            device_id_type=MESH,
        )
        cp.start()
        share_cp.append(cp)

    before, after, across = (lax.rem(y + n, ny) for n in (ny - 1, 1, ny - 2))
    relay_cp = []
    for t, (source, target) in enumerate(((before, after), (after, before))):
        al_cp[t][0].wait_recv()
        cp = pltpu.make_async_remote_copy(
            al_bf.at[source, quarters[t]],
            al_bf.at[source, quarters[t]],
            relay_send.at[t],
            relay_recv.at[t],
            device_id={"bel": target},
            device_id_type=MESH,
        )
        cp.start()
        relay_cp.append(cp)
    for t, source in enumerate((before, after)):
        share(source, quarters[t])
    for t, source in enumerate((before, after)):
        al_cp[t][1].wait_recv()
        share(source, quarters[1 - t])
    for source in (before, after):
        spread_alpha(source, c * half_y, half_y)
    for t in range(2):
        relay_cp[t].wait_recv()
        share(across, quarters[t])
    spread_alpha(across, c * half_y, half_y)
    for t in far_first(nz):
        ob_cp[t].wait_recv()
        decode(obs_all, lax.rem(z + nz - 1 - t, nz))
    for h in range(halves):
        tot_own[h] = totals[h]
    tot_cp = [
        pltpu.make_async_remote_copy(
            tot_own, tot_buf.at[t], tot_send.at[t], tot_recv.at[t], device_id=to_g(t), device_id_type=MESH
        )
        for t in range(ng - 1)
    ]
    for cp in tot_cp:
        cp.start()

    other = (1 - c) * half_y
    for cp, (source, n) in zip(
        share_cp, ((before, 0), (after, 1), (before, 1), (after, 0), (across, 0), (across, 1))
    ):
        cp.wait_recv()
        spread_alpha(source, other + n * quarter, quarter)
    own_ts.wait()
    for cp in ts_cp:
        cp.wait_recv()

    def trans_share(which, n, target):
        return pltpu.make_async_remote_copy(
            t_blk.at[which],
            t_blk.at[which],
            ty_send.at[n],
            ty_recv.at[n],
            device_id={"bel": target},
            device_id_type=MESH,
        )

    ty_cp = [trans_share(mine, n, to) for n, to in enumerate((across, after, before))]
    for cp in ty_cp:
        cp.start()
    for pair in to_scalar:
        for cp in pair:
            cp.wait()
    rs_cp = []
    for t in range(ng):
        j = g_at(t) if t < ng - 1 else g

        def one_belief(r, carry):
            b = j * own_rows + r
            a = act_s[b]
            sums = [None] * 4
            for n in range(nz):
                probs = obs_rows[n * actions + a]
                for o in range(obs_local):
                    term = al_rows[pl.ds(pk_s[n][o][0, b], halves), :] * probs[o * halves : (o + 1) * halves]
                    sums[o % 4] = term if n == 0 else sums[o % 4] + term
            part[pl.ds(pl.multiple_of(b * halves, halves), halves), :] = (sums[0] + sums[1]) + (
                sums[2] + sums[3]
            )
            return carry

        lax.fori_loop(0, own_rows, one_belief, 0, unroll=4)
        if t < ng - 1:
            rows = own_rows * halves
            cp = pltpu.make_async_remote_copy(
                part.at[pl.ds(pl.multiple_of(j * rows, rows), rows), :],
                rs_buf.at[t],
                rs_send.at[t],
                rs_recv.at[t],
                device_id=to_g(t),
                device_id_type=MESH,
            )
            cp.start()
            rs_cp.append(cp)

    for cp in tot_cp:
        cp.wait_recv()
    for cp in rs_cp:
        cp.wait_recv()
    act_own = act_i[pl.ds(pl.multiple_of(g * own_rows, own_rows), own_rows), :]
    values = []
    for h in range(halves):
        total = tot_own[h]
        for t in range(ng - 1):
            total = total + tot_buf[t, h]
        raw = part[pl.ds(g * own_rows * halves + h, own_rows, stride=halves), :]
        for t in range(ng - 1):
            raw = raw + rs_buf[t, pl.ds(h, own_rows, stride=halves), :]
        divisor = jnp.ones((own_rows, LANES), jnp.float32)
        for a in range(actions):
            divisor = jnp.where(act_own == a, total[a : a + 1, :], divisor)
        values.append(raw / divisor)
    coded, level = to_codes(values)
    for h in range(halves):
        cols = slice(h * LANES, (h + 1) * LANES)
        w_all[g, :own_rows, cols] = coded[h].astype(jnp.int16)
        w_all[g, own_rows:, cols] = level.astype(jnp.int16)

    w_cp = [
        pltpu.make_async_remote_copy(
            w_all.at[g], w_all.at[g], w_send.at[t], w_recv.at[t], device_id=to_g(t), device_id_type=MESH
        )
        for t in range(ng - 1)
    ]
    for cp in w_cp:
        cp.start()

    def spread_owner(j):
        rows = pl.ds(pl.multiple_of(j * own_rows, own_rows), own_rows)
        low_rows = pl.ds(pl.multiple_of(bel + j * own_rows, own_rows), own_rows)
        w_scale[rows, :] = jnp.broadcast_to(
            scale_of(w_all[j, own_rows : own_rows + 1, :].astype(jnp.int32).astype(jnp.float32)), (own_rows, width)
        )[:, :qwidth]
        act = act_b[rows, :]
        pieces = []
        for h in range(halves):
            q = w_all[j, :own_rows, h * LANES : (h + 1) * LANES].astype(jnp.int32)
            high = jnp.right_shift(q + 128, 8)
            low = q - jnp.left_shift(high, 8)
            pieces.append((high.astype(jnp.float32).astype(jnp.bfloat16), low.astype(jnp.float32).astype(jnp.bfloat16)))

        for a in range(actions):
            hot = act == jnp.asarray(a, jnp.bfloat16)
            for h in range(halves):
                high, low = pieces[h]
                cols = slice(a * width + h * LANES, a * width + (h + 1) * LANES)
                spread[rows, cols] = jnp.where(hot, high, jnp.zeros_like(high))
                spread[low_rows, cols] = jnp.where(hot, low, jnp.zeros_like(low))

    spread_owner(g)
    own_t.wait()
    for cp in t_cp:
        cp.wait_recv()
    for cp in ty_cp:
        cp.wait_recv()

    def total_action(a, carry):
        tt_own[pl.ds(a, 1), :] = jnp.sum(
            t_blk[a].astype(jnp.float32), axis=0, keepdims=True
        )
        return carry

    lax.fori_loop(0, actions, total_action, 0)
    tt_cp = [
        pltpu.make_async_remote_copy(
            tt_own, tt_buf.at[t], tt_send.at[t], tt_recv.at[t], device_id=to_z(t), device_id_type=MESH
        )
        for t in range(nz - 1)
    ]
    for cp in tt_cp:
        cp.start()

    for t in range(ng - 1):
        w_cp[t].wait_recv()
        spread_owner(g_from(t))
    both = jnp.dot(
        spread[...],
        t_blk[...].reshape(actions * width, qwidth),
        preferred_element_type=jnp.float32,
    )
    fut[...] = (256.0 * both[:bel] + both[bel:]) * w_scale[...]

    def send_future(j, t):
        rows = pl.ds(pl.multiple_of(j * z_rows, z_rows), z_rows)
        act = act_i[rows, :]
        values = []
        for h in range(qwidth // LANES):
            cols = slice(h * LANES, (h + 1) * LANES)
            divisor = jnp.ones((z_rows, LANES), jnp.float32)
            for a in range(actions):
                divisor = jnp.where(act == a, tt_all[a : a + 1, cols], divisor)
            values.append(fut[rows, cols] / divisor)
        coded, level = to_codes(values)
        for n in range(ng):
            parts = [code[n * last : (n + 1) * last] for code in coded]
            piece = jnp.concatenate(parts + [level[: PIECE - used]], axis=0)
            fut_q[t + 1, n] = piece.astype(jnp.int16)
        for u in range(-1, ng - 1):
            if t < 0 and u < 0:
                continue
            n = g if u < 0 else g_at(u)
            cp = pltpu.make_async_remote_copy(
                fut_q.at[t + 1, n, pl.ds(0, used + 2)],
                f_buf.at[t + 1, u + 1, pl.ds(0, used + 2)],
                f_send.at[t + 1, u + 1],
                f_recv.at[t + 1, u + 1],
                device_id={"obs_0": j, "obs_1": n // nc, "obs_2": lax.rem(n, nc)},
                device_id_type=MESH,
            )
            cp.start()
            f_cp.append(cp)

    for cp in tt_cp:
        cp.wait_recv()
    total = tt_own[...]
    for t in range(nz - 1):
        total = total + tt_buf[t]
    tt_all[...] = total
    f_cp = []
    for t in far_first(nz):
        send_future(z_at(t), t)
    send_future(z, -1)
    own_rew.wait()
    for r in range(last):
        rew_ref[r : r + 1, :] = rew_v[pl.ds(act_s[(z * ng + g) * last + r], 1), :]
    for cp in f_cp:
        cp.wait_recv()

    for u in range(ng):
        at = g if u == 0 else g_from(u - 1)
        future = None
        for t in range(nz):
            codes = fut_q[0, g] if u == 0 and t == 0 else f_buf[t, u]
            codes = codes.astype(jnp.int32).astype(jnp.float32)
            term = codes * scale_of(codes[used : used + 1])
            future = term if future is None else future + term
        for h in range(qwidth // LANES):
            out_ref[:, pl.ds(pl.multiple_of(at * qwidth + h * LANES, LANES), LANES)] = future[
                h * last : (h + 1) * last
            ]
    for cp in ob_cp + pk_cp + al_cp[0] + al_cp[1] + share_cp + ts_cp + ty_cp + t_cp + relay_cp + tot_cp + rs_cp + w_cp + f_cp + tt_cp:
        cp.wait_send()


def body(dims, alpha_set, transitions, obs_weights, rewards, chosen_idx, chosen_action):
    ny, nz, nx, nc = dims
    ng = nx * nc
    actions, states = rewards.shape
    bel = chosen_action.shape[0]
    obs_local = obs_weights.shape[0]
    width = states // nz
    qwidth = states // ng
    halves = width // LANES
    count = alpha_set.shape[0] * ny
    f32, b16, i32 = jnp.float32, jnp.bfloat16, jnp.int32
    dma = pltpu.SemaphoreType.DMA
    vmem = pl.BlockSpec(memory_space=pltpu.VMEM)
    hbm = pl.BlockSpec(memory_space=pl.ANY)
    z_rows = bel // nz
    own_rows = bel // ng
    scratch = [
        pltpu.VMEM((ny, count // ny, width), b16),
        pltpu.VMEM((count * halves, LANES), f32),
        pltpu.SMEM((bel,), i32),
        pltpu.VMEM((bel,), i32),
        pltpu.VMEM((actions, obs_local, bel), i32),
        pltpu.VMEM((bel, LANES), i32),
        pltpu.VMEM((bel, LANES), b16),
        pltpu.VMEM((obs_local, actions, states), f32),
        pltpu.VMEM((nz, obs_local, actions, width), jnp.int16),
        pltpu.VMEM((nz, obs_local, actions, width), jnp.int16),
        pltpu.VMEM((nz * actions, obs_local * halves, LANES), f32),
        pltpu.VMEM((obs_local, 1, bel), i32),
        pltpu.VMEM((nz, obs_local, 1, bel), i32),
        [[pltpu.SMEM((1, bel), i32) for _ in range(obs_local)] for _ in range(nz)],
        pltpu.VMEM((bel * halves, LANES), f32),
        pltpu.VMEM((ng - 1, own_rows * halves, LANES), f32),
        pltpu.VMEM((halves, actions, LANES), f32),
        pltpu.VMEM((ng - 1, halves, actions, LANES), f32),
        pltpu.VMEM((ng, own_rows + 8, width), jnp.int16),
        pltpu.VMEM((actions, width, qwidth), b16),
        pltpu.VMEM((2 * bel, actions * width), b16),
        pltpu.VMEM((bel, qwidth), f32),
        pltpu.VMEM((bel, qwidth), f32),
        pltpu.VMEM((nz, ng, PIECE, LANES), jnp.int16),
        pltpu.VMEM((nz, ng, PIECE, LANES), jnp.int16),
        pltpu.VMEM((actions, qwidth), f32),
        pltpu.VMEM((nz - 1, actions, qwidth), f32),
        pltpu.VMEM((actions, states), f32),
        pltpu.VMEM((actions, qwidth), f32),
        dma((8 + nz * obs_local,)),
        dma((nz - 1,)),
        dma((nz - 1,)),
        dma((2, 2)),
        dma((2, 2)),
        dma((2,)),
        dma((2,)),
        dma((6,)),
        dma((6,)),
        dma((nz - 1,)),
        dma((nz - 1,)),
        dma((ng - 1,)),
        dma((ng - 1,)),
        dma((ng - 1,)),
        dma((ng - 1,)),
        dma((ny - 1,)),
        dma((ny - 1,)),
        dma((ng - 1,)),
        dma((ng - 1,)),
        dma((ng - 1,)),
        dma((ng - 1,)),
        dma((ng - 1,)),
        dma((ng - 1,)),
        dma((nz, ng)),
        dma((nz, ng)),
        dma((nz - 1,)),
        dma((nz - 1,)),
    ]
    rows = pltpu.VMEM((bel // (nz * ng), states), f32)
    future, reward = pl.pallas_call(
        functools.partial(kernel, dims),
        out_shape=(rows, rows),
        in_specs=[
            hbm,
            hbm,
            hbm,
            hbm,
            hbm,
            hbm,
        ],
        out_specs=(vmem, vmem),
        scratch_shapes=scratch,
        compiler_params=pltpu.CompilerParams(
            collective_id=0, has_side_effects=True, vmem_limit_bytes=60 * 1024 * 1024
        ),
        name="backup",
    )(
        chosen_action,
        jnp.transpose(chosen_idx, (1, 2, 0)),
        alpha_set,
        transitions,
        obs_weights,
        rewards,
    )
    return reward + DISCOUNT * future


def solution(mesh):
    dims = (mesh.shape["bel"], 8, 4, 2)
    torus = Mesh(
        mesh.devices.reshape(*dims[1:], dims[0]), ("obs_0", "obs_1", "obs_2", "bel")
    )
    return jax.shard_map(
        functools.partial(body, dims),
        mesh=torus,
        in_specs=(
            P("bel", None),
            P(None, OBS, None),
            P(OBS, None, None),
            P(),
            P("bel", None, OBS),
            P("bel"),
        ),
        out_specs=P(BEL_OBS, None),
        check_vma=False,
    )
```

```python
import functools

import jax
import jax.numpy as jnp
from jax import lax
from jax.experimental import pallas as pl
from jax.experimental.pallas import tpu as pltpu
from jax.sharding import Mesh
from jax.sharding import PartitionSpec as P

OBS = ("obs_0", "obs_1", "obs_2")
BEL_OBS = ("bel", "obs_0", "obs_1", "obs_2")
LANES = 128
PIECE = 16
DISCOUNT = 0.95
CODE_SCALE = 14114.0
CODE_SHIFT = 2.302585093 * CODE_SCALE
MESH = pl.DeviceIdType.MESH


def to_codes(values):
    largest = functools.reduce(
        jnp.maximum, [jnp.max(jnp.abs(v), axis=(0, 1), keepdims=True) for v in values]
    )
    level = jnp.ceil(32.0 * jnp.log(jnp.maximum(largest, 1e-30) * (1.0 / 32760.0)))
    inverse = jnp.exp(level * (-1.0 / 32.0))
    coded = [
        jnp.clip(jnp.round(v * inverse), -32767.0, 32767.0).astype(jnp.int32)
        for v in values
    ]
    return coded, jnp.broadcast_to(level, (8, LANES)).astype(jnp.int32)


def scale_of(level):
    return jnp.exp(level * (1.0 / 32.0))


def far_first(n):
    return sorted(range(n - 1), key=lambda t: -min(t + 1, n - 1 - t))


def group_offsets(nx, nc):
    steps = [(dx, dc) for dx in range(nx) for dc in range(nc) if dx or dc]
    return sorted(steps, key=lambda step: -min(step[0], nx - step[0]))


def kernel(
    dims,
    act_hbm,
    idx_hbm,
    alpha_hbm,
    trans_hbm,
    obs_hbm,
    rew_hbm,
    out_ref,
    rew_ref,
    al_bf,
    al_rows,
    act_s,
    act_v,
    idx_v,
    act_i,
    act_b,
    obs_v,
    obs_code,
    obs_all,
    obs_rows,
    pk_own,
    pk_v,
    pk_s,
    part,
    rs_buf,
    tot_own,
    tot_buf,
    w_all,
    t_blk,
    spread,
    w_scale,
    fut,
    fut_q,
    f_buf,
    tt_share,
    tt_own,
    tt_buf,
    rew_v,
    tt_all,
    local_sem,
    pk_send,
    pk_recv,
    al_send,
    al_recv,
    relay_send,
    relay_recv,
    share_send,
    share_recv,
    ob_send,
    ob_recv,
    t_send,
    t_recv,
    ts_send,
    ts_recv,
    ty_send,
    ty_recv,
    tp_send,
    tp_recv,
    tot_send,
    tot_recv,
    rs_send,
    rs_recv,
    w_send,
    w_recv,
    f_send,
    f_recv,
    tt_send,
    tt_recv,
):
    ny, nz, nx, nc = dims
    ng = nx * nc
    actions = t_blk.shape[0]
    width = t_blk.shape[1]
    qwidth = t_blk.shape[2]
    halves = width // LANES
    bel = fut.shape[0]
    own_rows = bel // ng
    z_rows = bel // nz
    rows_y = alpha_hbm.shape[0]
    half_y = rows_y // nc
    obs_local = obs_hbm.shape[0]
    t_rows = trans_hbm.shape[1]
    last = out_ref.shape[0]
    used = last * (qwidth // LANES)
    per_y = actions // (2 * ny)
    direct = actions - per_y * ny

    y = lax.axis_index("bel")
    z = lax.axis_index("obs_0")
    x = lax.axis_index("obs_1")
    c = lax.axis_index("obs_2")
    g = x * nc + c

    def y_at(t):
        return lax.rem(y + 1 + t, ny)

    def z_at(t):
        return lax.rem(z + 1 + t, nz)

    offsets = group_offsets(nx, nc)

    def g_at(t):
        dx, dc = offsets[t]
        return lax.rem(x + dx, nx) * nc + lax.rem(c + dc, nc)

    def g_from(t):
        dx, dc = offsets[t]
        return lax.rem(x + nx - dx, nx) * nc + lax.rem(c + nc - dc, nc)

    def to_y(t):
        return {"bel": y_at(t)}

    def to_z(t):
        return {"obs_0": z_at(t)}

    def to_g(t):
        j = g_at(t)
        return {"obs_1": j // nc, "obs_2": lax.rem(j, nc)}

    peers = (
        [to_y(t) for t in range(ny - 1)]
        + [to_z(t) for t in range(nz - 1)]
        + [to_g(t) for t in range(ng - 1)]
    )
    barrier = pltpu.get_barrier_semaphore()
    for peer in peers:
        pl.semaphore_signal(barrier, inc=1, device_id=peer, device_id_type=MESH)

    z_cols = pl.ds(pl.multiple_of(z * width, width), width)
    q_cols = pl.ds(pl.multiple_of(g * qwidth, qwidth), qwidth)

    own_al = pltpu.make_async_copy(alpha_hbm.at[:, z_cols], al_bf.at[y], local_sem.at[7])
    own_ob = pltpu.make_async_copy(obs_hbm, obs_v, local_sem.at[2])
    g_rows = pl.ds(pl.multiple_of(g * t_rows, t_rows), t_rows)
    mine = pl.ds(direct + y * per_y, per_y)
    own_t = pltpu.make_async_copy(
        trans_hbm.at[:direct, :, q_cols], t_blk.at[:direct, g_rows, :], local_sem.at[3]
    )
    own_ts = pltpu.make_async_copy(
        trans_hbm.at[mine, :, q_cols], t_blk.at[mine, g_rows, :], local_sem.at[0]
    )
    own_rew = pltpu.make_async_copy(rew_hbm, rew_v, local_sem.at[4])
    own_act = [
        pltpu.make_async_copy(act_hbm, act_s, local_sem.at[1]),
        pltpu.make_async_copy(act_hbm, act_v, local_sem.at[5]),
        pltpu.make_async_copy(idx_hbm, idx_v, local_sem.at[6]),
    ]
    for cp in own_act:
        cp.start()
    own_ob.start()
    own_al.start()
    own_t.start()
    own_ts.start()
    own_rew.start()

    for cp in own_act:
        cp.wait()
    act_row = act_v[...].reshape(1, bel)
    picks = jnp.zeros((obs_local, bel), jnp.int32)
    for a in range(actions):
        picks = jnp.where(act_row == a, idx_v[a] * halves, picks)
    for o in range(obs_local):
        pk_own[o] = picks[o : o + 1, :]
        pk_v[z, o] = picks[o : o + 1, :]

    def fill_action(b, carry):
        act_i[pl.ds(b, 1), :] = jnp.full((1, LANES), act_s[b], jnp.int32)
        return carry

    lax.fori_loop(0, bel, fill_action, 0, unroll=8)
    act_b[...] = act_i[...].astype(jnp.float32).astype(jnp.bfloat16)
    own_ob.wait()
    for n in range(nz):
        for o in range(obs_local):
            v = jnp.log(obs_v[o, :, n * width : (n + 1) * width])
            obs_code[n, o] = jnp.round(v * CODE_SCALE + CODE_SHIFT).astype(jnp.int32).astype(jnp.int16)
    pl.semaphore_wait(barrier, len(peers))

    quarter = half_y // 2
    quarters = [pl.ds(pl.multiple_of(c * half_y + n * quarter, quarter), quarter) for n in range(2)]
    pk_cp = [
        pltpu.make_async_remote_copy(
            pk_own,
            pk_v.at[z],
            pk_send.at[t],
            pk_recv.at[t],
            device_id=to_z(t),
            device_id_type=MESH,
        )
        for t in range(nz - 1)
    ]
    al_cp = [
        [
            pltpu.make_async_remote_copy(
                al_bf.at[y, quarters[n]],
                al_bf.at[y, quarters[n]],
                al_send.at[t, m],
                al_recv.at[t, m],
                device_id={"bel": lax.rem(y + step, ny)},
                device_id_type=MESH,
            )
            for m, n in enumerate((t, 1 - t))
        ]
        for t, step in ((0, 1), (1, ny - 1))
    ]
    ob_cp = [
        pltpu.make_async_remote_copy(
            obs_code.at[z_at(t)],
            obs_all.at[z],
            ob_send.at[t],
            ob_recv.at[t],
            device_id=to_z(t),
            device_id_type=MESH,
        )
        for t in range(nz - 1)
    ]
    def trans_copy(t, which, send, recv):
        return pltpu.make_async_remote_copy(
            trans_hbm.at[which, :, pl.ds(pl.multiple_of(g_at(t) * qwidth, qwidth), qwidth)],
            t_blk.at[which, g_rows, :],
            send.at[t],
            recv.at[t],
            device_id=to_g(t),
            device_id_type=MESH,
        )

    ts_cp = [trans_copy(t, mine, ts_send, ts_recv) for t in range(ng - 1)]
    t_cp = [trans_copy(t, pl.ds(0, direct), t_send, t_recv) for t in range(ng - 1)]
    for cp in pk_cp:
        cp.start()
    own_al.wait()
    across = lax.rem(y + ny - 2, ny)
    relay_cp = [
        pltpu.make_async_remote_copy(
            al_bf.at[y, quarters[n]],
            al_bf.at[y, quarters[n]],
            relay_send.at[n],
            relay_recv.at[n],
            device_id={"bel": across},
            device_id_type=MESH,
        )
        for n in range(2)
    ]
    for m in range(2):
        relay_cp[m].start()
        for pair in al_cp:
            pair[m].start()
    for t in far_first(nz):
        ob_cp[t].start()
    for cp in ts_cp:
        cp.start()
    for cp in t_cp:
        cp.start()

    def spread_alpha(block, start, rows):
        def rows16(n, carry):
            r = pl.multiple_of(start + n * 16, 16)
            v = al_bf[block, pl.ds(r, 16), :].astype(jnp.float32)
            for h in range(halves):
                al_rows[pl.ds((block * rows_y + r) * halves + h, 16, stride=halves), :] = v[
                    :, h * LANES : (h + 1) * LANES
                ]
            return carry

        lax.fori_loop(0, rows // 16, rows16, 0, unroll=4)

    spread_alpha(y, 0, rows_y)

    for cp in pk_cp:
        cp.wait_recv()
    to_scalar = [
        [
            pltpu.make_async_copy(pk_v.at[n, o], pk_s[n][o], local_sem.at[8 + n * obs_local + o])
            for o in range(obs_local)
        ]
        for n in range(nz)
    ]
    for pair in to_scalar:
        for cp in pair:
            cp.start()

    totals = [jnp.zeros((actions, LANES), jnp.float32) for _ in range(halves)]

    def decode(code_ref, slot):
        for o in range(obs_local):
            v = jnp.exp(
                code_ref[slot, o].astype(jnp.int32).astype(jnp.float32) * (1.0 / CODE_SCALE)
            )
            for h in range(halves):
                part_h = v[:, h * LANES : (h + 1) * LANES]
                totals[h] = totals[h] + part_h
                obs_rows[pl.ds(slot * actions, actions), o * halves + h, :] = part_h

    decode(obs_code, z)
    share_cp = []

    def share(block, rows):
        cp = pltpu.make_async_remote_copy(
            al_bf.at[block, rows],
            al_bf.at[block, rows],
            share_send.at[len(share_cp)],
            share_recv.at[len(share_cp)],
            device_id={"obs_2": 1 - c},
            device_id_type=MESH,
        )
        cp.start()
        share_cp.append(cp)

    before, after, across = (lax.rem(y + n, ny) for n in (ny - 1, 1, ny - 2))
    for t, source in enumerate((before, after)):
        al_cp[t][0].wait_recv()
        share(source, quarters[t])
    for t, source in enumerate((before, after)):
        al_cp[t][1].wait_recv()
        share(source, quarters[1 - t])
    for source in (before, after):
        spread_alpha(source, c * half_y, half_y)
    for t in range(2):
        relay_cp[t].wait_recv()
        share(across, quarters[t])
    spread_alpha(across, c * half_y, half_y)
    for t in far_first(nz):
        ob_cp[t].wait_recv()
        decode(obs_all, lax.rem(z + nz - 1 - t, nz))
    for h in range(halves):
        tot_own[h] = totals[h]
    tot_cp = [
        pltpu.make_async_remote_copy(
            tot_own, tot_buf.at[t], tot_send.at[t], tot_recv.at[t], device_id=to_g(t), device_id_type=MESH
        )
        for t in range(ng - 1)
    ]
    for cp in tot_cp:
        cp.start()

    other = (1 - c) * half_y
    for cp, (source, n) in zip(
        share_cp, ((before, 0), (after, 1), (before, 1), (after, 0), (across, 0), (across, 1))
    ):
        cp.wait_recv()
        spread_alpha(source, other + n * quarter, quarter)
    own_ts.wait()
    for cp in ts_cp:
        cp.wait_recv()

    def trans_total(a):
        return jnp.sum(t_blk[a].astype(jnp.float32), axis=0, keepdims=True)

    for n in range(per_y):
        tt_share[y, n : n + 1, :] = trans_total(direct + y * per_y + n)
    tp_cp = [
        pltpu.make_async_remote_copy(
            tt_share.at[y],
            tt_share.at[y],
            tp_send.at[n],
            tp_recv.at[n],
            device_id={"bel": to},
            device_id_type=MESH,
        )
        for n, to in enumerate((across, after, before))
    ]
    for cp in tp_cp:
        cp.start()

    def trans_share(which, n, target):
        return pltpu.make_async_remote_copy(
            t_blk.at[which],
            t_blk.at[which],
            ty_send.at[n],
            ty_recv.at[n],
            device_id={"bel": target},
            device_id_type=MESH,
        )

    ty_cp = [trans_share(mine, n, to) for n, to in enumerate((across, after, before))]
    for cp in ty_cp:
        cp.start()
    for pair in to_scalar:
        for cp in pair:
            cp.wait()
    rs_cp = []
    for t in range(ng):
        j = g_at(t) if t < ng - 1 else g

        def one_belief(r, carry):
            b = j * own_rows + r
            a = act_s[b]
            sums = [None] * 4
            for n in range(nz):
                probs = obs_rows[n * actions + a]
                for o in range(obs_local):
                    term = al_rows[pl.ds(pk_s[n][o][0, b], halves), :] * probs[o * halves : (o + 1) * halves]
                    sums[o % 4] = term if n == 0 else sums[o % 4] + term
            part[pl.ds(pl.multiple_of(b * halves, halves), halves), :] = (sums[0] + sums[1]) + (
                sums[2] + sums[3]
            )
            return carry

        lax.fori_loop(0, own_rows, one_belief, 0, unroll=4)
        if t < ng - 1:
            rows = own_rows * halves
            cp = pltpu.make_async_remote_copy(
                part.at[pl.ds(pl.multiple_of(j * rows, rows), rows), :],
                rs_buf.at[t],
                rs_send.at[t],
                rs_recv.at[t],
                device_id=to_g(t),
                device_id_type=MESH,
            )
            cp.start()
            rs_cp.append(cp)

    for cp in tot_cp:
        cp.wait_recv()
    for cp in rs_cp:
        cp.wait_recv()
    act_own = act_i[pl.ds(pl.multiple_of(g * own_rows, own_rows), own_rows), :]
    values = []
    for h in range(halves):
        total = tot_own[h]
        for t in range(ng - 1):
            total = total + tot_buf[t, h]
        raw = part[pl.ds(g * own_rows * halves + h, own_rows, stride=halves), :]
        for t in range(ng - 1):
            raw = raw + rs_buf[t, pl.ds(h, own_rows, stride=halves), :]
        divisor = jnp.ones((own_rows, LANES), jnp.float32)
        for a in range(actions):
            divisor = jnp.where(act_own == a, total[a : a + 1, :], divisor)
        values.append(raw / divisor)
    coded, level = to_codes(values)
    for h in range(halves):
        cols = slice(h * LANES, (h + 1) * LANES)
        w_all[g, :own_rows, cols] = coded[h].astype(jnp.int16)
        w_all[g, own_rows:, cols] = level.astype(jnp.int16)

    w_cp = [
        pltpu.make_async_remote_copy(
            w_all.at[g], w_all.at[g], w_send.at[t], w_recv.at[t], device_id=to_g(t), device_id_type=MESH
        )
        for t in range(ng - 1)
    ]
    for cp in w_cp:
        cp.start()

    def spread_owner(j):
        rows = pl.ds(pl.multiple_of(j * own_rows, own_rows), own_rows)
        low_rows = pl.ds(pl.multiple_of(bel + j * own_rows, own_rows), own_rows)
        w_scale[rows, :] = jnp.broadcast_to(
            scale_of(w_all[j, own_rows : own_rows + 1, :].astype(jnp.int32).astype(jnp.float32)), (own_rows, width)
        )[:, :qwidth]
        act = act_b[rows, :]
        pieces = []
        for h in range(halves):
            q = w_all[j, :own_rows, h * LANES : (h + 1) * LANES].astype(jnp.int32)
            high = jnp.right_shift(q + 128, 8)
            low = q - jnp.left_shift(high, 8)
            pieces.append((high.astype(jnp.float32).astype(jnp.bfloat16), low.astype(jnp.float32).astype(jnp.bfloat16)))

        for a in range(actions):
            hot = act == jnp.asarray(a, jnp.bfloat16)
            for h in range(halves):
                high, low = pieces[h]
                cols = slice(a * width + h * LANES, a * width + (h + 1) * LANES)
                spread[rows, cols] = jnp.where(hot, high, jnp.zeros_like(high))
                spread[low_rows, cols] = jnp.where(hot, low, jnp.zeros_like(low))

    spread_owner(g)
    own_t.wait()
    for cp in t_cp:
        cp.wait_recv()

    def total_action(a, carry):
        tt_own[pl.ds(a, 1), :] = trans_total(a)
        return carry

    lax.fori_loop(0, direct, total_action, 0)
    for cp in tp_cp:
        cp.wait_recv()
    for n in range(ny):
        tt_own[direct + n * per_y : direct + (n + 1) * per_y, :] = tt_share[n]
    tt_cp = [
        pltpu.make_async_remote_copy(
            tt_own, tt_buf.at[t], tt_send.at[t], tt_recv.at[t], device_id=to_z(t), device_id_type=MESH
        )
        for t in range(nz - 1)
    ]
    for cp in tt_cp:
        cp.start()

    for t in range(ng - 1):
        w_cp[t].wait_recv()
        spread_owner(g_from(t))
    for cp in ty_cp:
        cp.wait_recv()
    both = jnp.dot(
        spread[...],
        t_blk[...].reshape(actions * width, qwidth),
        preferred_element_type=jnp.float32,
    )
    fut[...] = (256.0 * both[:bel] + both[bel:]) * w_scale[...]

    def send_future(j, t):
        rows = pl.ds(pl.multiple_of(j * z_rows, z_rows), z_rows)
        act = act_i[rows, :]
        values = []
        for h in range(qwidth // LANES):
            cols = slice(h * LANES, (h + 1) * LANES)
            divisor = jnp.ones((z_rows, LANES), jnp.float32)
            for a in range(actions):
                divisor = jnp.where(act == a, tt_all[a : a + 1, cols], divisor)
            values.append(fut[rows, cols] / divisor)
        coded, level = to_codes(values)
        for n in range(ng):
            parts = [code[n * last : (n + 1) * last] for code in coded]
            piece = jnp.concatenate(parts + [level[: PIECE - used]], axis=0)
            fut_q[t + 1, n] = piece.astype(jnp.int16)
        for u in range(-1, ng - 1):
            if t < 0 and u < 0:
                continue
            n = g if u < 0 else g_at(u)
            cp = pltpu.make_async_remote_copy(
                fut_q.at[t + 1, n, pl.ds(0, used + 2)],
                f_buf.at[t + 1, u + 1, pl.ds(0, used + 2)],
                f_send.at[t + 1, u + 1],
                f_recv.at[t + 1, u + 1],
                device_id={"obs_0": j, "obs_1": n // nc, "obs_2": lax.rem(n, nc)},
                device_id_type=MESH,
            )
            cp.start()
            f_cp.append(cp)

    for cp in tt_cp:
        cp.wait_recv()
    total = tt_own[...]
    for t in range(nz - 1):
        total = total + tt_buf[t]
    tt_all[...] = total
    f_cp = []
    for t in far_first(nz):
        send_future(z_at(t), t)
    send_future(z, -1)
    own_rew.wait()
    for r in range(last):
        rew_ref[r : r + 1, :] = rew_v[pl.ds(act_s[(z * ng + g) * last + r], 1), :]
    for cp in f_cp:
        cp.wait_recv()

    for u in range(ng):
        at = g if u == 0 else g_from(u - 1)
        future = None
        for t in range(nz):
            codes = fut_q[0, g] if u == 0 and t == 0 else f_buf[t, u]
            codes = codes.astype(jnp.int32).astype(jnp.float32)
            term = codes * scale_of(codes[used : used + 1])
            future = term if future is None else future + term
        for h in range(qwidth // LANES):
            out_ref[:, pl.ds(pl.multiple_of(at * qwidth + h * LANES, LANES), LANES)] = future[
                h * last : (h + 1) * last
            ]
    for cp in ob_cp + pk_cp + al_cp[0] + al_cp[1] + share_cp + ts_cp + tp_cp + ty_cp + t_cp + relay_cp + tot_cp + rs_cp + w_cp + f_cp + tt_cp:
        cp.wait_send()


def body(dims, alpha_set, transitions, obs_weights, rewards, chosen_idx, chosen_action):
    ny, nz, nx, nc = dims
    ng = nx * nc
    actions, states = rewards.shape
    bel = chosen_action.shape[0]
    obs_local = obs_weights.shape[0]
    width = states // nz
    qwidth = states // ng
    halves = width // LANES
    count = alpha_set.shape[0] * ny
    f32, b16, i32 = jnp.float32, jnp.bfloat16, jnp.int32
    dma = pltpu.SemaphoreType.DMA
    vmem = pl.BlockSpec(memory_space=pltpu.VMEM)
    hbm = pl.BlockSpec(memory_space=pl.ANY)
    z_rows = bel // nz
    own_rows = bel // ng
    scratch = [
        pltpu.VMEM((ny, count // ny, width), b16),
        pltpu.VMEM((count * halves, LANES), f32),
        pltpu.SMEM((bel,), i32),
        pltpu.VMEM((bel,), i32),
        pltpu.VMEM((actions, obs_local, bel), i32),
        pltpu.VMEM((bel, LANES), i32),
        pltpu.VMEM((bel, LANES), b16),
        pltpu.VMEM((obs_local, actions, states), f32),
        pltpu.VMEM((nz, obs_local, actions, width), jnp.int16),
        pltpu.VMEM((nz, obs_local, actions, width), jnp.int16),
        pltpu.VMEM((nz * actions, obs_local * halves, LANES), f32),
        pltpu.VMEM((obs_local, 1, bel), i32),
        pltpu.VMEM((nz, obs_local, 1, bel), i32),
        [[pltpu.SMEM((1, bel), i32) for _ in range(obs_local)] for _ in range(nz)],
        pltpu.VMEM((bel * halves, LANES), f32),
        pltpu.VMEM((ng - 1, own_rows * halves, LANES), f32),
        pltpu.VMEM((halves, actions, LANES), f32),
        pltpu.VMEM((ng - 1, halves, actions, LANES), f32),
        pltpu.VMEM((ng, own_rows + 8, width), jnp.int16),
        pltpu.VMEM((actions, width, qwidth), b16),
        pltpu.VMEM((2 * bel, actions * width), b16),
        pltpu.VMEM((bel, qwidth), f32),
        pltpu.VMEM((bel, qwidth), f32),
        pltpu.VMEM((nz, ng, PIECE, LANES), jnp.int16),
        pltpu.VMEM((nz, ng, PIECE, LANES), jnp.int16),
        pltpu.VMEM((dims[0], actions // (2 * dims[0]), qwidth), f32),
        pltpu.VMEM((actions, qwidth), f32),
        pltpu.VMEM((nz - 1, actions, qwidth), f32),
        pltpu.VMEM((actions, states), f32),
        pltpu.VMEM((actions, qwidth), f32),
        dma((8 + nz * obs_local,)),
        dma((nz - 1,)),
        dma((nz - 1,)),
        dma((2, 2)),
        dma((2, 2)),
        dma((2,)),
        dma((2,)),
        dma((6,)),
        dma((6,)),
        dma((nz - 1,)),
        dma((nz - 1,)),
        dma((ng - 1,)),
        dma((ng - 1,)),
        dma((ng - 1,)),
        dma((ng - 1,)),
        dma((ny - 1,)),
        dma((ny - 1,)),
        dma((ny - 1,)),
        dma((ny - 1,)),
        dma((ng - 1,)),
        dma((ng - 1,)),
        dma((ng - 1,)),
        dma((ng - 1,)),
        dma((ng - 1,)),
        dma((ng - 1,)),
        dma((nz, ng)),
        dma((nz, ng)),
        dma((nz - 1,)),
        dma((nz - 1,)),
    ]
    rows = pltpu.VMEM((bel // (nz * ng), states), f32)
    future, reward = pl.pallas_call(
        functools.partial(kernel, dims),
        out_shape=(rows, rows),
        in_specs=[
            hbm,
            hbm,
            hbm,
            hbm,
            hbm,
            hbm,
        ],
        out_specs=(vmem, vmem),
        scratch_shapes=scratch,
        compiler_params=pltpu.CompilerParams(
            collective_id=0, has_side_effects=True, vmem_limit_bytes=60 * 1024 * 1024
        ),
        name="backup",
    )(
        chosen_action,
        jnp.transpose(chosen_idx, (1, 2, 0)),
        alpha_set,
        transitions,
        obs_weights,
        rewards,
    )
    return reward + DISCOUNT * future


def solution(mesh):
    dims = (mesh.shape["bel"], 8, 4, 2)
    torus = Mesh(
        mesh.devices.reshape(*dims[1:], dims[0]), ("obs_0", "obs_1", "obs_2", "bel")
    )
    return jax.shard_map(
        functools.partial(body, dims),
        mesh=torus,
        in_specs=(
            P("bel", None),
            P(None, OBS, None),
            P(OBS, None, None),
            P(),
            P("bel", None, OBS),
            P("bel"),
        ),
        out_specs=P(BEL_OBS, None),
        check_vma=False,
    )
```

```python
import functools

import jax
import jax.numpy as jnp
from jax import lax
from jax.experimental import pallas as pl
from jax.experimental.pallas import tpu as pltpu
from jax.sharding import Mesh
from jax.sharding import PartitionSpec as P

OBS = ("obs_0", "obs_1", "obs_2")
BEL_OBS = ("bel", "obs_0", "obs_1", "obs_2")
LANES = 128
PIECE = 16
DISCOUNT = 0.95
CODE_SCALE = 14114.0
CODE_SHIFT = 2.302585093 * CODE_SCALE
MESH = pl.DeviceIdType.MESH


def to_codes(values):
    largest = functools.reduce(
        jnp.maximum, [jnp.max(jnp.abs(v), axis=(0, 1), keepdims=True) for v in values]
    )
    level = jnp.ceil(32.0 * jnp.log(jnp.maximum(largest, 1e-30) * (1.0 / 32760.0)))
    inverse = jnp.exp(level * (-1.0 / 32.0))
    coded = [
        jnp.clip(jnp.round(v * inverse), -32767.0, 32767.0).astype(jnp.int32)
        for v in values
    ]
    return coded, jnp.broadcast_to(level, (8, LANES)).astype(jnp.int32)


def scale_of(level):
    return jnp.exp(level * (1.0 / 32.0))


def far_first(n):
    return sorted(range(n - 1), key=lambda t: -min(t + 1, n - 1 - t))


def group_offsets(nx, nc):
    steps = [(dx, dc) for dx in range(nx) for dc in range(nc) if dx or dc]
    return sorted(steps, key=lambda step: -min(step[0], nx - step[0]))


def kernel(
    dims,
    act_hbm,
    idx_hbm,
    alpha_hbm,
    trans_hbm,
    obs_hbm,
    rew_hbm,
    out_ref,
    rew_ref,
    al_bf,
    al_rows,
    act_s,
    act_v,
    idx_v,
    act_i,
    act_b,
    obs_v,
    obs_code,
    obs_all,
    obs_rows,
    pk_own,
    pk_v,
    pk_s,
    part,
    sib_buf,
    rs_buf,
    tot_own,
    tot_buf,
    w_all,
    t_blk,
    spread,
    w_scale,
    fut,
    fut_q,
    f_buf,
    tt_share,
    tt_own,
    tt_buf,
    rew_v,
    tt_all,
    local_sem,
    pk_send,
    pk_recv,
    al_send,
    al_recv,
    relay_send,
    relay_recv,
    share_send,
    share_recv,
    ob_send,
    ob_recv,
    t_send,
    t_recv,
    ts_send,
    ts_recv,
    ty_send,
    ty_recv,
    tp_send,
    tp_recv,
    tot_send,
    tot_recv,
    rs_send,
    rs_recv,
    w_send,
    w_recv,
    f_send,
    f_recv,
    tt_send,
    tt_recv,
):
    ny, nz, nx, nc = dims
    ng = nx * nc
    actions = t_blk.shape[0]
    width = t_blk.shape[1]
    qwidth = t_blk.shape[2]
    halves = width // LANES
    bel = fut.shape[0]
    own_rows = bel // ng
    z_rows = bel // nz
    rows_y = alpha_hbm.shape[0]
    half_y = rows_y // nc
    obs_local = obs_hbm.shape[0]
    t_rows = trans_hbm.shape[1]
    last = out_ref.shape[0]
    used = last * (qwidth // LANES)
    per_y = actions // (2 * ny)
    direct = actions - per_y * ny

    y = lax.axis_index("bel")
    z = lax.axis_index("obs_0")
    x = lax.axis_index("obs_1")
    c = lax.axis_index("obs_2")
    g = x * nc + c

    def y_at(t):
        return lax.rem(y + 1 + t, ny)

    def z_at(t):
        return lax.rem(z + 1 + t, nz)

    offsets = group_offsets(nx, nc)

    def g_at(t):
        dx, dc = offsets[t]
        return lax.rem(x + dx, nx) * nc + lax.rem(c + dc, nc)

    def g_from(t):
        dx, dc = offsets[t]
        return lax.rem(x + nx - dx, nx) * nc + lax.rem(c + nc - dc, nc)

    def to_y(t):
        return {"bel": y_at(t)}

    def to_z(t):
        return {"obs_0": z_at(t)}

    def to_g(t):
        j = g_at(t)
        return {"obs_1": j // nc, "obs_2": lax.rem(j, nc)}

    peers = (
        [to_y(t) for t in range(ny - 1)]
        + [to_z(t) for t in range(nz - 1)]
        + [to_g(t) for t in range(ng - 1)]
    )
    barrier = pltpu.get_barrier_semaphore()
    for peer in peers:
        pl.semaphore_signal(barrier, inc=1, device_id=peer, device_id_type=MESH)

    z_cols = pl.ds(pl.multiple_of(z * width, width), width)
    q_cols = pl.ds(pl.multiple_of(g * qwidth, qwidth), qwidth)

    own_al = pltpu.make_async_copy(alpha_hbm.at[:, z_cols], al_bf.at[y], local_sem.at[7])
    own_ob = pltpu.make_async_copy(obs_hbm, obs_v, local_sem.at[2])
    g_rows = pl.ds(pl.multiple_of(g * t_rows, t_rows), t_rows)
    mine = pl.ds(direct + y * per_y, per_y)
    own_t = pltpu.make_async_copy(
        trans_hbm.at[:direct, :, q_cols], t_blk.at[:direct, g_rows, :], local_sem.at[3]
    )
    own_ts = pltpu.make_async_copy(
        trans_hbm.at[mine, :, q_cols], t_blk.at[mine, g_rows, :], local_sem.at[0]
    )
    own_rew = pltpu.make_async_copy(rew_hbm, rew_v, local_sem.at[4])
    own_act = [
        pltpu.make_async_copy(act_hbm, act_s, local_sem.at[1]),
        pltpu.make_async_copy(act_hbm, act_v, local_sem.at[5]),
        pltpu.make_async_copy(idx_hbm, idx_v, local_sem.at[6]),
    ]
    for cp in own_act:
        cp.start()
    own_ob.start()
    own_al.start()
    own_t.start()
    own_ts.start()
    own_rew.start()

    for cp in own_act:
        cp.wait()
    act_row = act_v[...].reshape(1, bel)
    picks = jnp.zeros((obs_local, bel), jnp.int32)
    for a in range(actions):
        picks = jnp.where(act_row == a, idx_v[a] * halves, picks)
    for o in range(obs_local):
        pk_own[o] = picks[o : o + 1, :]
        pk_v[z, o] = picks[o : o + 1, :]

    own_ob.wait()
    for n in range(nz):
        for o in range(obs_local):
            v = jnp.log(obs_v[o, :, n * width : (n + 1) * width])
            obs_code[n, o] = jnp.round(v * CODE_SCALE + CODE_SHIFT).astype(jnp.int32).astype(jnp.int16)
    pl.semaphore_wait(barrier, len(peers))

    quarter = half_y // 2
    quarters = [pl.ds(pl.multiple_of(c * half_y + n * quarter, quarter), quarter) for n in range(2)]
    pk_cp = [
        pltpu.make_async_remote_copy(
            pk_own,
            pk_v.at[z],
            pk_send.at[t],
            pk_recv.at[t],
            device_id=to_z(t),
            device_id_type=MESH,
        )
        for t in range(nz - 1)
    ]
    al_cp = [
        [
            pltpu.make_async_remote_copy(
                al_bf.at[y, quarters[n]],
                al_bf.at[y, quarters[n]],
                al_send.at[t, m],
                al_recv.at[t, m],
                device_id={"bel": lax.rem(y + step, ny)},
                device_id_type=MESH,
            )
            for m, n in enumerate((t, 1 - t))
        ]
        for t, step in ((0, 1), (1, ny - 1))
    ]
    ob_cp = [
        pltpu.make_async_remote_copy(
            obs_code.at[z_at(t)],
            obs_all.at[z],
            ob_send.at[t],
            ob_recv.at[t],
            device_id=to_z(t),
            device_id_type=MESH,
        )
        for t in range(nz - 1)
    ]
    def trans_copy(t, which, send, recv):
        return pltpu.make_async_remote_copy(
            trans_hbm.at[which, :, pl.ds(pl.multiple_of(g_at(t) * qwidth, qwidth), qwidth)],
            t_blk.at[which, g_rows, :],
            send.at[t],
            recv.at[t],
            device_id=to_g(t),
            device_id_type=MESH,
        )

    ts_cp = [trans_copy(t, mine, ts_send, ts_recv) for t in range(ng - 1)]
    t_cp = [trans_copy(t, pl.ds(0, direct), t_send, t_recv) for t in range(ng - 1)]
    for cp in pk_cp:
        cp.start()
    own_al.wait()
    across = lax.rem(y + ny - 2, ny)
    relay_cp = [
        pltpu.make_async_remote_copy(
            al_bf.at[y, quarters[n]],
            al_bf.at[y, quarters[n]],
            relay_send.at[n],
            relay_recv.at[n],
            device_id={"bel": across},
            device_id_type=MESH,
        )
        for n in range(2)
    ]
    for m in range(2):
        relay_cp[m].start()
        for pair in al_cp:
            pair[m].start()
    for t in far_first(nz):
        ob_cp[t].start()
    for cp in ts_cp:
        cp.start()
    for cp in t_cp:
        cp.start()

    def spread_alpha(block, start, rows):
        def rows16(n, carry):
            r = pl.multiple_of(start + n * 16, 16)
            v = al_bf[block, pl.ds(r, 16), :].astype(jnp.float32)
            for h in range(halves):
                al_rows[pl.ds((block * rows_y + r) * halves + h, 16, stride=halves), :] = v[
                    :, h * LANES : (h + 1) * LANES
                ]
            return carry

        lax.fori_loop(0, rows // 16, rows16, 0, unroll=4)

    spread_alpha(y, 0, rows_y)

    def fill_action(b, carry):
        act_i[pl.ds(b, 1), :] = jnp.full((1, LANES), act_s[b], jnp.int32)
        return carry

    lax.fori_loop(0, bel, fill_action, 0, unroll=8)
    act_b[...] = act_i[...].astype(jnp.float32).astype(jnp.bfloat16)

    totals = [jnp.zeros((actions, LANES), jnp.float32) for _ in range(halves)]

    def decode(code_ref, slot):
        for o in range(obs_local):
            v = jnp.exp(
                code_ref[slot, o].astype(jnp.int32).astype(jnp.float32) * (1.0 / CODE_SCALE)
            )
            for h in range(halves):
                part_h = v[:, h * LANES : (h + 1) * LANES]
                totals[h] = totals[h] + part_h
                obs_rows[pl.ds(slot * actions, actions), o * halves + h, :] = part_h

    decode(obs_code, z)
    share_cp = []

    def share(block, rows):
        cp = pltpu.make_async_remote_copy(
            al_bf.at[block, rows],
            al_bf.at[block, rows],
            share_send.at[len(share_cp)],
            share_recv.at[len(share_cp)],
            device_id={"obs_2": 1 - c},
            device_id_type=MESH,
        )
        cp.start()
        share_cp.append(cp)

    before, after, across = (lax.rem(y + n, ny) for n in (ny - 1, 1, ny - 2))
    for t, source in enumerate((before, after)):
        al_cp[t][0].wait_recv()
        share(source, quarters[t])
    for t, source in enumerate((before, after)):
        al_cp[t][1].wait_recv()
        share(source, quarters[1 - t])
    for t in range(2):
        relay_cp[t].wait_recv()
        share(across, quarters[t])
    for cp in pk_cp:
        cp.wait_recv()
    to_scalar = [
        [
            pltpu.make_async_copy(pk_v.at[n, o], pk_s[n][o], local_sem.at[8 + n * obs_local + o])
            for o in range(obs_local)
        ]
        for n in range(nz)
    ]
    for pair in to_scalar:
        for cp in pair:
            cp.start()
    for source in (before, after):
        spread_alpha(source, c * half_y, half_y)
    spread_alpha(across, c * half_y, half_y)
    for t in far_first(nz):
        ob_cp[t].wait_recv()
        decode(obs_all, lax.rem(z + nz - 1 - t, nz))
    for h in range(halves):
        tot_own[h] = totals[h]
    tot_cp = [
        pltpu.make_async_remote_copy(
            tot_own, tot_buf.at[t], tot_send.at[t], tot_recv.at[t], device_id=to_g(t), device_id_type=MESH
        )
        for t in range(ng - 1)
    ]
    for cp in tot_cp:
        cp.start()

    other = (1 - c) * half_y
    for cp, (source, n) in zip(
        share_cp, ((before, 0), (after, 1), (before, 1), (after, 0), (across, 0), (across, 1))
    ):
        cp.wait_recv()
        spread_alpha(source, other + n * quarter, quarter)
    own_ts.wait()
    for cp in ts_cp:
        cp.wait_recv()

    def trans_total(a):
        return jnp.sum(t_blk[a].astype(jnp.float32), axis=0, keepdims=True)

    for n in range(per_y):
        tt_share[y, n : n + 1, :] = trans_total(direct + y * per_y + n)
    tp_cp = [
        pltpu.make_async_remote_copy(
            tt_share.at[y],
            tt_share.at[y],
            tp_send.at[n],
            tp_recv.at[n],
            device_id={"bel": to},
            device_id_type=MESH,
        )
        for n, to in enumerate((across, after, before))
    ]
    for cp in tp_cp:
        cp.start()

    def trans_share(which, n, target):
        return pltpu.make_async_remote_copy(
            t_blk.at[which],
            t_blk.at[which],
            ty_send.at[n],
            ty_recv.at[n],
            device_id={"bel": target},
            device_id_type=MESH,
        )

    ty_cp = [trans_share(mine, n, to) for n, to in enumerate((across, after, before))]
    for cp in ty_cp:
        cp.start()
    for pair in to_scalar:
        for cp in pair:
            cp.wait()
    rs_cp = []
    rows = own_rows * halves

    def part_rows(j):
        return pl.ds(pl.multiple_of(j * rows, rows), rows)

    def weigh(j):
        def one_belief(r, carry):
            b = j * own_rows + r
            a = act_s[b]
            sums = [None] * 4
            for n in range(nz):
                probs = obs_rows[n * actions + a]
                for o in range(obs_local):
                    term = al_rows[pl.ds(pk_s[n][o][0, b], halves), :] * probs[o * halves : (o + 1) * halves]
                    sums[o % 4] = term if n == 0 else sums[o % 4] + term
            part[pl.ds(pl.multiple_of(b * halves, halves), halves), :] = (sums[0] + sums[1]) + (
                sums[2] + sums[3]
            )
            return carry

        lax.fori_loop(0, own_rows, one_belief, 0, unroll=4)

    def send_part(j, landing, n, to):
        cp = pltpu.make_async_remote_copy(
            part.at[part_rows(j), :],
            landing,
            rs_send.at[n],
            rs_recv.at[n],
            device_id=to,
            device_id_type=MESH,
        )
        cp.start()
        rs_cp.append(cp)

    steps = sorted(range(1, nx), key=lambda d: -min(d, nx - d))
    for n, d in enumerate(steps):
        j = lax.rem(x + d, nx) * nc + (1 - c)
        weigh(j)
        send_part(j, sib_buf.at[n], n, {"obs_2": 1 - c})
    for n, d in enumerate(steps):
        j = lax.rem(x + d, nx) * nc + c
        weigh(j)
        rs_cp[n].wait_recv()
        part[part_rows(j), :] = part[part_rows(j), :] + sib_buf[n]
        send_part(j, rs_buf.at[n], nx - 1 + n, {"obs_1": lax.rem(x + d, nx)})
    weigh(x * nc + (1 - c))
    send_part(x * nc + (1 - c), rs_buf.at[nx - 1], ng - 2, {"obs_2": 1 - c})
    weigh(g)
    for cp in tot_cp:
        cp.wait_recv()
    for cp in rs_cp[nx - 1 :]:
        cp.wait_recv()
    act_own = act_i[pl.ds(pl.multiple_of(g * own_rows, own_rows), own_rows), :]
    values = []
    for h in range(halves):
        total = tot_own[h]
        for t in range(ng - 1):
            total = total + tot_buf[t, h]
        raw = part[pl.ds(g * own_rows * halves + h, own_rows, stride=halves), :]
        for t in range(nx):
            raw = raw + rs_buf[t, pl.ds(h, own_rows, stride=halves), :]
        divisor = jnp.ones((own_rows, LANES), jnp.float32)
        for a in range(actions):
            divisor = jnp.where(act_own == a, total[a : a + 1, :], divisor)
        values.append(raw / divisor)
    coded, level = to_codes(values)
    for h in range(halves):
        cols = slice(h * LANES, (h + 1) * LANES)
        w_all[g, :own_rows, cols] = coded[h].astype(jnp.int16)
        w_all[g, own_rows:, cols] = level.astype(jnp.int16)

    w_cp = [
        pltpu.make_async_remote_copy(
            w_all.at[g], w_all.at[g], w_send.at[t], w_recv.at[t], device_id=to_g(t), device_id_type=MESH
        )
        for t in range(ng - 1)
    ]
    for cp in w_cp:
        cp.start()

    def spread_owner(j):
        rows = pl.ds(pl.multiple_of(j * own_rows, own_rows), own_rows)
        low_rows = pl.ds(pl.multiple_of(bel + j * own_rows, own_rows), own_rows)
        w_scale[rows, :] = jnp.broadcast_to(
            scale_of(w_all[j, own_rows : own_rows + 1, :].astype(jnp.int32).astype(jnp.float32)), (own_rows, width)
        )[:, :qwidth]
        act = act_b[rows, :]
        pieces = []
        for h in range(halves):
            q = w_all[j, :own_rows, h * LANES : (h + 1) * LANES].astype(jnp.int32)
            high = jnp.right_shift(q + 128, 8)
            low = q - jnp.left_shift(high, 8)
            pieces.append((high.astype(jnp.float32).astype(jnp.bfloat16), low.astype(jnp.float32).astype(jnp.bfloat16)))

        for a in range(actions):
            hot = act == jnp.asarray(a, jnp.bfloat16)
            for h in range(halves):
                high, low = pieces[h]
                cols = slice(a * width + h * LANES, a * width + (h + 1) * LANES)
                spread[rows, cols] = jnp.where(hot, high, jnp.zeros_like(high))
                spread[low_rows, cols] = jnp.where(hot, low, jnp.zeros_like(low))

    spread_owner(g)
    own_t.wait()
    for cp in t_cp:
        cp.wait_recv()

    def total_action(a, carry):
        tt_own[pl.ds(a, 1), :] = trans_total(a)
        return carry

    lax.fori_loop(0, direct, total_action, 0)
    for cp in tp_cp:
        cp.wait_recv()
    for n in range(ny):
        tt_own[direct + n * per_y : direct + (n + 1) * per_y, :] = tt_share[n]
    tt_cp = [
        pltpu.make_async_remote_copy(
            tt_own, tt_buf.at[t], tt_send.at[t], tt_recv.at[t], device_id=to_z(t), device_id_type=MESH
        )
        for t in range(nz - 1)
    ]
    for cp in tt_cp:
        cp.start()

    for t in range(ng - 1):
        w_cp[t].wait_recv()
        spread_owner(g_from(t))
    for cp in ty_cp:
        cp.wait_recv()
    both = jnp.dot(
        spread[...],
        t_blk[...].reshape(actions * width, qwidth),
        preferred_element_type=jnp.float32,
    )
    fut[...] = (256.0 * both[:bel] + both[bel:]) * w_scale[...]

    def send_future(j, t):
        rows = pl.ds(pl.multiple_of(j * z_rows, z_rows), z_rows)
        act = act_i[rows, :]
        values = []
        for h in range(qwidth // LANES):
            cols = slice(h * LANES, (h + 1) * LANES)
            divisor = jnp.ones((z_rows, LANES), jnp.float32)
            for a in range(actions):
                divisor = jnp.where(act == a, tt_all[a : a + 1, cols], divisor)
            values.append(fut[rows, cols] / divisor)
        coded, level = to_codes(values)
        for n in range(ng):
            parts = [code[n * last : (n + 1) * last] for code in coded]
            piece = jnp.concatenate(parts + [level[: PIECE - used]], axis=0)
            fut_q[t + 1, n] = piece.astype(jnp.int16)
        for u in range(-1, ng - 1):
            if t < 0 and u < 0:
                continue
            n = g if u < 0 else g_at(u)
            cp = pltpu.make_async_remote_copy(
                fut_q.at[t + 1, n, pl.ds(0, used + 2)],
                f_buf.at[t + 1, u + 1, pl.ds(0, used + 2)],
                f_send.at[t + 1, u + 1],
                f_recv.at[t + 1, u + 1],
                device_id={"obs_0": j, "obs_1": n // nc, "obs_2": lax.rem(n, nc)},
                device_id_type=MESH,
            )
            cp.start()
            f_cp.append(cp)

    for cp in tt_cp:
        cp.wait_recv()
    total = tt_own[...]
    for t in range(nz - 1):
        total = total + tt_buf[t]
    tt_all[...] = total
    f_cp = []
    for t in far_first(nz):
        send_future(z_at(t), t)
    send_future(z, -1)
    own_rew.wait()
    for r in range(last):
        rew_ref[r : r + 1, :] = rew_v[pl.ds(act_s[(z * ng + g) * last + r], 1), :]
    for cp in f_cp:
        cp.wait_recv()

    for u in range(ng):
        at = g if u == 0 else g_from(u - 1)
        future = None
        for t in range(nz):
            codes = fut_q[0, g] if u == 0 and t == 0 else f_buf[t, u]
            codes = codes.astype(jnp.int32).astype(jnp.float32)
            term = codes * scale_of(codes[used : used + 1])
            future = term if future is None else future + term
        for h in range(qwidth // LANES):
            out_ref[:, pl.ds(pl.multiple_of(at * qwidth + h * LANES, LANES), LANES)] = future[
                h * last : (h + 1) * last
            ]
    for cp in ob_cp + pk_cp + al_cp[0] + al_cp[1] + share_cp + ts_cp + tp_cp + ty_cp + t_cp + relay_cp + tot_cp + rs_cp + w_cp + f_cp + tt_cp:
        cp.wait_send()


def body(dims, alpha_set, transitions, obs_weights, rewards, chosen_idx, chosen_action):
    ny, nz, nx, nc = dims
    ng = nx * nc
    actions, states = rewards.shape
    bel = chosen_action.shape[0]
    obs_local = obs_weights.shape[0]
    width = states // nz
    qwidth = states // ng
    halves = width // LANES
    count = alpha_set.shape[0] * ny
    f32, b16, i32 = jnp.float32, jnp.bfloat16, jnp.int32
    dma = pltpu.SemaphoreType.DMA
    vmem = pl.BlockSpec(memory_space=pltpu.VMEM)
    hbm = pl.BlockSpec(memory_space=pl.ANY)
    z_rows = bel // nz
    own_rows = bel // ng
    scratch = [
        pltpu.VMEM((ny, count // ny, width), b16),
        pltpu.VMEM((count * halves, LANES), f32),
        pltpu.SMEM((bel,), i32),
        pltpu.VMEM((bel,), i32),
        pltpu.VMEM((actions, obs_local, bel), i32),
        pltpu.VMEM((bel, LANES), i32),
        pltpu.VMEM((bel, LANES), b16),
        pltpu.VMEM((obs_local, actions, states), f32),
        pltpu.VMEM((nz, obs_local, actions, width), jnp.int16),
        pltpu.VMEM((nz, obs_local, actions, width), jnp.int16),
        pltpu.VMEM((nz * actions, obs_local * halves, LANES), f32),
        pltpu.VMEM((obs_local, 1, bel), i32),
        pltpu.VMEM((nz, obs_local, 1, bel), i32),
        [[pltpu.SMEM((1, bel), i32) for _ in range(obs_local)] for _ in range(nz)],
        pltpu.VMEM((bel * halves, LANES), f32),
        pltpu.VMEM((dims[2] - 1, own_rows * halves, LANES), f32),
        pltpu.VMEM((dims[2], own_rows * halves, LANES), f32),
        pltpu.VMEM((halves, actions, LANES), f32),
        pltpu.VMEM((ng - 1, halves, actions, LANES), f32),
        pltpu.VMEM((ng, own_rows + 8, width), jnp.int16),
        pltpu.VMEM((actions, width, qwidth), b16),
        pltpu.VMEM((2 * bel, actions * width), b16),
        pltpu.VMEM((bel, qwidth), f32),
        pltpu.VMEM((bel, qwidth), f32),
        pltpu.VMEM((nz, ng, PIECE, LANES), jnp.int16),
        pltpu.VMEM((nz, ng, PIECE, LANES), jnp.int16),
        pltpu.VMEM((dims[0], actions // (2 * dims[0]), qwidth), f32),
        pltpu.VMEM((actions, qwidth), f32),
        pltpu.VMEM((nz - 1, actions, qwidth), f32),
        pltpu.VMEM((actions, states), f32),
        pltpu.VMEM((actions, qwidth), f32),
        dma((8 + nz * obs_local,)),
        dma((nz - 1,)),
        dma((nz - 1,)),
        dma((2, 2)),
        dma((2, 2)),
        dma((2,)),
        dma((2,)),
        dma((6,)),
        dma((6,)),
        dma((nz - 1,)),
        dma((nz - 1,)),
        dma((ng - 1,)),
        dma((ng - 1,)),
        dma((ng - 1,)),
        dma((ng - 1,)),
        dma((ny - 1,)),
        dma((ny - 1,)),
        dma((ny - 1,)),
        dma((ny - 1,)),
        dma((ng - 1,)),
        dma((ng - 1,)),
        dma((ng - 1,)),
        dma((ng - 1,)),
        dma((ng - 1,)),
        dma((ng - 1,)),
        dma((nz, ng)),
        dma((nz, ng)),
        dma((nz - 1,)),
        dma((nz - 1,)),
    ]
    rows = pltpu.VMEM((bel // (nz * ng), states), f32)
    future, reward = pl.pallas_call(
        functools.partial(kernel, dims),
        out_shape=(rows, rows),
        in_specs=[
            hbm,
            hbm,
            hbm,
            hbm,
            hbm,
            hbm,
        ],
        out_specs=(vmem, vmem),
        scratch_shapes=scratch,
        compiler_params=pltpu.CompilerParams(
            collective_id=0, has_side_effects=True, vmem_limit_bytes=60 * 1024 * 1024
        ),
        name="backup",
    )(
        chosen_action,
        jnp.transpose(chosen_idx, (1, 2, 0)),
        alpha_set,
        transitions,
        obs_weights,
        rewards,
    )
    return reward + DISCOUNT * future


def solution(mesh):
    dims = (mesh.shape["bel"], 8, 4, 2)
    torus = Mesh(
        mesh.devices.reshape(*dims[1:], dims[0]), ("obs_0", "obs_1", "obs_2", "bel")
    )
    return jax.shard_map(
        functools.partial(body, dims),
        mesh=torus,
        in_specs=(
            P("bel", None),
            P(None, OBS, None),
            P(OBS, None, None),
            P(),
            P("bel", None, OBS),
            P("bel"),
        ),
        out_specs=P(BEL_OBS, None),
        check_vma=False,
    )
```

```python
import functools

import jax
import jax.numpy as jnp
from jax import lax
from jax.experimental import pallas as pl
from jax.experimental.pallas import tpu as pltpu
from jax.sharding import Mesh
from jax.sharding import PartitionSpec as P

OBS = ("obs_0", "obs_1", "obs_2")
BEL_OBS = ("bel", "obs_0", "obs_1", "obs_2")
LANES = 128
PIECE = 16
DISCOUNT = 0.95
CODE_SCALE = 14114.0
CODE_SHIFT = 2.302585093 * CODE_SCALE
MESH = pl.DeviceIdType.MESH


def to_codes(values):
    largest = functools.reduce(
        jnp.maximum, [jnp.max(jnp.abs(v), axis=(0, 1), keepdims=True) for v in values]
    )
    level = jnp.ceil(32.0 * jnp.log(jnp.maximum(largest, 1e-30) * (1.0 / 32760.0)))
    inverse = jnp.exp(level * (-1.0 / 32.0))
    coded = [
        jnp.clip(jnp.round(v * inverse), -32767.0, 32767.0).astype(jnp.int32)
        for v in values
    ]
    return coded, jnp.broadcast_to(level, (8, LANES)).astype(jnp.int32)


def scale_of(level):
    return jnp.exp(level * (1.0 / 32.0))


def far_first(n):
    return sorted(range(n - 1), key=lambda t: -min(t + 1, n - 1 - t))


def group_offsets(nx, nc):
    steps = [(dx, dc) for dx in range(nx) for dc in range(nc) if dx or dc]
    return sorted(steps, key=lambda step: -min(step[0], nx - step[0]))


def kernel(
    dims,
    act_hbm,
    idx_hbm,
    alpha_hbm,
    trans_hbm,
    obs_hbm,
    rew_hbm,
    out_ref,
    rew_ref,
    al_bf,
    al_rows,
    act_s,
    act_v,
    idx_v,
    act_i,
    act_b,
    obs_v,
    obs_code,
    obs_all,
    obs_rows,
    pk_own,
    pk_v,
    pk_s,
    part,
    sib_buf,
    rs_buf,
    tot_own,
    tot_buf,
    w_all,
    t_blk,
    spread,
    w_scale,
    fut,
    fut_q,
    f_buf,
    tt_share,
    tt_own,
    tt_buf,
    rew_v,
    tt_all,
    local_sem,
    pk_send,
    pk_recv,
    al_send,
    al_recv,
    relay_send,
    relay_recv,
    share_send,
    share_recv,
    ob_send,
    ob_recv,
    t_send,
    t_recv,
    ts_send,
    ts_recv,
    ty_send,
    ty_recv,
    tp_send,
    tp_recv,
    tot_send,
    tot_recv,
    rs_send,
    rs_recv,
    w_send,
    w_recv,
    f_send,
    f_recv,
    tt_send,
    tt_recv,
):
    ny, nz, nx, nc = dims
    ng = nx * nc
    actions = t_blk.shape[0]
    width = t_blk.shape[1]
    qwidth = t_blk.shape[2]
    halves = width // LANES
    bel = fut.shape[0]
    own_rows = bel // ng
    z_rows = bel // nz
    rows_y = alpha_hbm.shape[0]
    half_y = rows_y // nc
    obs_local = obs_hbm.shape[0]
    t_rows = trans_hbm.shape[1]
    last = out_ref.shape[0]
    used = last * (qwidth // LANES)
    per_y = actions // (2 * ny)
    direct = actions - per_y * ny

    y = lax.axis_index("bel")
    z = lax.axis_index("obs_0")
    x = lax.axis_index("obs_1")
    c = lax.axis_index("obs_2")
    g = x * nc + c

    def y_at(t):
        return lax.rem(y + 1 + t, ny)

    def z_at(t):
        return lax.rem(z + 1 + t, nz)

    offsets = group_offsets(nx, nc)

    def g_at(t):
        dx, dc = offsets[t]
        return lax.rem(x + dx, nx) * nc + lax.rem(c + dc, nc)

    def g_from(t):
        dx, dc = offsets[t]
        return lax.rem(x + nx - dx, nx) * nc + lax.rem(c + nc - dc, nc)

    def to_y(t):
        return {"bel": y_at(t)}

    def to_z(t):
        return {"obs_0": z_at(t)}

    def to_g(t):
        j = g_at(t)
        return {"obs_1": j // nc, "obs_2": lax.rem(j, nc)}

    peers = (
        [to_y(t) for t in range(ny - 1)]
        + [to_z(t) for t in range(nz - 1)]
        + [to_g(t) for t in range(ng - 1)]
    )
    barrier = pltpu.get_barrier_semaphore()
    for peer in peers:
        pl.semaphore_signal(barrier, inc=1, device_id=peer, device_id_type=MESH)

    z_cols = pl.ds(pl.multiple_of(z * width, width), width)
    q_cols = pl.ds(pl.multiple_of(g * qwidth, qwidth), qwidth)

    own_al = pltpu.make_async_copy(alpha_hbm.at[:, z_cols], al_bf.at[y], local_sem.at[7])
    own_ob = pltpu.make_async_copy(obs_hbm, obs_v, local_sem.at[2])
    g_rows = pl.ds(pl.multiple_of(g * t_rows, t_rows), t_rows)
    mine = pl.ds(direct + y * per_y, per_y)
    own_t = pltpu.make_async_copy(
        trans_hbm.at[:direct, :, q_cols], t_blk.at[:direct, g_rows, :], local_sem.at[3]
    )
    own_ts = pltpu.make_async_copy(
        trans_hbm.at[mine, :, q_cols], t_blk.at[mine, g_rows, :], local_sem.at[0]
    )
    own_rew = pltpu.make_async_copy(rew_hbm, rew_v, local_sem.at[4])
    own_act = [
        pltpu.make_async_copy(act_hbm, act_s, local_sem.at[1]),
        pltpu.make_async_copy(act_hbm, act_v, local_sem.at[5]),
        pltpu.make_async_copy(idx_hbm, idx_v, local_sem.at[6]),
    ]
    for cp in own_act:
        cp.start()
    own_ob.start()
    own_al.start()
    own_t.start()
    own_ts.start()
    own_rew.start()

    for cp in own_act:
        cp.wait()
    act_row = act_v[...].reshape(1, bel)
    picks = jnp.zeros((obs_local, bel), jnp.int32)
    for a in range(actions):
        picks = jnp.where(act_row == a, idx_v[a] * halves, picks)
    for o in range(obs_local):
        pk_own[o] = picks[o : o + 1, :]
        pk_v[z, o] = picks[o : o + 1, :]

    own_ob.wait()
    for n in range(nz):
        for o in range(obs_local):
            v = jnp.log(obs_v[o, :, n * width : (n + 1) * width])
            obs_code[n, o] = jnp.round(v * CODE_SCALE + CODE_SHIFT).astype(jnp.int32).astype(jnp.int16)
    pl.semaphore_wait(barrier, len(peers))

    quarter = half_y // 2
    quarters = [pl.ds(pl.multiple_of(c * half_y + n * quarter, quarter), quarter) for n in range(2)]
    pk_cp = [
        pltpu.make_async_remote_copy(
            pk_own,
            pk_v.at[z],
            pk_send.at[t],
            pk_recv.at[t],
            device_id=to_z(t),
            device_id_type=MESH,
        )
        for t in range(nz - 1)
    ]
    al_cp = [
        [
            pltpu.make_async_remote_copy(
                al_bf.at[y, quarters[n]],
                al_bf.at[y, quarters[n]],
                al_send.at[t, m],
                al_recv.at[t, m],
                device_id={"bel": lax.rem(y + step, ny)},
                device_id_type=MESH,
            )
            for m, n in enumerate((t, 1 - t))
        ]
        for t, step in ((0, 1), (1, ny - 1))
    ]
    ob_cp = [
        pltpu.make_async_remote_copy(
            obs_code.at[z_at(t)],
            obs_all.at[z],
            ob_send.at[t],
            ob_recv.at[t],
            device_id=to_z(t),
            device_id_type=MESH,
        )
        for t in range(nz - 1)
    ]
    def trans_copy(t, which, send, recv):
        return pltpu.make_async_remote_copy(
            trans_hbm.at[which, :, pl.ds(pl.multiple_of(g_at(t) * qwidth, qwidth), qwidth)],
            t_blk.at[which, g_rows, :],
            send.at[t],
            recv.at[t],
            device_id=to_g(t),
            device_id_type=MESH,
        )

    ts_cp = [trans_copy(t, mine, ts_send, ts_recv) for t in range(ng - 1)]
    t_cp = [trans_copy(t, pl.ds(0, direct), t_send, t_recv) for t in range(ng - 1)]
    for cp in pk_cp:
        cp.start()
    own_al.wait()
    across = lax.rem(y + ny - 2, ny)
    relay_cp = [
        pltpu.make_async_remote_copy(
            al_bf.at[y, quarters[n]],
            al_bf.at[y, quarters[n]],
            relay_send.at[n],
            relay_recv.at[n],
            device_id={"bel": across},
            device_id_type=MESH,
        )
        for n in range(2)
    ]
    for m in range(2):
        for pair in al_cp:
            pair[m].start()
    for m in range(2):
        relay_cp[m].start()
    for t in far_first(nz):
        ob_cp[t].start()
    for cp in ts_cp:
        cp.start()
    for cp in t_cp:
        cp.start()

    def spread_alpha(block, start, rows):
        def rows16(n, carry):
            r = pl.multiple_of(start + n * 16, 16)
            v = al_bf[block, pl.ds(r, 16), :].astype(jnp.float32)
            for h in range(halves):
                al_rows[pl.ds((block * rows_y + r) * halves + h, 16, stride=halves), :] = v[
                    :, h * LANES : (h + 1) * LANES
                ]
            return carry

        lax.fori_loop(0, rows // 16, rows16, 0, unroll=4)

    spread_alpha(y, 0, rows_y)

    def fill_action(b, carry):
        act_i[pl.ds(b, 1), :] = jnp.full((1, LANES), act_s[b], jnp.int32)
        return carry

    lax.fori_loop(0, bel, fill_action, 0, unroll=8)
    act_b[...] = act_i[...].astype(jnp.float32).astype(jnp.bfloat16)

    totals = [jnp.zeros((actions, LANES), jnp.float32) for _ in range(halves)]

    def decode(code_ref, slot):
        for o in range(obs_local):
            v = jnp.exp(
                code_ref[slot, o].astype(jnp.int32).astype(jnp.float32) * (1.0 / CODE_SCALE)
            )
            for h in range(halves):
                part_h = v[:, h * LANES : (h + 1) * LANES]
                totals[h] = totals[h] + part_h
                obs_rows[pl.ds(slot * actions, actions), o * halves + h, :] = part_h

    decode(obs_code, z)
    share_cp = []

    def share(block, rows):
        cp = pltpu.make_async_remote_copy(
            al_bf.at[block, rows],
            al_bf.at[block, rows],
            share_send.at[len(share_cp)],
            share_recv.at[len(share_cp)],
            device_id={"obs_2": 1 - c},
            device_id_type=MESH,
        )
        cp.start()
        share_cp.append(cp)

    before, after, across = (lax.rem(y + n, ny) for n in (ny - 1, 1, ny - 2))
    for t, source in enumerate((before, after)):
        al_cp[t][0].wait_recv()
        share(source, quarters[t])
    for t, source in enumerate((before, after)):
        al_cp[t][1].wait_recv()
        share(source, quarters[1 - t])
    for t in range(2):
        relay_cp[t].wait_recv()
        share(across, quarters[t])
    for cp in pk_cp:
        cp.wait_recv()
    to_scalar = [
        [
            pltpu.make_async_copy(pk_v.at[n, o], pk_s[n][o], local_sem.at[8 + n * obs_local + o])
            for o in range(obs_local)
        ]
        for n in range(nz)
    ]
    for pair in to_scalar:
        for cp in pair:
            cp.start()
    for source in (before, after):
        spread_alpha(source, c * half_y, half_y)
    spread_alpha(across, c * half_y, half_y)
    for t in far_first(nz):
        ob_cp[t].wait_recv()
        decode(obs_all, lax.rem(z + nz - 1 - t, nz))
    for h in range(halves):
        tot_own[h] = totals[h]
    tot_cp = [
        pltpu.make_async_remote_copy(
            tot_own, tot_buf.at[t], tot_send.at[t], tot_recv.at[t], device_id=to_g(t), device_id_type=MESH
        )
        for t in range(ng - 1)
    ]
    for cp in tot_cp:
        cp.start()

    other = (1 - c) * half_y
    for cp, (source, n) in zip(
        share_cp, ((before, 0), (after, 1), (before, 1), (after, 0), (across, 0), (across, 1))
    ):
        cp.wait_recv()
        spread_alpha(source, other + n * quarter, quarter)
    own_ts.wait()
    for cp in ts_cp:
        cp.wait_recv()

    def trans_total(a):
        return jnp.sum(t_blk[a].astype(jnp.float32), axis=0, keepdims=True)

    for n in range(per_y):
        tt_share[y, n : n + 1, :] = trans_total(direct + y * per_y + n)
    tp_cp = [
        pltpu.make_async_remote_copy(
            tt_share.at[y],
            tt_share.at[y],
            tp_send.at[n],
            tp_recv.at[n],
            device_id={"bel": to},
            device_id_type=MESH,
        )
        for n, to in enumerate((across, after, before))
    ]
    for cp in tp_cp:
        cp.start()

    def trans_share(which, n, target):
        return pltpu.make_async_remote_copy(
            t_blk.at[which],
            t_blk.at[which],
            ty_send.at[n],
            ty_recv.at[n],
            device_id={"bel": target},
            device_id_type=MESH,
        )

    ty_cp = [trans_share(mine, n, to) for n, to in enumerate((across, after, before))]
    for cp in ty_cp:
        cp.start()
    for pair in to_scalar:
        for cp in pair:
            cp.wait()
    rs_cp = []
    rows = own_rows * halves

    def part_rows(j):
        return pl.ds(pl.multiple_of(j * rows, rows), rows)

    def weigh(j):
        def one_belief(r, carry):
            b = j * own_rows + r
            a = act_s[b]
            sums = [None] * 4
            for n in range(nz):
                probs = obs_rows[n * actions + a]
                for o in range(obs_local):
                    term = al_rows[pl.ds(pk_s[n][o][0, b], halves), :] * probs[o * halves : (o + 1) * halves]
                    sums[o % 4] = term if n == 0 else sums[o % 4] + term
            part[pl.ds(pl.multiple_of(b * halves, halves), halves), :] = (sums[0] + sums[1]) + (
                sums[2] + sums[3]
            )
            return carry

        lax.fori_loop(0, own_rows, one_belief, 0, unroll=8)

    def send_part(j, landing, n, to):
        cp = pltpu.make_async_remote_copy(
            part.at[part_rows(j), :],
            landing,
            rs_send.at[n],
            rs_recv.at[n],
            device_id=to,
            device_id_type=MESH,
        )
        cp.start()
        rs_cp.append(cp)

    steps = sorted(range(1, nx), key=lambda d: -min(d, nx - d))
    for n, d in enumerate(steps):
        j = lax.rem(x + d, nx) * nc + (1 - c)
        weigh(j)
        send_part(j, sib_buf.at[n], n, {"obs_2": 1 - c})
    for n, d in enumerate(steps):
        j = lax.rem(x + d, nx) * nc + c
        weigh(j)
        rs_cp[n].wait_recv()
        part[part_rows(j), :] = part[part_rows(j), :] + sib_buf[n]
        send_part(j, rs_buf.at[n], nx - 1 + n, {"obs_1": lax.rem(x + d, nx)})
    weigh(x * nc + (1 - c))
    send_part(x * nc + (1 - c), rs_buf.at[nx - 1], ng - 2, {"obs_2": 1 - c})
    weigh(g)
    for cp in tot_cp:
        cp.wait_recv()
    for cp in rs_cp[nx - 1 :]:
        cp.wait_recv()
    act_own = act_i[pl.ds(pl.multiple_of(g * own_rows, own_rows), own_rows), :]
    values = []
    for h in range(halves):
        total = tot_own[h]
        for t in range(ng - 1):
            total = total + tot_buf[t, h]
        raw = part[pl.ds(g * own_rows * halves + h, own_rows, stride=halves), :]
        for t in range(nx):
            raw = raw + rs_buf[t, pl.ds(h, own_rows, stride=halves), :]
        divisor = jnp.ones((own_rows, LANES), jnp.float32)
        for a in range(actions):
            divisor = jnp.where(act_own == a, total[a : a + 1, :], divisor)
        values.append(raw / divisor)
    coded, level = to_codes(values)
    for h in range(halves):
        cols = slice(h * LANES, (h + 1) * LANES)
        w_all[g, :own_rows, cols] = coded[h].astype(jnp.int16)
        w_all[g, own_rows:, cols] = level.astype(jnp.int16)

    w_cp = [
        pltpu.make_async_remote_copy(
            w_all.at[g], w_all.at[g], w_send.at[t], w_recv.at[t], device_id=to_g(t), device_id_type=MESH
        )
        for t in range(ng - 1)
    ]
    for cp in w_cp:
        cp.start()

    def spread_owner(j):
        rows = pl.ds(pl.multiple_of(j * own_rows, own_rows), own_rows)
        low_rows = pl.ds(pl.multiple_of(bel + j * own_rows, own_rows), own_rows)
        w_scale[rows, :] = jnp.broadcast_to(
            scale_of(w_all[j, own_rows : own_rows + 1, :].astype(jnp.int32).astype(jnp.float32)), (own_rows, width)
        )[:, :qwidth]
        act = act_b[rows, :]
        pieces = []
        for h in range(halves):
            q = w_all[j, :own_rows, h * LANES : (h + 1) * LANES].astype(jnp.int32)
            high = jnp.right_shift(q + 128, 8)
            low = q - jnp.left_shift(high, 8)
            pieces.append((high.astype(jnp.float32).astype(jnp.bfloat16), low.astype(jnp.float32).astype(jnp.bfloat16)))

        for a in range(actions):
            hot = act == jnp.asarray(a, jnp.bfloat16)
            for h in range(halves):
                high, low = pieces[h]
                cols = slice(a * width + h * LANES, a * width + (h + 1) * LANES)
                spread[rows, cols] = jnp.where(hot, high, jnp.zeros_like(high))
                spread[low_rows, cols] = jnp.where(hot, low, jnp.zeros_like(low))

    spread_owner(g)
    own_t.wait()
    for cp in t_cp:
        cp.wait_recv()

    def total_action(a, carry):
        tt_own[pl.ds(a, 1), :] = trans_total(a)
        return carry

    lax.fori_loop(0, direct, total_action, 0)
    for cp in tp_cp:
        cp.wait_recv()
    for n in range(ny):
        tt_own[direct + n * per_y : direct + (n + 1) * per_y, :] = tt_share[n]
    tt_cp = [
        pltpu.make_async_remote_copy(
            tt_own, tt_buf.at[t], tt_send.at[t], tt_recv.at[t], device_id=to_z(t), device_id_type=MESH
        )
        for t in range(nz - 1)
    ]
    for cp in tt_cp:
        cp.start()

    for t in range(ng - 1):
        w_cp[t].wait_recv()
        spread_owner(g_from(t))
    for cp in ty_cp:
        cp.wait_recv()
    both = jnp.dot(
        spread[...],
        t_blk[...].reshape(actions * width, qwidth),
        preferred_element_type=jnp.float32,
    )
    fut[...] = (256.0 * both[:bel] + both[bel:]) * w_scale[...]

    def send_future(j, t):
        rows = pl.ds(pl.multiple_of(j * z_rows, z_rows), z_rows)
        act = act_i[rows, :]
        values = []
        for h in range(qwidth // LANES):
            cols = slice(h * LANES, (h + 1) * LANES)
            divisor = jnp.ones((z_rows, LANES), jnp.float32)
            for a in range(actions):
                divisor = jnp.where(act == a, tt_all[a : a + 1, cols], divisor)
            values.append(fut[rows, cols] / divisor)
        coded, level = to_codes(values)
        for n in range(ng):
            parts = [code[n * last : (n + 1) * last] for code in coded]
            piece = jnp.concatenate(parts + [level[: PIECE - used]], axis=0)
            fut_q[t + 1, n] = piece.astype(jnp.int16)
        for u in range(-1, ng - 1):
            if t < 0 and u < 0:
                continue
            n = g if u < 0 else g_at(u)
            cp = pltpu.make_async_remote_copy(
                fut_q.at[t + 1, n, pl.ds(0, used + 2)],
                f_buf.at[t + 1, u + 1, pl.ds(0, used + 2)],
                f_send.at[t + 1, u + 1],
                f_recv.at[t + 1, u + 1],
                device_id={"obs_0": j, "obs_1": n // nc, "obs_2": lax.rem(n, nc)},
                device_id_type=MESH,
            )
            cp.start()
            f_cp.append(cp)

    for cp in tt_cp:
        cp.wait_recv()
    total = tt_own[...]
    for t in range(nz - 1):
        total = total + tt_buf[t]
    tt_all[...] = total
    f_cp = []
    for t in far_first(nz):
        send_future(z_at(t), t)
    send_future(z, -1)
    own_rew.wait()
    for r in range(last):
        rew_ref[r : r + 1, :] = rew_v[pl.ds(act_s[(z * ng + g) * last + r], 1), :]
    for cp in f_cp:
        cp.wait_recv()

    for u in range(ng):
        at = g if u == 0 else g_from(u - 1)
        future = None
        for t in range(nz):
            codes = fut_q[0, g] if u == 0 and t == 0 else f_buf[t, u]
            codes = codes.astype(jnp.int32).astype(jnp.float32)
            term = codes * scale_of(codes[used : used + 1])
            future = term if future is None else future + term
        for h in range(qwidth // LANES):
            out_ref[:, pl.ds(pl.multiple_of(at * qwidth + h * LANES, LANES), LANES)] = future[
                h * last : (h + 1) * last
            ]
    for cp in ob_cp + pk_cp + al_cp[0] + al_cp[1] + share_cp + ts_cp + tp_cp + ty_cp + t_cp + relay_cp + tot_cp + rs_cp + w_cp + f_cp + tt_cp:
        cp.wait_send()


def body(dims, alpha_set, transitions, obs_weights, rewards, chosen_idx, chosen_action):
    ny, nz, nx, nc = dims
    ng = nx * nc
    actions, states = rewards.shape
    bel = chosen_action.shape[0]
    obs_local = obs_weights.shape[0]
    width = states // nz
    qwidth = states // ng
    halves = width // LANES
    count = alpha_set.shape[0] * ny
    f32, b16, i32 = jnp.float32, jnp.bfloat16, jnp.int32
    dma = pltpu.SemaphoreType.DMA
    vmem = pl.BlockSpec(memory_space=pltpu.VMEM)
    hbm = pl.BlockSpec(memory_space=pl.ANY)
    z_rows = bel // nz
    own_rows = bel // ng
    scratch = [
        pltpu.VMEM((ny, count // ny, width), b16),
        pltpu.VMEM((count * halves, LANES), f32),
        pltpu.SMEM((bel,), i32),
        pltpu.VMEM((bel,), i32),
        pltpu.VMEM((actions, obs_local, bel), i32),
        pltpu.VMEM((bel, LANES), i32),
        pltpu.VMEM((bel, LANES), b16),
        pltpu.VMEM((obs_local, actions, states), f32),
        pltpu.VMEM((nz, obs_local, actions, width), jnp.int16),
        pltpu.VMEM((nz, obs_local, actions, width), jnp.int16),
        pltpu.VMEM((nz * actions, obs_local * halves, LANES), f32),
        pltpu.VMEM((obs_local, 1, bel), i32),
        pltpu.VMEM((nz, obs_local, 1, bel), i32),
        [[pltpu.SMEM((1, bel), i32) for _ in range(obs_local)] for _ in range(nz)],
        pltpu.VMEM((bel * halves, LANES), f32),
        pltpu.VMEM((dims[2] - 1, own_rows * halves, LANES), f32),
        pltpu.VMEM((dims[2], own_rows * halves, LANES), f32),
        pltpu.VMEM((halves, actions, LANES), f32),
        pltpu.VMEM((ng - 1, halves, actions, LANES), f32),
        pltpu.VMEM((ng, own_rows + 8, width), jnp.int16),
        pltpu.VMEM((actions, width, qwidth), b16),
        pltpu.VMEM((2 * bel, actions * width), b16),
        pltpu.VMEM((bel, qwidth), f32),
        pltpu.VMEM((bel, qwidth), f32),
        pltpu.VMEM((nz, ng, PIECE, LANES), jnp.int16),
        pltpu.VMEM((nz, ng, PIECE, LANES), jnp.int16),
        pltpu.VMEM((dims[0], actions // (2 * dims[0]), qwidth), f32),
        pltpu.VMEM((actions, qwidth), f32),
        pltpu.VMEM((nz - 1, actions, qwidth), f32),
        pltpu.VMEM((actions, states), f32),
        pltpu.VMEM((actions, qwidth), f32),
        dma((8 + nz * obs_local,)),
        dma((nz - 1,)),
        dma((nz - 1,)),
        dma((2, 2)),
        dma((2, 2)),
        dma((2,)),
        dma((2,)),
        dma((6,)),
        dma((6,)),
        dma((nz - 1,)),
        dma((nz - 1,)),
        dma((ng - 1,)),
        dma((ng - 1,)),
        dma((ng - 1,)),
        dma((ng - 1,)),
        dma((ny - 1,)),
        dma((ny - 1,)),
        dma((ny - 1,)),
        dma((ny - 1,)),
        dma((ng - 1,)),
        dma((ng - 1,)),
        dma((ng - 1,)),
        dma((ng - 1,)),
        dma((ng - 1,)),
        dma((ng - 1,)),
        dma((nz, ng)),
        dma((nz, ng)),
        dma((nz - 1,)),
        dma((nz - 1,)),
    ]
    rows = pltpu.VMEM((bel // (nz * ng), states), f32)
    future, reward = pl.pallas_call(
        functools.partial(kernel, dims),
        out_shape=(rows, rows),
        in_specs=[
            hbm,
            hbm,
            hbm,
            hbm,
            hbm,
            hbm,
        ],
        out_specs=(vmem, vmem),
        scratch_shapes=scratch,
        compiler_params=pltpu.CompilerParams(
            collective_id=0, has_side_effects=True, vmem_limit_bytes=60 * 1024 * 1024
        ),
        name="backup",
    )(
        chosen_action,
        jnp.transpose(chosen_idx, (1, 2, 0)),
        alpha_set,
        transitions,
        obs_weights,
        rewards,
    )
    return reward + DISCOUNT * future


def solution(mesh):
    dims = (mesh.shape["bel"], 8, 4, 2)
    torus = Mesh(
        mesh.devices.reshape(*dims[1:], dims[0]), ("obs_0", "obs_1", "obs_2", "bel")
    )
    return jax.shard_map(
        functools.partial(body, dims),
        mesh=torus,
        in_specs=(
            P("bel", None),
            P(None, OBS, None),
            P(OBS, None, None),
            P(),
            P("bel", None, OBS),
            P("bel"),
        ),
        out_specs=P(BEL_OBS, None),
        check_vma=False,
    )
```

```python
import functools

import jax
import jax.numpy as jnp
from jax import lax
from jax.experimental import pallas as pl
from jax.experimental.pallas import tpu as pltpu
from jax.sharding import Mesh
from jax.sharding import PartitionSpec as P

OBS = ("obs_0", "obs_1", "obs_2")
BEL_OBS = ("bel", "obs_0", "obs_1", "obs_2")
LANES = 128
PIECE = 16
DISCOUNT = 0.95
CODE_SCALE = 14114.0
CODE_SHIFT = 2.302585093 * CODE_SCALE
MESH = pl.DeviceIdType.MESH


def to_codes(values):
    largest = functools.reduce(
        jnp.maximum, [jnp.max(jnp.abs(v), axis=(0, 1), keepdims=True) for v in values]
    )
    level = jnp.ceil(32.0 * jnp.log(jnp.maximum(largest, 1e-30) * (1.0 / 32760.0)))
    inverse = jnp.exp(level * (-1.0 / 32.0))
    coded = [
        jnp.clip(jnp.round(v * inverse), -32767.0, 32767.0).astype(jnp.int32)
        for v in values
    ]
    return coded, jnp.broadcast_to(level, (8, LANES)).astype(jnp.int32)


def scale_of(level):
    return jnp.exp(level * (1.0 / 32.0))


def far_first(n):
    return sorted(range(n - 1), key=lambda t: -min(t + 1, n - 1 - t))


def group_offsets(nx, nc):
    steps = [(dx, dc) for dx in range(nx) for dc in range(nc) if dx or dc]
    return sorted(steps, key=lambda step: -min(step[0], nx - step[0]))


def kernel(
    dims,
    act_hbm,
    idx_hbm,
    alpha_hbm,
    trans_hbm,
    obs_hbm,
    rew_hbm,
    out_ref,
    rew_ref,
    al_bf,
    al_rows,
    act_s,
    act_v,
    idx_v,
    act_i,
    act_b,
    obs_v,
    obs_code,
    obs_all,
    obs_rows,
    pk_own,
    pk_v,
    pk_s,
    part,
    sib_buf,
    rs_buf,
    tot_own,
    tot_buf,
    w_all,
    t_blk,
    spread,
    w_scale,
    fut,
    fut_q,
    f_buf,
    tt_share,
    tt_own,
    tt_buf,
    rew_v,
    tt_all,
    local_sem,
    pk_send,
    pk_recv,
    al_send,
    al_recv,
    relay_send,
    relay_recv,
    share_send,
    share_recv,
    ob_send,
    ob_recv,
    t_send,
    t_recv,
    ts_send,
    ts_recv,
    ty_send,
    ty_recv,
    tp_send,
    tp_recv,
    tot_send,
    tot_recv,
    rs_send,
    rs_recv,
    w_send,
    w_recv,
    f_send,
    f_recv,
    tt_send,
    tt_recv,
):
    ny, nz, nx, nc = dims
    ng = nx * nc
    actions = t_blk.shape[0]
    width = t_blk.shape[1]
    qwidth = t_blk.shape[2]
    halves = width // LANES
    bel = fut.shape[0]
    own_rows = bel // ng
    z_rows = bel // nz
    rows_y = alpha_hbm.shape[0]
    half_y = rows_y // nc
    obs_local = obs_hbm.shape[0]
    t_rows = trans_hbm.shape[1]
    last = out_ref.shape[0]
    used = last * (qwidth // LANES)
    per_y = actions // (2 * ny)
    direct = actions - per_y * ny

    y = lax.axis_index("bel")
    z = lax.axis_index("obs_0")
    x = lax.axis_index("obs_1")
    c = lax.axis_index("obs_2")
    g = x * nc + c

    def y_at(t):
        return lax.rem(y + 1 + t, ny)

    def z_at(t):
        return lax.rem(z + 1 + t, nz)

    offsets = group_offsets(nx, nc)

    def g_at(t):
        dx, dc = offsets[t]
        return lax.rem(x + dx, nx) * nc + lax.rem(c + dc, nc)

    def g_from(t):
        dx, dc = offsets[t]
        return lax.rem(x + nx - dx, nx) * nc + lax.rem(c + nc - dc, nc)

    def to_y(t):
        return {"bel": y_at(t)}

    def to_z(t):
        return {"obs_0": z_at(t)}

    def to_g(t):
        j = g_at(t)
        return {"obs_1": j // nc, "obs_2": lax.rem(j, nc)}

    peers = (
        [to_y(t) for t in range(ny - 1)]
        + [to_z(t) for t in range(nz - 1)]
        + [to_g(t) for t in range(ng - 1)]
    )
    barrier = pltpu.get_barrier_semaphore()
    for peer in peers:
        pl.semaphore_signal(barrier, inc=1, device_id=peer, device_id_type=MESH)

    z_cols = pl.ds(pl.multiple_of(z * width, width), width)
    q_cols = pl.ds(pl.multiple_of(g * qwidth, qwidth), qwidth)

    own_al = pltpu.make_async_copy(alpha_hbm.at[:, z_cols], al_bf.at[y], local_sem.at[7])
    own_ob = pltpu.make_async_copy(obs_hbm, obs_v, local_sem.at[2])
    g_rows = pl.ds(pl.multiple_of(g * t_rows, t_rows), t_rows)
    mine = pl.ds(direct + y * per_y, per_y)
    own_t = pltpu.make_async_copy(
        trans_hbm.at[:direct, :, q_cols], t_blk.at[:direct, g_rows, :], local_sem.at[3]
    )
    own_ts = pltpu.make_async_copy(
        trans_hbm.at[mine, :, q_cols], t_blk.at[mine, g_rows, :], local_sem.at[0]
    )
    own_rew = pltpu.make_async_copy(rew_hbm, rew_v, local_sem.at[4])
    own_act = [
        pltpu.make_async_copy(act_hbm, act_s, local_sem.at[1]),
        pltpu.make_async_copy(act_hbm, act_v, local_sem.at[5]),
        pltpu.make_async_copy(idx_hbm, idx_v, local_sem.at[6]),
    ]
    for cp in own_act:
        cp.start()
    own_ob.start()
    own_al.start()
    own_t.start()
    own_ts.start()
    own_rew.start()

    pl.semaphore_wait(barrier, len(peers))

    quarter = half_y // 2
    quarters = [pl.ds(pl.multiple_of(c * half_y + n * quarter, quarter), quarter) for n in range(2)]
    pk_cp = [
        pltpu.make_async_remote_copy(
            pk_own,
            pk_v.at[z],
            pk_send.at[t],
            pk_recv.at[t],
            device_id=to_z(t),
            device_id_type=MESH,
        )
        for t in range(nz - 1)
    ]
    al_cp = [
        [
            pltpu.make_async_remote_copy(
                al_bf.at[y, quarters[n]],
                al_bf.at[y, quarters[n]],
                al_send.at[t, m],
                al_recv.at[t, m],
                device_id={"bel": lax.rem(y + step, ny)},
                device_id_type=MESH,
            )
            for m, n in enumerate((t, 1 - t))
        ]
        for t, step in ((0, 1), (1, ny - 1))
    ]
    ob_cp = [
        pltpu.make_async_remote_copy(
            obs_code.at[z_at(t)],
            obs_all.at[z],
            ob_send.at[t],
            ob_recv.at[t],
            device_id=to_z(t),
            device_id_type=MESH,
        )
        for t in range(nz - 1)
    ]
    def trans_copy(t, which, send, recv):
        return pltpu.make_async_remote_copy(
            trans_hbm.at[which, :, pl.ds(pl.multiple_of(g_at(t) * qwidth, qwidth), qwidth)],
            t_blk.at[which, g_rows, :],
            send.at[t],
            recv.at[t],
            device_id=to_g(t),
            device_id_type=MESH,
        )

    ts_cp = [trans_copy(t, mine, ts_send, ts_recv) for t in range(ng - 1)]
    t_cp = [trans_copy(t, pl.ds(0, direct), t_send, t_recv) for t in range(ng - 1)]
    own_al.wait()
    across = lax.rem(y + ny - 2, ny)
    relay_cp = [
        pltpu.make_async_remote_copy(
            al_bf.at[y, quarters[n]],
            al_bf.at[y, quarters[n]],
            relay_send.at[n],
            relay_recv.at[n],
            device_id={"bel": across},
            device_id_type=MESH,
        )
        for n in range(2)
    ]
    for m in range(2):
        for pair in al_cp:
            pair[m].start()
    for m in range(2):
        relay_cp[m].start()
    for cp in ts_cp:
        cp.start()
    for cp in t_cp:
        cp.start()

    for cp in own_act:
        cp.wait()
    act_row = act_v[...].reshape(1, bel)
    picks = jnp.zeros((obs_local, bel), jnp.int32)
    for a in range(actions):
        picks = jnp.where(act_row == a, idx_v[a] * halves, picks)
    for o in range(obs_local):
        pk_own[o] = picks[o : o + 1, :]
        pk_v[z, o] = picks[o : o + 1, :]
    for cp in pk_cp:
        cp.start()
    own_ob.wait()
    for n in range(nz):
        for o in range(obs_local):
            v = jnp.log(obs_v[o, :, n * width : (n + 1) * width])
            obs_code[n, o] = jnp.round(v * CODE_SCALE + CODE_SHIFT).astype(jnp.int32).astype(jnp.int16)
    for t in far_first(nz):
        ob_cp[t].start()

    def spread_alpha(block, start, rows):
        def rows16(n, carry):
            r = pl.multiple_of(start + n * 16, 16)
            v = al_bf[block, pl.ds(r, 16), :].astype(jnp.float32)
            for h in range(halves):
                al_rows[pl.ds((block * rows_y + r) * halves + h, 16, stride=halves), :] = v[
                    :, h * LANES : (h + 1) * LANES
                ]
            return carry

        lax.fori_loop(0, rows // 16, rows16, 0, unroll=4)

    spread_alpha(y, 0, rows_y)

    def fill_action(b, carry):
        act_i[pl.ds(b, 1), :] = jnp.full((1, LANES), act_s[b], jnp.int32)
        return carry

    lax.fori_loop(0, bel, fill_action, 0, unroll=8)
    act_b[...] = act_i[...].astype(jnp.float32).astype(jnp.bfloat16)

    totals = [jnp.zeros((actions, LANES), jnp.float32) for _ in range(halves)]

    def decode(code_ref, slot):
        for o in range(obs_local):
            v = jnp.exp(
                code_ref[slot, o].astype(jnp.int32).astype(jnp.float32) * (1.0 / CODE_SCALE)
            )
            for h in range(halves):
                part_h = v[:, h * LANES : (h + 1) * LANES]
                totals[h] = totals[h] + part_h
                obs_rows[pl.ds(slot * actions, actions), o * halves + h, :] = part_h

    decode(obs_code, z)
    share_cp = []

    def share(block, rows):
        cp = pltpu.make_async_remote_copy(
            al_bf.at[block, rows],
            al_bf.at[block, rows],
            share_send.at[len(share_cp)],
            share_recv.at[len(share_cp)],
            device_id={"obs_2": 1 - c},
            device_id_type=MESH,
        )
        cp.start()
        share_cp.append(cp)

    before, after, across = (lax.rem(y + n, ny) for n in (ny - 1, 1, ny - 2))
    for t, source in enumerate((before, after)):
        al_cp[t][0].wait_recv()
        share(source, quarters[t])
    for t, source in enumerate((before, after)):
        al_cp[t][1].wait_recv()
        share(source, quarters[1 - t])
    for t in range(2):
        relay_cp[t].wait_recv()
        share(across, quarters[t])
    for cp in pk_cp:
        cp.wait_recv()
    to_scalar = [
        [
            pltpu.make_async_copy(pk_v.at[n, o], pk_s[n][o], local_sem.at[8 + n * obs_local + o])
            for o in range(obs_local)
        ]
        for n in range(nz)
    ]
    for pair in to_scalar:
        for cp in pair:
            cp.start()
    for source in (before, after):
        spread_alpha(source, c * half_y, half_y)
    spread_alpha(across, c * half_y, half_y)
    for t in far_first(nz):
        ob_cp[t].wait_recv()
        decode(obs_all, lax.rem(z + nz - 1 - t, nz))
    for h in range(halves):
        tot_own[h] = totals[h]
    tot_cp = [
        pltpu.make_async_remote_copy(
            tot_own, tot_buf.at[t], tot_send.at[t], tot_recv.at[t], device_id=to_g(t), device_id_type=MESH
        )
        for t in range(ng - 1)
    ]
    for cp in tot_cp:
        cp.start()

    other = (1 - c) * half_y
    for cp, (source, n) in zip(
        share_cp, ((before, 0), (after, 1), (before, 1), (after, 0), (across, 0), (across, 1))
    ):
        cp.wait_recv()
        spread_alpha(source, other + n * quarter, quarter)
    own_ts.wait()
    for cp in ts_cp:
        cp.wait_recv()

    def trans_total(a):
        return jnp.sum(t_blk[a].astype(jnp.float32), axis=0, keepdims=True)

    for n in range(per_y):
        tt_share[y, n : n + 1, :] = trans_total(direct + y * per_y + n)
    tp_cp = [
        pltpu.make_async_remote_copy(
            tt_share.at[y],
            tt_share.at[y],
            tp_send.at[n],
            tp_recv.at[n],
            device_id={"bel": to},
            device_id_type=MESH,
        )
        for n, to in enumerate((across, after, before))
    ]
    for cp in tp_cp:
        cp.start()

    def trans_share(which, n, target):
        return pltpu.make_async_remote_copy(
            t_blk.at[which],
            t_blk.at[which],
            ty_send.at[n],
            ty_recv.at[n],
            device_id={"bel": target},
            device_id_type=MESH,
        )

    ty_cp = [trans_share(mine, n, to) for n, to in enumerate((across, after, before))]
    for cp in ty_cp:
        cp.start()
    for pair in to_scalar:
        for cp in pair:
            cp.wait()
    rs_cp = []
    rows = own_rows * halves

    def part_rows(j):
        return pl.ds(pl.multiple_of(j * rows, rows), rows)

    def weigh(j):
        def one_belief(r, carry):
            b = j * own_rows + r
            a = act_s[b]
            sums = [None] * 4
            for n in range(nz):
                probs = obs_rows[n * actions + a]
                for o in range(obs_local):
                    term = al_rows[pl.ds(pk_s[n][o][0, b], halves), :] * probs[o * halves : (o + 1) * halves]
                    sums[o % 4] = term if n == 0 else sums[o % 4] + term
            part[pl.ds(pl.multiple_of(b * halves, halves), halves), :] = (sums[0] + sums[1]) + (
                sums[2] + sums[3]
            )
            return carry

        lax.fori_loop(0, own_rows, one_belief, 0, unroll=8)

    def send_part(j, landing, n, to):
        cp = pltpu.make_async_remote_copy(
            part.at[part_rows(j), :],
            landing,
            rs_send.at[n],
            rs_recv.at[n],
            device_id=to,
            device_id_type=MESH,
        )
        cp.start()
        rs_cp.append(cp)

    steps = sorted(range(1, nx), key=lambda d: -min(d, nx - d))
    for n, d in enumerate(steps):
        j = lax.rem(x + d, nx) * nc + (1 - c)
        weigh(j)
        send_part(j, sib_buf.at[n], n, {"obs_2": 1 - c})
    for n, d in enumerate(steps):
        j = lax.rem(x + d, nx) * nc + c
        weigh(j)
        rs_cp[n].wait_recv()
        part[part_rows(j), :] = part[part_rows(j), :] + sib_buf[n]
        send_part(j, rs_buf.at[n], nx - 1 + n, {"obs_1": lax.rem(x + d, nx)})
    weigh(x * nc + (1 - c))
    send_part(x * nc + (1 - c), rs_buf.at[nx - 1], ng - 2, {"obs_2": 1 - c})
    weigh(g)
    for cp in tot_cp:
        cp.wait_recv()
    for cp in rs_cp[nx - 1 :]:
        cp.wait_recv()
    act_own = act_i[pl.ds(pl.multiple_of(g * own_rows, own_rows), own_rows), :]
    values = []
    for h in range(halves):
        total = tot_own[h]
        for t in range(ng - 1):
            total = total + tot_buf[t, h]
        raw = part[pl.ds(g * own_rows * halves + h, own_rows, stride=halves), :]
        for t in range(nx):
            raw = raw + rs_buf[t, pl.ds(h, own_rows, stride=halves), :]
        divisor = jnp.ones((own_rows, LANES), jnp.float32)
        for a in range(actions):
            divisor = jnp.where(act_own == a, total[a : a + 1, :], divisor)
        values.append(raw / divisor)
    coded, level = to_codes(values)
    for h in range(halves):
        w_all[g, h * own_rows : (h + 1) * own_rows, :] = coded[h].astype(jnp.int16)
    w_used = halves * own_rows
    w_all[g, w_used : w_used + 8, :] = level.astype(jnp.int16)

    w_cp = [
        pltpu.make_async_remote_copy(
            w_all.at[g, pl.ds(0, w_used + 2)],
            w_all.at[g, pl.ds(0, w_used + 2)],
            w_send.at[t],
            w_recv.at[t],
            device_id=to_g(t),
            device_id_type=MESH,
        )
        for t in range(ng - 1)
    ]
    for cp in w_cp:
        cp.start()

    def spread_owner(j):
        rows = pl.ds(pl.multiple_of(j * own_rows, own_rows), own_rows)
        low_rows = pl.ds(pl.multiple_of(bel + j * own_rows, own_rows), own_rows)
        scale = scale_of(w_all[j, w_used : w_used + 1, :].astype(jnp.int32).astype(jnp.float32))
        for h in range(qwidth // LANES):
            w_scale[rows, h * LANES : (h + 1) * LANES] = jnp.broadcast_to(scale, (own_rows, LANES))
        act = act_b[rows, :]
        pieces = []
        for h in range(halves):
            q = w_all[j, h * own_rows : (h + 1) * own_rows, :].astype(jnp.int32)
            high = jnp.right_shift(q + 128, 8)
            low = q - jnp.left_shift(high, 8)
            pieces.append((high.astype(jnp.float32).astype(jnp.bfloat16), low.astype(jnp.float32).astype(jnp.bfloat16)))

        for a in range(actions):
            hot = act == jnp.asarray(a, jnp.bfloat16)
            for h in range(halves):
                high, low = pieces[h]
                cols = slice(a * width + h * LANES, a * width + (h + 1) * LANES)
                spread[rows, cols] = jnp.where(hot, high, jnp.zeros_like(high))
                spread[low_rows, cols] = jnp.where(hot, low, jnp.zeros_like(low))

    spread_owner(g)
    own_t.wait()
    for cp in t_cp:
        cp.wait_recv()

    def total_action(a, carry):
        tt_own[pl.ds(a, 1), :] = trans_total(a)
        return carry

    lax.fori_loop(0, direct, total_action, 0)
    for cp in tp_cp:
        cp.wait_recv()
    for n in range(ny):
        tt_own[direct + n * per_y : direct + (n + 1) * per_y, :] = tt_share[n]
    tt_cp = [
        pltpu.make_async_remote_copy(
            tt_own, tt_buf.at[t], tt_send.at[t], tt_recv.at[t], device_id=to_z(t), device_id_type=MESH
        )
        for t in range(nz - 1)
    ]
    for cp in tt_cp:
        cp.start()

    for t in range(ng - 1):
        w_cp[t].wait_recv()
        spread_owner(g_from(t))
    for cp in ty_cp:
        cp.wait_recv()
    both = jnp.dot(
        spread[...],
        t_blk[...].reshape(actions * width, qwidth),
        preferred_element_type=jnp.float32,
    )
    fut[...] = (256.0 * both[:bel] + both[bel:]) * w_scale[...]

    def send_future(j, t):
        rows = pl.ds(pl.multiple_of(j * z_rows, z_rows), z_rows)
        act = act_i[rows, :]
        values = []
        for h in range(qwidth // LANES):
            cols = slice(h * LANES, (h + 1) * LANES)
            divisor = jnp.ones((z_rows, LANES), jnp.float32)
            for a in range(actions):
                divisor = jnp.where(act == a, tt_all[a : a + 1, cols], divisor)
            values.append(fut[rows, cols] / divisor)
        coded, level = to_codes(values)
        for n in range(ng):
            parts = [code[n * last : (n + 1) * last] for code in coded]
            piece = jnp.concatenate(parts + [level[: PIECE - used]], axis=0)
            fut_q[t + 1, n] = piece.astype(jnp.int16)
        for u in range(-1, ng - 1):
            if t < 0 and u < 0:
                continue
            n = g if u < 0 else g_at(u)
            cp = pltpu.make_async_remote_copy(
                fut_q.at[t + 1, n, pl.ds(0, used + 2)],
                f_buf.at[t + 1, u + 1, pl.ds(0, used + 2)],
                f_send.at[t + 1, u + 1],
                f_recv.at[t + 1, u + 1],
                device_id={"obs_0": j, "obs_1": n // nc, "obs_2": lax.rem(n, nc)},
                device_id_type=MESH,
            )
            cp.start()
            f_cp.append(cp)

    for cp in tt_cp:
        cp.wait_recv()
    total = tt_own[...]
    for t in range(nz - 1):
        total = total + tt_buf[t]
    tt_all[...] = total
    f_cp = []
    for t in far_first(nz):
        send_future(z_at(t), t)
    send_future(z, -1)
    own_rew.wait()
    for r in range(last):
        rew_ref[r : r + 1, :] = rew_v[pl.ds(act_s[(z * ng + g) * last + r], 1), :]
    for cp in f_cp:
        cp.wait_recv()

    for u in range(ng):
        at = g if u == 0 else g_from(u - 1)
        future = None
        for t in range(nz):
            codes = fut_q[0, g] if u == 0 and t == 0 else f_buf[t, u]
            codes = codes.astype(jnp.int32).astype(jnp.float32)
            term = codes * scale_of(codes[used : used + 1])
            future = term if future is None else future + term
        for h in range(qwidth // LANES):
            out_ref[:, pl.ds(pl.multiple_of(at * qwidth + h * LANES, LANES), LANES)] = future[
                h * last : (h + 1) * last
            ]
    for cp in ob_cp + pk_cp + al_cp[0] + al_cp[1] + share_cp + ts_cp + tp_cp + ty_cp + t_cp + relay_cp + tot_cp + rs_cp + w_cp + f_cp + tt_cp:
        cp.wait_send()


def body(dims, alpha_set, transitions, obs_weights, rewards, chosen_idx, chosen_action):
    ny, nz, nx, nc = dims
    ng = nx * nc
    actions, states = rewards.shape
    bel = chosen_action.shape[0]
    obs_local = obs_weights.shape[0]
    width = states // nz
    qwidth = states // ng
    halves = width // LANES
    count = alpha_set.shape[0] * ny
    f32, b16, i32 = jnp.float32, jnp.bfloat16, jnp.int32
    dma = pltpu.SemaphoreType.DMA
    vmem = pl.BlockSpec(memory_space=pltpu.VMEM)
    hbm = pl.BlockSpec(memory_space=pl.ANY)
    z_rows = bel // nz
    own_rows = bel // ng
    scratch = [
        pltpu.VMEM((ny, count // ny, width), b16),
        pltpu.VMEM((count * halves, LANES), f32),
        pltpu.SMEM((bel,), i32),
        pltpu.VMEM((bel,), i32),
        pltpu.VMEM((actions, obs_local, bel), i32),
        pltpu.VMEM((bel, LANES), i32),
        pltpu.VMEM((bel, LANES), b16),
        pltpu.VMEM((obs_local, actions, states), f32),
        pltpu.VMEM((nz, obs_local, actions, width), jnp.int16),
        pltpu.VMEM((nz, obs_local, actions, width), jnp.int16),
        pltpu.VMEM((nz * actions, obs_local * halves, LANES), f32),
        pltpu.VMEM((obs_local, 1, bel), i32),
        pltpu.VMEM((nz, obs_local, 1, bel), i32),
        [[pltpu.SMEM((1, bel), i32) for _ in range(obs_local)] for _ in range(nz)],
        pltpu.VMEM((bel * halves, LANES), f32),
        pltpu.VMEM((dims[2] - 1, own_rows * halves, LANES), f32),
        pltpu.VMEM((dims[2], own_rows * halves, LANES), f32),
        pltpu.VMEM((halves, actions, LANES), f32),
        pltpu.VMEM((ng - 1, halves, actions, LANES), f32),
        pltpu.VMEM((ng, halves * own_rows + 16, LANES), jnp.int16),
        pltpu.VMEM((actions, width, qwidth), b16),
        pltpu.VMEM((2 * bel, actions * width), b16),
        pltpu.VMEM((bel, qwidth), f32),
        pltpu.VMEM((bel, qwidth), f32),
        pltpu.VMEM((nz, ng, PIECE, LANES), jnp.int16),
        pltpu.VMEM((nz, ng, PIECE, LANES), jnp.int16),
        pltpu.VMEM((dims[0], actions // (2 * dims[0]), qwidth), f32),
        pltpu.VMEM((actions, qwidth), f32),
        pltpu.VMEM((nz - 1, actions, qwidth), f32),
        pltpu.VMEM((actions, states), f32),
        pltpu.VMEM((actions, qwidth), f32),
        dma((8 + nz * obs_local,)),
        dma((nz - 1,)),
        dma((nz - 1,)),
        dma((2, 2)),
        dma((2, 2)),
        dma((2,)),
        dma((2,)),
        dma((6,)),
        dma((6,)),
        dma((nz - 1,)),
        dma((nz - 1,)),
        dma((ng - 1,)),
        dma((ng - 1,)),
        dma((ng - 1,)),
        dma((ng - 1,)),
        dma((ny - 1,)),
        dma((ny - 1,)),
        dma((ny - 1,)),
        dma((ny - 1,)),
        dma((ng - 1,)),
        dma((ng - 1,)),
        dma((ng - 1,)),
        dma((ng - 1,)),
        dma((ng - 1,)),
        dma((ng - 1,)),
        dma((nz, ng)),
        dma((nz, ng)),
        dma((nz - 1,)),
        dma((nz - 1,)),
    ]
    rows = pltpu.VMEM((bel // (nz * ng), states), f32)
    future, reward = pl.pallas_call(
        functools.partial(kernel, dims),
        out_shape=(rows, rows),
        in_specs=[
            hbm,
            hbm,
            hbm,
            hbm,
            hbm,
            hbm,
        ],
        out_specs=(vmem, vmem),
        scratch_shapes=scratch,
        compiler_params=pltpu.CompilerParams(
            collective_id=0, has_side_effects=True, vmem_limit_bytes=60 * 1024 * 1024
        ),
        name="backup",
    )(
        chosen_action,
        jnp.transpose(chosen_idx, (1, 2, 0)),
        alpha_set,
        transitions,
        obs_weights,
        rewards,
    )
    return reward + DISCOUNT * future


def solution(mesh):
    dims = (mesh.shape["bel"], 8, 4, 2)
    torus = Mesh(
        mesh.devices.reshape(*dims[1:], dims[0]), ("obs_0", "obs_1", "obs_2", "bel")
    )
    return jax.shard_map(
        functools.partial(body, dims),
        mesh=torus,
        in_specs=(
            P("bel", None),
            P(None, OBS, None),
            P(OBS, None, None),
            P(),
            P("bel", None, OBS),
            P("bel"),
        ),
        out_specs=P(BEL_OBS, None),
        check_vma=False,
    )
```
